8 devices in a mesh: col: 2 (over z, y), row: 4 (over x, core).
Axes of the slice: x: 2, y: 2, z: 1, core: 2. Of those that a mesh axis runs over, the one named last changes fastest.
Arguments:
- inter_mask: int32 [8192, 16384], P('row', 'col')
- user_emb: bfloat16 [8192, 64], P(('row', 'col'))
- item_emb: bfloat16 [16384, 64], P(('col', 'row'))
- triples: int32 [8192, 3], replicated
Outputs:
- output 1: bfloat16 [8192, 64], P(('row', 'col'))
- output 2: bfloat16 [16384, 64], P(('col', 'row'))
- output 3: float32 [], replicated
- output 4: float32 [8192, 64], P(('row', 'col'))
- output 5: float32 [16384, 64], P(('col', 'row'))
All inputs are finite; a program needn't handle non-finite values.
Results may differ from the reference program's by a relative error of at most 0.0104521.
Values are sent between devices in bfloat16 or wider.
A program may use at most 1 GiB of HBM per device.

```python
import jax
import jax.numpy as jnp
from jax import lax

NUM_USERS = 8192
NUM_ITEMS = 16384
EMBED_DIM = 64
BATCH_SIZE = 8192
LAYERS = 3


def setup_inputs(seed: int = 0) -> dict:
    base_key = jax.random.key(seed)
    key_list = jax.random.split(base_key, 10)
    act_user = jax.random.randint(key_list[0], (NUM_USERS,), 1, 5)
    act_item = jax.random.randint(key_list[1], (NUM_ITEMS,), 1, 5)
    draw_vals = jax.random.randint(key_list[2], (NUM_USERS, NUM_ITEMS), 0, 2 * NUM_ITEMS)
    inter_mask = (draw_vals < act_user[:, None] * act_item[None, :] * 10).astype(jnp.int32)
    emb_scale = EMBED_DIM ** -0.25
    mean_user = jax.random.normal(key_list[3], (EMBED_DIM,), jnp.float32)
    mean_item = jax.random.normal(key_list[4], (EMBED_DIM,), jnp.float32)
    noise_user = jax.random.normal(key_list[5], (NUM_USERS, EMBED_DIM), jnp.float32)
    noise_item = jax.random.normal(key_list[6], (NUM_ITEMS, EMBED_DIM), jnp.float32)
    user_emb = ((mean_user[None, :] + noise_user) * emb_scale).astype(jnp.bfloat16)
    item_emb = ((mean_item[None, :] + noise_item) * emb_scale).astype(jnp.bfloat16)
    user_ids = jax.random.randint(key_list[7], (BATCH_SIZE,), 0, NUM_USERS)
    user_ids = user_ids.at[0].set(NUM_USERS - 1).at[1].set(0)
    pos_ids = jax.random.randint(key_list[8], (BATCH_SIZE,), 0, NUM_ITEMS)
    pos_ids = pos_ids.at[0].set(NUM_ITEMS - 1).at[1].set(0)
    neg_ids = jax.random.randint(key_list[9], (BATCH_SIZE,), 0, NUM_ITEMS)
    neg_ids = neg_ids.at[0].set(0).at[1].set(NUM_ITEMS - 1)
    triples = jnp.stack([user_ids, pos_ids, neg_ids], axis=1).astype(jnp.int32)
    return {'inter_mask': inter_mask, 'user_emb': user_emb, 'item_emb': item_emb, 'triples': triples}


def reference(inter_mask, user_emb, item_emb, triples):
    deg_user = jnp.maximum(jnp.sum(inter_mask, axis=1, dtype=jnp.int32), 1)
    deg_item = jnp.maximum(jnp.sum(inter_mask, axis=0, dtype=jnp.int32), 1)
    scale_user = lax.rsqrt(deg_user.astype(jnp.float32))
    scale_item = lax.rsqrt(deg_item.astype(jnp.float32))
    adj_mat = (scale_user[:, None] * inter_mask.astype(jnp.float32) * scale_item[None, :]).astype(jnp.bfloat16)

    def to_users(item_side):
        return jnp.dot(adj_mat, item_side, preferred_element_type=jnp.float32)

    def to_items(user_side):
        return lax.dot_general(adj_mat, user_side, (((0,), (0,)), ((), ())), preferred_element_type=jnp.float32)

    user_cur = user_emb
    item_cur = item_emb
    user_acc = user_emb.astype(jnp.float32)
    item_acc = item_emb.astype(jnp.float32)
    for _ in range(LAYERS):
        user_next = to_users(item_cur).astype(jnp.bfloat16)
        item_next = to_items(user_cur).astype(jnp.bfloat16)
        user_acc = user_acc + user_next.astype(jnp.float32)
        item_acc = item_acc + item_next.astype(jnp.float32)
        user_cur, item_cur = user_next, item_next
    user_out = (user_acc / (LAYERS + 1)).astype(jnp.bfloat16)
    item_out = (item_acc / (LAYERS + 1)).astype(jnp.bfloat16)

    def score_loss(user_table, item_table):
        e_user = jnp.take(user_table, triples[:, 0], axis=0)
        e_pos = jnp.take(item_table, triples[:, 1], axis=0)
        e_neg = jnp.take(item_table, triples[:, 2], axis=0)
        margin = jnp.sum(e_user * e_pos, axis=1) - jnp.sum(e_user * e_neg, axis=1)
        return jnp.mean(jax.nn.softplus(-margin))

    bpr_loss, pullback = jax.vjp(score_loss, user_out.astype(jnp.float32), item_out.astype(jnp.float32))
    grad_user_out, grad_item_out = pullback(jnp.ones_like(bpr_loss))
    src_user = grad_user_out / (LAYERS + 1)
    src_item = grad_item_out / (LAYERS + 1)
    cot_user = src_user.astype(jnp.bfloat16)
    cot_item = src_item.astype(jnp.bfloat16)
    for _ in range(LAYERS - 1):
        new_user = (src_user + to_users(cot_item)).astype(jnp.bfloat16)
        new_item = (src_item + to_items(cot_user)).astype(jnp.bfloat16)
        cot_user, cot_item = new_user, new_item
    grad_user = src_user + to_users(cot_item)
    grad_item = src_item + to_items(cot_user)
    return user_out, item_out, bpr_loss, grad_user, grad_item
```

```python
import jax
import jax.numpy as jnp
from jax import lax
from jax.experimental import pallas as pl
from jax.experimental.pallas import tpu as pltpu
from jax.sharding import PartitionSpec as P

MESH = pl.DeviceIdType.MESH
F32 = jnp.float32
BF16 = jnp.bfloat16

D = 64
UB = 1024
IB = 2048
RU = 2048
CI = 8192
STEPS = 3
SX = 4
WX = IB // SX
SY = 2
WY = UB // SY
TB = 1024
NT = 8192
PU = UB // 2
PI = IB // 2
PR = PU + PI

FD, XR, FO, GP, GX, GF, YR, YG = range(8)
VMEM_LIMIT = 67043328


def _coords():
    c = lax.axis_index('col')
    r = lax.axis_index('row')
    x = r // 2
    h = r % 2
    return c, r, x, h


def _dot(a, b):
    return lax.dot_general(a, b, (((1,), (0,)), ((), ())), preferred_element_type=F32)


def _dot_t(a, b):
    return lax.dot_general(a, b, (((1,), (1,)), ((), ())), preferred_element_type=F32)


def _al(v, m):
    return pl.multiple_of(v, m)


class Links:
    def __init__(self):
        self.c, self.r, self.x, self.h = _coords()
        c, r, x, h = self.c, self.r, self.x, self.h
        self.partner = (c, 2 * x + (1 - h))
        self.xn = (c, 2 * (1 - x) + h)
        self.yn = (1 - c, r)
        self.diag = (1 - c, 2 * (1 - x) + h)
        self.xpartner = (c, 2 * (1 - x) + (1 - h))
        self.slot = r * 2 + c

    def barrier(self):
        sem = pltpu.get_barrier_semaphore()
        peers = (self.partner, self.xn, self.yn, self.diag, self.xpartner)
        for p in peers:
            pl.semaphore_signal(sem, inc=1, device_id=p, device_id_type=MESH)
        pl.semaphore_wait(sem, len(peers))


def _slot_of(dev):
    return dev[1] * 2 + dev[0]


def _remote(src, dst, ss, rs, dev):
    return pltpu.make_async_remote_copy(src_ref=src, dst_ref=dst, send_sem=ss, recv_sem=rs, device_id=dev, device_id_type=MESH)


class Prop:
    def __init__(self, lk, a, ei, eu, pi, pu, rf, ro, rx, ry, ss, rs):
        self.lk = lk
        self.a, self.ei, self.eu, self.pi, self.pu = a, ei, eu, pi, pu
        self.rf, self.ro, self.rx, self.ry = rf, ro, rx, ry
        self.ss, self.rs = ss, rs

    def msg(self, kind, k, s):
        lk = self.lk
        ss, rs = self.ss.at[k, kind, s], self.rs.at[k, kind, s]
        other = 1 - lk.x
        if kind == FD:
            src = self.pi.at[:, pl.ds(_al((2 * other + 1 - lk.h) * IB + s * WX, 128), WX)]
            dst = self.rf.at[k, :, pl.ds(_al(s * WX, 128), WX)]
            return _remote(src, dst, ss, rs, lk.partner)
        if kind == XR:
            src = self.pi.at[:, pl.ds(_al((2 * other + lk.h) * IB + s * WX, 128), WX)]
            dst = self.rx.at[k, :, pl.ds(_al(s * WX, 128), WX)]
            return _remote(src, dst, ss, rs, lk.xn)
        if kind == FO:
            src = self.pi.at[:, pl.ds(_al((2 * lk.x + 1 - lk.h) * IB + s * WX, 128), WX)]
            dst = self.ro.at[k, :, pl.ds(_al(s * WX, 128), WX)]
            return _remote(src, dst, ss, rs, lk.partner)
        if kind in (GP, GX):
            ref = self.ei.at[k, :, pl.ds(_al(lk.r * IB + s * WX, 128), WX)]
            return _remote(ref, ref, ss, rs, lk.partner if kind == GP else lk.xn)
        if kind == GF:
            ref = self.ei.at[k, :, pl.ds(_al((2 * other + lk.h) * IB + s * WX, 128), WX)]
            return _remote(ref, ref, ss, rs, lk.partner)
        if kind == YR:
            src = self.pu.at[:, pl.ds(_al((1 - lk.c) * UB + s * WY, 128), WY)]
            dst = self.ry.at[k, :, pl.ds(_al(s * WY, 128), WY)]
            return _remote(src, dst, ss, rs, lk.yn)
        ref = self.eu.at[k, :, pl.ds(_al(lk.c * UB + s * WY, 128), WY)]
        return _remote(ref, ref, ss, rs, lk.yn)

    def put_item(self, k, s, value):
        self.ei[k, :, pl.ds(_al(self.lk.r * IB + s * WX, 128), WX)] = value
        self.msg(GX, k, s).start()
        self.msg(GP, k, s).start()

    def put_user(self, k, s, value):
        self.eu[k, :, pl.ds(_al(self.lk.c * UB + s * WY, 128), WY)] = value
        self.msg(YG, k, s).start()

    def wait_puts(self, k):
        for s in range(SX):
            self.msg(GX, k, s).wait_send()
            self.msg(GP, k, s).wait_send()
            self.msg(GF, k, s).wait_send()
        for s in range(SY):
            self.msg(YG, k, s).wait_send()

    def step(self, k, user_final, item_final):
        lk = self.lk
        a, ei, eu, pi, pu = self.a, self.ei, self.eu, self.pi, self.pu
        far = (1 - lk.x) * 2 * IB
        near = lk.x * 2 * IB
        own_u = lk.c * UB
        peer_u = (1 - lk.c) * UB

        if k > 0:
            for s in range(SX):
                self.msg(FD, k - 1, s).wait_send()
                self.msg(XR, k - 1, s).wait_send()

        def far_own(j, _):
            cols = pl.ds(_al(far + j * 1024, 128), 1024)
            pi[:, cols] = _dot(eu[k, :, pl.ds(_al(own_u, 128), UB)], a[pl.ds(_al(own_u, 128), UB), cols])
            return 0

        lax.fori_loop(0, 4, far_own, 0)
        for s in range(SY):
            self.msg(YG, k, s).wait_recv()

        def chip_sum(s):
            self.msg(FD, k, s).wait_recv()
            cols = pl.ds(_al((2 * (1 - lk.x) + lk.h) * IB + s * WX, 128), WX)
            pi[:, cols] = pi[:, cols] + self.rf[k, :, pl.ds(_al(s * WX, 128), WX)]
            self.msg(XR, k, s).start()

        def far_peer(s, _):
            e = eu[k, :, pl.ds(_al(peer_u, 128), UB)]
            rows = pl.ds(_al(peer_u, 128), UB)
            c1 = pl.ds(_al(far + (1 - lk.h) * IB + s * WX, 128), WX)
            c2 = pl.ds(_al(far + lk.h * IB + s * WX, 128), WX)
            pi[:, c1] = pi[:, c1] + _dot(e, a[rows, c1])
            pi[:, c2] = pi[:, c2] + _dot(e, a[rows, c2])
            self.msg(FD, k, s).start()

            @pl.when(s >= 1)
            def _():
                chip_sum(s - 1)
            return 0

        lax.fori_loop(0, SX, far_peer, 0)

        if k > 0:
            for s in range(SY):
                self.msg(YR, k - 1, s).wait_send()

        def near_items(j, _):
            rows = pl.ds(_al(j * 512, 512), 512)
            cols = pl.ds(_al(near, 128), 2 * IB)
            pu[:, pl.ds(_al(j * 512, 128), 512)] = _dot_t(ei[k, :, cols], a[rows, cols])

            @pl.when(j == 0)
            def _():
                chip_sum(SX - 1)
            self.msg(GX, k, j).wait_recv()
            self.msg(GF, k, j).start()
            return 0

        for s in range(SX):
            self.msg(GP, k, s).wait_recv()
        lax.fori_loop(0, 4, near_items, 0)
        for s in range(SX):
            self.msg(GF, k, s).wait_recv()

        def far_items(j, _):
            half = j // 2
            base = half * own_u + (1 - half) * peer_u + (j % 2) * WY
            rows = pl.ds(_al(base, 512), WY)
            cols = pl.ds(_al(far, 128), 2 * IB)
            uc = pl.ds(_al(base, 128), WY)
            pu[:, uc] = pu[:, uc] + _dot_t(ei[k, :, cols], a[rows, cols])

            @pl.when(j < SY)
            def _():
                self.msg(YR, k, j).start()
            return 0

        lax.fori_loop(0, 4, far_items, 0)

        if k > 0:
            for s in range(SX):
                self.msg(FO, k - 1, s).wait_send()

        def near_items_t(s, _):
            e = eu[k]
            c1 = pl.ds(_al(near + (1 - lk.h) * IB + s * WX, 128), WX)
            c2 = pl.ds(_al(near + lk.h * IB + s * WX, 128), WX)
            pi[:, c1] = _dot(e, a[:, c1])
            self.msg(FO, k, s).start()
            pi[:, c2] = _dot(e, a[:, c2])
            return 0

        lax.fori_loop(0, SX, near_items_t, 0)

        for s in range(SY):
            self.msg(YR, k, s).wait_recv()
            uc = pl.ds(_al(own_u + s * WY, 128), WY)
            user_final(k, s, pu[:, uc] + self.ry[k, :, s * WY:(s + 1) * WY])
        for s in range(SX):
            self.msg(FO, k, s).wait_recv()
            self.msg(XR, k, s).wait_recv()
            c2 = pl.ds(_al(near + lk.h * IB + s * WX, 128), WX)
            piece = slice(s * WX, (s + 1) * WX)
            item_final(k, s, (pi[:, c2] + self.ro[k, :, piece]) + self.rx[k, :, piece])

    def finish(self):
        k = STEPS - 1
        for s in range(SX):
            self.msg(FD, k, s).wait_send()
            self.msg(XR, k, s).wait_send()
            self.msg(FO, k, s).wait_send()
        for s in range(SY):
            self.msg(YR, k, s).wait_send()
        for k in range(STEPS):
            self.wait_puts(k)


class AllGather:
    def __init__(self, lk, ref, rows, ss, rs):
        self.lk, self.ref, self.rows, self.ss, self.rs = lk, ref, rows, ss, rs

    def _copy(self, i):
        lk = self.lk
        own = lk.slot
        xs, ys, ds_ = _slot_of(lk.xn), _slot_of(lk.yn), _slot_of(lk.diag)
        src_slot = (own, own, own, own, xs, ys, ds_)[i]
        dev = (lk.partner, lk.xn, lk.yn, lk.diag, lk.partner, lk.partner, lk.partner)[i]
        ref = self.ref.at[src_slot, self.rows]
        return _remote(ref, ref, self.ss.at[i], self.rs.at[i], dev)

    def start(self):
        for i in (1, 2, 0, 3):
            self._copy(i).start()

    def arrive(self, i):
        self._copy(i).wait_recv()
        if i in (1, 2, 3):
            self._copy(i + 3).start()

    def slot(self, i):
        lk = self.lk
        c, x, h = lk.c, lk.x, lk.h
        row = (2 * x + 1 - h, 2 * (1 - x) + h, lk.r, 2 * (1 - x) + h,
               2 * (1 - x) + 1 - h, 2 * x + 1 - h, 2 * (1 - x) + 1 - h)[i]
        col = (c, c, 1 - c, 1 - c, c, 1 - c, 1 - c)[i]
        return row * 2 + col

    def drain(self):
        for i in range(7):
            self._copy(i).wait_send()


ORDER = (0, 1, 2, 4, 5, 3, 6)


def _unpack_t(xt):
    n = xt.shape[1] // 2
    return jnp.concatenate([xt[:, :n], xt[:, n:]], axis=0).T


PROP_SCRATCH = [
    pltpu.VMEM((RU, CI), BF16),
    pltpu.VMEM((STEPS, D, CI), BF16),
    pltpu.VMEM((STEPS, D, RU), BF16),
    pltpu.VMEM((D, CI), F32),
    pltpu.VMEM((D, RU), F32),
    pltpu.VMEM((STEPS, D, IB), F32),
    pltpu.VMEM((STEPS, D, IB), F32),
    pltpu.VMEM((STEPS, D, IB), F32),
    pltpu.VMEM((STEPS, D, UB), F32),
    pltpu.SemaphoreType.DMA((STEPS, 8, 4)),
    pltpu.SemaphoreType.DMA((STEPS, 8, 4)),
]

CH = 64
NBUF = 4
NCH = RU // CH
AW = 8


def forward_kernel(mask, e0u, e0i, out_u, out_i, table, a_hbm,
                   a, ei, eu, pi, pu, rf, ro, rx, ry, ss, rs,
                   mbuf, msem, csum, rpart, dcol, drow, dss, drs, su, si, uacc, iacc, asem, tss, trs, iss, irs):
    lk = Links()

    def mask_copy(j):
        slot = j % NBUF
        return pltpu.make_async_copy(mask.at[pl.ds(_al(j * CH, CH), CH), :], mbuf.at[slot], msem.at[slot])

    for j in range(NBUF):
        mask_copy(j).start()
    lk.barrier()
    pr = Prop(lk, a, ei, eu, pi, pu, rf, ro, rx, ry, ss, rs)

    iacc[...] = e0i[...].astype(F32)
    for s in range(SX):
        pr.put_item(0, s, e0i[:, s * WX:(s + 1) * WX])
    uacc[...] = e0u[...].astype(F32)
    for s in range(SY):
        pr.put_user(0, s, e0u[:, s * WY:(s + 1) * WY])

    csum[...] = jnp.zeros_like(csum)

    def chunk(j, _):
        slot = j % NBUF
        mask_copy(j).wait()
        rows = pl.ds(_al(j * CH, CH), CH)

        def cols_body(w, acc):
            cols = pl.ds(_al(w * 512, 512), 512)
            v = mbuf[slot, :, cols].astype(F32)
            a[rows, cols] = v.astype(BF16)
            csum[:, cols] = csum[:, cols] + jnp.sum(v.reshape(CH // 8, 8, 512), axis=0)
            return acc + ((v[:, 0:128] + v[:, 128:256]) + (v[:, 256:384] + v[:, 384:512]))

        rpart[rows, :] = lax.fori_loop(0, CI // 512, cols_body, jnp.zeros((CH, 128), F32))

        @pl.when(j + NBUF < NCH)
        def _():
            mask_copy(j + NBUF).start()
        return 0

    lax.fori_loop(0, NCH, chunk, 0)

    ctot = jnp.sum(csum[...], axis=0, keepdims=True)
    for j in range(8):
        dcol[0, j:j + 1, :] = ctot[:, j * 1024:(j + 1) * 1024]
    drow[0] = _dot_t(jnp.ones((8, 128), BF16), rpart[...].astype(BF16))
    dcopies = [_remote(dcol.at[0], dcol.at[1 + i], dss.at[i], drs.at[i], dev)
               for i, dev in enumerate((lk.partner, lk.xn, lk.xpartner))]
    dcopies.append(_remote(drow.at[0], drow.at[1], dss.at[3], drs.at[3], lk.yn))
    for cp in dcopies:
        cp.start()
    for cp in dcopies:
        cp.wait_recv()
    ctot8 = (dcol[0] + dcol[1]) + (dcol[2] + dcol[3])
    sc8 = lax.rsqrt(jnp.maximum(ctot8, 1.0))
    for j in range(8):
        si[:, j * 1024:(j + 1) * 1024] = sc8[j:j + 1, :]
    su8 = lax.rsqrt(jnp.maximum(drow[0] + drow[1], 1.0))
    for j in range(RU // 128):
        su[j * 128:(j + 1) * 128, :] = jnp.broadcast_to(su8[0:1, j * 128:(j + 1) * 128], (128, 128)).T

    def a_copy(j):
        rows = pl.ds(_al(j * (RU // AW), RU // AW), RU // AW)
        return pltpu.make_async_copy(a.at[rows, :], a_hbm.at[rows, :], asem.at[j])

    def scale_rows(m, _):
        rows = pl.ds(_al(m * 64, 64), 64)
        s = su[rows, :]
        s4 = jnp.concatenate([s, s, s, s], axis=1)

        def scale_cols(w, _):
            cols = pl.ds(_al(w * 512, 512), 512)
            a[rows, cols] = ((s4 * a[rows, cols].astype(F32)) * si[:, cols]).astype(BF16)
            return 0

        lax.fori_loop(0, CI // 512, scale_cols, 0)
        return 0

    for j in range(AW):
        n = RU // AW // 64
        lax.fori_loop(j * n, (j + 1) * n, scale_rows, 0)
        a_copy(j).start()

    def user_final(k, s, v):
        b = v.astype(BF16)
        if k < STEPS - 1:
            pr.put_user(k + 1, s, b)
        uacc[:, s * WY:(s + 1) * WY] = uacc[:, s * WY:(s + 1) * WY] + b.astype(F32)
        if k == STEPS - 1 and s == SY - 1:
            t = uacc[...] * 0.25
            table[lk.slot, 0:PU, :] = _unpack_t(t).astype(BF16)
            ag_u.start()
            out_u[...] = t.astype(BF16)

    def item_final(k, s, v):
        b = v.astype(BF16)
        if k < STEPS - 1:
            pr.put_item(k + 1, s, b)
        iacc[:, s * WX:(s + 1) * WX] = iacc[:, s * WX:(s + 1) * WX] + b.astype(F32)
        if k == STEPS - 1 and s == SX - 1:
            t = iacc[...] * 0.25
            table[lk.slot, PU:PR, :] = _unpack_t(t).astype(BF16)
            ag_i.start()
            out_i[...] = t.astype(BF16)

    ag_u = AllGather(lk, table, pl.ds(0, PU), tss, trs)
    ag_i = AllGather(lk, table, pl.ds(PU, PI), iss, irs)
    for k in range(STEPS):
        pr.step(k, user_final, item_final)
    for ag in (ag_u, ag_i):
        for i in ORDER:
            ag.arrive(i)
    for cp in dcopies:
        cp.wait_send()
    for j in range(AW):
        a_copy(j).wait()
    pr.finish()
    ag_u.drain()
    ag_i.drain()


def lookup_kernel(table, ru, rp, rn, out, tab, gu, gp, gn):
    def unpack(b, _):
        for lo, n, dst in ((0, PU, 0), (PU, PI, UB)):
            for o in range(0, n, 128):
                v = table[b, lo + o:lo + o + 128, :].astype(F32)
                base = b * (UB + IB) + dst + o
                tab[pl.ds(_al(base, 128), 128), :] = v
                tab[pl.ds(_al(base + n, 128), 128), :] = pltpu.roll(v, D, 1)
        return 0

    lax.fori_loop(0, 8, unpack, 0)

    def gather(g, _):
        for o in range(8):
            t = g * 8 + o
            gu[pl.ds(t, 1), :] = tab[pl.ds(ru[t], 1), :]
            gp[pl.ds(t, 1), :] = tab[pl.ds(rp[t], 1), :]
            gn[pl.ds(t, 1), :] = tab[pl.ds(rn[t], 1), :]
        return 0

    lax.fori_loop(0, TB // 8, gather, 0)

    def block(m, tot):
        rows = pl.ds(_al(m * 128, 128), 128)
        left = lax.broadcasted_iota(jnp.int32, (128, 128), 1) < D
        e_u = gu[rows, :]
        e_d = gp[rows, :] - gn[rows, :]
        x = jnp.sum(jnp.where(left, e_u * e_d, 0.0), axis=1, keepdims=True)
        z = jnp.exp(-jnp.abs(x))
        loss = jnp.maximum(-x, 0.0) + jnp.log1p(z)
        sig = jnp.where(x >= 0.0, z, 1.0) / (1.0 + z)
        coef = sig * (-1.0 / NT)
        out[rows, :] = jnp.where(left, coef * e_d, pltpu.roll(coef * e_u, D, 1))
        return tot + jnp.sum(loss, axis=0, keepdims=True)

    tot = lax.fori_loop(0, TB // 128, block, jnp.zeros((1, 1), F32))
    out[TB:TB + 8, :] = jnp.broadcast_to(tot, (8, 128))


def backward_kernel(a_hbm, g_in, uid, pid, nid, out_u, out_i, out_l,
                    a, ei, eu, pi, pu, rf, ro, rx, ry, ss, rs,
                    asem, g_all, gsem, gss, grs, wu, wi, acc_u, acc_i, su, si):
    lk = Links()
    loads = [pltpu.make_async_copy(a_hbm, a, asem)]
    gcopy = pltpu.make_async_copy(g_in, g_all.at[lk.slot], gsem)
    gcopy.start()
    loads[0].start()
    lk.barrier()
    pr = Prop(lk, a, ei, eu, pi, pu, rf, ro, rx, ry, ss, rs)
    gcopy.wait()
    ag = AllGather(lk, g_all, pl.ds(0, TB + 8), gss, grs)
    ag.start()
    acc_u[...] = jnp.zeros_like(acc_u)
    acc_i[...] = jnp.zeros_like(acc_i)
    base_u = lk.slot * UB
    base_i = (lk.c * 4 + lk.r) * IB

    def scatter(b):
        def split(m, _):
            rows = pl.ds(_al(m * 128, 128), 128)
            left = lax.broadcasted_iota(jnp.int32, (128, 128), 1) < D
            g = g_all[b, rows, :]
            hi = g.astype(BF16).astype(F32)
            r1 = g - hi
            mid = r1.astype(BF16).astype(F32)
            lo = r1 - mid
            wu[rows, 0:128] = jnp.where(left, hi, pltpu.roll(mid, D, 1)).astype(BF16)
            wu[rows, 128:256] = lo.astype(BF16)
            wi[rows, 0:128] = jnp.where(left, pltpu.roll(hi, D, 1), mid).astype(BF16)
            wi[rows, 128:256] = pltpu.roll(lo, D, 1).astype(BF16)
            return 0

        lax.fori_loop(0, TB // 128, split, 0)
        cols = pl.ds(_al(b * TB, 128), TB)

        def users(m, _):
            ids = lax.broadcasted_iota(jnp.int32, (256, TB), 0) + (base_u + m * 256)
            hot = jnp.where(ids == uid[:, cols], 1.0, 0.0).astype(BF16)
            rows = pl.ds(_al(m * 256, 256), 256)
            acc_u[rows, :] = acc_u[rows, :] + _dot(hot, wu[...])
            return 0

        def items(m, _):
            ids = lax.broadcasted_iota(jnp.int32, (256, TB), 0) + (base_i + m * 256)
            hot = (jnp.where(ids == pid[:, cols], 1.0, 0.0) - jnp.where(ids == nid[:, cols], 1.0, 0.0)).astype(BF16)
            rows = pl.ds(_al(m * 256, 256), 256)
            acc_i[rows, :] = acc_i[rows, :] + _dot(hot, wi[...])
            return 0

        lax.fori_loop(0, UB // 256, users, 0)
        lax.fori_loop(0, IB // 256, items, 0)

    scatter(lk.slot)
    for i in ORDER:
        ag.arrive(i)
        scatter(ag.slot(i))

    loss = g_all[0, TB:TB + 8, :]
    for b in range(1, 8):
        loss = loss + g_all[b, TB:TB + 8, :]
    out_l[...] = loss * (1.0 / NT)

    def seed(acc):
        s = (acc[:, 0:128] + pltpu.roll(acc[:, 0:128], D, 1)) + acc[:, 128:256]
        n = s.shape[0] // 2
        s = s * 0.25
        left = lax.broadcasted_iota(jnp.int32, (n, 128), 1) < D
        return jnp.where(left, s[:n], pltpu.roll(s[n:], D, 1)).T

    xi = seed(acc_i[...])
    for s in range(SX):
        src = xi[:D] if s < SX // 2 else xi[D:]
        o = (s % (SX // 2)) * WX
        v = src[:, o:o + WX]
        si[:, s * WX:(s + 1) * WX] = v
        pr.put_item(0, s, v.astype(BF16))
    xu = seed(acc_u[...])
    for s in range(SY):
        v = xu[:D] if s == 0 else xu[D:]
        su[:, s * WY:(s + 1) * WY] = v
        pr.put_user(0, s, v.astype(BF16))

    def user_final(k, s, v):
        v = su[:, s * WY:(s + 1) * WY] + v
        if k < STEPS - 1:
            pr.put_user(k + 1, s, v.astype(BF16))
        else:
            out_u[:, s * WY:(s + 1) * WY] = v

    def item_final(k, s, v):
        v = si[:, s * WX:(s + 1) * WX] + v
        if k < STEPS - 1:
            pr.put_item(k + 1, s, v.astype(BF16))
        else:
            out_i[:, s * WX:(s + 1) * WX] = v

    loads[0].wait()
    for k in range(STEPS):
        pr.step(k, user_final, item_final)
    pr.finish()
    ag.drain()


VM = pl.BlockSpec(memory_space=pltpu.VMEM)
SM = pl.BlockSpec(memory_space=pltpu.SMEM)
ANY = pl.BlockSpec(memory_space=pl.ANY)
DMA = pltpu.SemaphoreType.DMA


def _params(cid):
    return pltpu.CompilerParams(collective_id=cid, has_side_effects=True, vmem_limit_bytes=VMEM_LIMIT)


def solution(mesh):
    def local_fn(mask, e0u, e0i, triples):
        c, r, _, _ = _coords()
        slot = r * 2 + c
        out_u, out_i, table, a_hbm = pl.pallas_call(
            forward_kernel,
            name='forward',
            out_shape=(jax.ShapeDtypeStruct((D, UB), BF16), jax.ShapeDtypeStruct((D, IB), BF16),
                       jax.ShapeDtypeStruct((8, PR, 128), BF16), jax.ShapeDtypeStruct((RU, CI), BF16)),
            in_specs=[ANY, VM, VM],
            out_specs=(VM, VM, VM, ANY),
            scratch_shapes=PROP_SCRATCH + [
                pltpu.VMEM((NBUF, CH, CI), jnp.int32), DMA((NBUF,)),
                pltpu.VMEM((8, CI), F32), pltpu.VMEM((RU, 128), F32),
                pltpu.VMEM((4, 8, 1024), F32), pltpu.VMEM((2, 8, RU), F32), DMA((4,)), DMA((4,)),
                pltpu.VMEM((RU, 128), F32), pltpu.VMEM((1, CI), F32),
                pltpu.VMEM((D, UB), F32), pltpu.VMEM((D, IB), F32), DMA((AW,)),
                DMA((7,)), DMA((7,)), DMA((7,)), DMA((7,)),
            ],
            compiler_params=_params(0),
        )(mask, e0u.T, e0i.T)

        cols = triples.T
        mine = lax.dynamic_slice(cols, (0, slot * TB), (3, TB))
        per = UB + IB
        row_u = (mine[0] // UB) * per + mine[0] % UB
        blk = mine[1:] // IB
        row_i = ((blk % 4) * 2 + blk // 4) * per + UB + mine[1:] % IB
        g = pl.pallas_call(
            lookup_kernel,
            name='lookup',
            out_shape=jax.ShapeDtypeStruct((TB + 8, 128), F32),
            in_specs=[VM, SM, SM, SM],
            out_specs=VM,
            scratch_shapes=[pltpu.VMEM((8 * per, 128), F32)] + [pltpu.VMEM((TB, 128), F32)] * 3,
            compiler_params=pltpu.CompilerParams(vmem_limit_bytes=40 * 1024 * 1024),
        )(table, row_u, row_i[0], row_i[1])

        d_u, d_i, loss = pl.pallas_call(
            backward_kernel,
            name='backward',
            out_shape=(jax.ShapeDtypeStruct((D, UB), F32), jax.ShapeDtypeStruct((D, IB), F32),
                       jax.ShapeDtypeStruct((8, 128), F32)),
            in_specs=[ANY, ANY, VM, VM, VM],
            out_specs=(VM, VM, VM),
            scratch_shapes=PROP_SCRATCH + [
                DMA, pltpu.VMEM((8, TB + 8, 128), F32), DMA, DMA((7,)), DMA((7,)),
                pltpu.VMEM((TB, 256), BF16), pltpu.VMEM((TB, 256), BF16),
                pltpu.VMEM((UB, 256), F32), pltpu.VMEM((IB, 256), F32),
                pltpu.VMEM((D, UB), F32), pltpu.VMEM((D, IB), F32),
            ],
            compiler_params=_params(1),
        )(a_hbm, g, cols[0:1], cols[1:2], cols[2:3])
        return out_u.T, out_i.T, loss[0, 0], d_u.T, d_i.T

    user_spec = P(('row', 'col'), None)
    item_spec = P(('col', 'row'), None)
    return jax.shard_map(local_fn, mesh=mesh, in_specs=(P('row', 'col'), user_spec, item_spec, P()),
                         out_specs=(user_spec, item_spec, P(), user_spec, item_spec), check_vma=False)
```

```python
import jax
import jax.numpy as jnp
from jax import lax
from jax.experimental import pallas as pl
from jax.experimental.pallas import tpu as pltpu
from jax.sharding import PartitionSpec as P

MESH = pl.DeviceIdType.MESH
F32 = jnp.float32
BF16 = jnp.bfloat16

D = 64
UB = 1024
IB = 2048
RU = 2048
CI = 8192
STEPS = 3
SX = 4
WX = IB // SX
SY = 2
WY = UB // SY
TB = 1024
NT = 8192
PU = UB // 2
PI = IB // 2
PR = PU + PI

FD, XR, FO, GP, GX, GF, YR, YG = range(8)
VMEM_LIMIT = 67043328


def _coords():
    c = lax.axis_index('col')
    r = lax.axis_index('row')
    x = r // 2
    h = r % 2
    return c, r, x, h


def _dot(a, b):
    return lax.dot_general(a, b, (((1,), (0,)), ((), ())), preferred_element_type=F32)


def _dot_t(a, b):
    return lax.dot_general(a, b, (((1,), (1,)), ((), ())), preferred_element_type=F32)


def _al(v, m):
    return pl.multiple_of(v, m)


class Links:
    def __init__(self):
        self.c, self.r, self.x, self.h = _coords()
        c, r, x, h = self.c, self.r, self.x, self.h
        self.partner = (c, 2 * x + (1 - h))
        self.xn = (c, 2 * (1 - x) + h)
        self.yn = (1 - c, r)
        self.diag = (1 - c, 2 * (1 - x) + h)
        self.xpartner = (c, 2 * (1 - x) + (1 - h))
        self.slot = r * 2 + c

    def barrier(self):
        sem = pltpu.get_barrier_semaphore()
        peers = (self.partner, self.xn, self.yn, self.diag, self.xpartner)
        for p in peers:
            pl.semaphore_signal(sem, inc=1, device_id=p, device_id_type=MESH)
        pl.semaphore_wait(sem, len(peers))


def _slot_of(dev):
    return dev[1] * 2 + dev[0]


def _remote(src, dst, ss, rs, dev):
    return pltpu.make_async_remote_copy(src_ref=src, dst_ref=dst, send_sem=ss, recv_sem=rs, device_id=dev, device_id_type=MESH)


class Prop:
    def __init__(self, lk, a, ei, eu, pi, pu, rf, ro, rx, ry, ss, rs):
        self.lk = lk
        self.a, self.ei, self.eu, self.pi, self.pu = a, ei, eu, pi, pu
        self.rf, self.ro, self.rx, self.ry = rf, ro, rx, ry
        self.ss, self.rs = ss, rs

    def msg(self, kind, k, s):
        lk = self.lk
        ss, rs = self.ss.at[k, kind, s], self.rs.at[k, kind, s]
        other = 1 - lk.x
        if kind == FD:
            src = self.pi.at[:, pl.ds(_al((2 * other + 1 - lk.h) * IB + s * WX, 128), WX)]
            dst = self.rf.at[k, :, pl.ds(_al(s * WX, 128), WX)]
            return _remote(src, dst, ss, rs, lk.partner)
        if kind == XR:
            src = self.pi.at[:, pl.ds(_al((2 * other + lk.h) * IB + s * WX, 128), WX)]
            dst = self.rx.at[k, :, pl.ds(_al(s * WX, 128), WX)]
            return _remote(src, dst, ss, rs, lk.xn)
        if kind == FO:
            src = self.pi.at[:, pl.ds(_al((2 * lk.x + 1 - lk.h) * IB + s * WX, 128), WX)]
            dst = self.ro.at[k, :, pl.ds(_al(s * WX, 128), WX)]
            return _remote(src, dst, ss, rs, lk.partner)
        if kind in (GP, GX):
            ref = self.ei.at[k, :, pl.ds(_al(lk.r * IB + s * WX, 128), WX)]
            return _remote(ref, ref, ss, rs, lk.partner if kind == GP else lk.xn)
        if kind == GF:
            ref = self.ei.at[k, :, pl.ds(_al((2 * other + lk.h) * IB + s * WX, 128), WX)]
            return _remote(ref, ref, ss, rs, lk.partner)
        if kind == YR:
            src = self.pu.at[:, pl.ds(_al((1 - lk.c) * UB + s * WY, 128), WY)]
            dst = self.ry.at[k, :, pl.ds(_al(s * WY, 128), WY)]
            return _remote(src, dst, ss, rs, lk.yn)
        ref = self.eu.at[k, :, pl.ds(_al(lk.c * UB + s * WY, 128), WY)]
        return _remote(ref, ref, ss, rs, lk.yn)

    def put_item(self, k, s, value):
        self.ei[k, :, pl.ds(_al(self.lk.r * IB + s * WX, 128), WX)] = value
        self.msg(GX, k, s).start()
        self.msg(GP, k, s).start()

    def put_user(self, k, s, value):
        self.eu[k, :, pl.ds(_al(self.lk.c * UB + s * WY, 128), WY)] = value
        self.msg(YG, k, s).start()

    def wait_puts(self, k):
        for s in range(SX):
            self.msg(GX, k, s).wait_send()
            self.msg(GP, k, s).wait_send()
            if k == STEPS - 1:
                self.msg(GF, k, s).wait_send()
        for s in range(SY):
            self.msg(YG, k, s).wait_send()

    def step(self, k, user_final, item_final, between=None):
        lk = self.lk
        a, ei, eu, pi, pu = self.a, self.ei, self.eu, self.pi, self.pu
        far = (1 - lk.x) * 2 * IB
        near = lk.x * 2 * IB
        own_u = lk.c * UB
        peer_u = (1 - lk.c) * UB

        def far_cols(piece, half):
            return _al(far + half * IB + piece * 1024, 128)

        if k > 0:
            for s in range(SX):
                self.msg(FD, k - 1, s).wait_send()
                self.msg(XR, k - 1, s).wait_send()
                self.msg(GF, k - 1, s).wait_send()

        def far_own(j, _):
            cols = pl.ds(_al(far + j * 1024, 128), 1024)
            pi[:, cols] = _dot(eu[k, :, pl.ds(_al(own_u, 128), UB)], a[pl.ds(_al(own_u, 128), UB), cols])
            return 0

        lax.fori_loop(0, 4, far_own, 0)
        for s in range(SY):
            self.msg(YG, k, s).wait_recv()

        def far_peer(j, _):
            e = eu[k, :, pl.ds(_al(peer_u, 128), UB)]
            rows = pl.ds(_al(peer_u, 128), UB)
            first = j < 2
            half = jnp.where(first, 1 - lk.h, lk.h)
            p = j % 2
            cols = pl.ds(far_cols(p, half), 1024)
            pi[:, cols] = pi[:, cols] + _dot(e, a[rows, cols])

            @pl.when(first)
            def _():
                for q in range(2):
                    self.msg(FD, k, 2 * p + q).start()

            @pl.when(j >= 2)
            def _():
                for q in range(2):
                    s = 2 * p + q
                    self.msg(FD, k, s).wait_recv()
                    cs = pl.ds(_al(far + lk.h * IB + s * WX, 128), WX)
                    pi[:, cs] = pi[:, cs] + self.rf[k, :, pl.ds(_al(s * WX, 128), WX)]
                    self.msg(XR, k, s).start()
            return 0

        lax.fori_loop(0, 4, far_peer, 0)
        if between is not None:
            between()

        if k > 0:
            for s in range(SX):
                self.msg(FO, k - 1, s).wait_send()

        def near_items_t(s, _):
            e = eu[k]
            c1 = pl.ds(_al(near + (1 - lk.h) * IB + s * WX, 128), WX)
            c2 = pl.ds(_al(near + lk.h * IB + s * WX, 128), WX)
            pi[:, c1] = _dot(e, a[:, c1])
            self.msg(FO, k, s).start()
            pi[:, c2] = _dot(e, a[:, c2])
            self.msg(GX, k, s).wait_recv()
            self.msg(GF, k, s).start()
            return 0

        lax.fori_loop(0, SX, near_items_t, 0)

        if k > 0:
            for s in range(SY):
                self.msg(YR, k - 1, s).wait_send()
        for s in range(SX):
            self.msg(GP, k, s).wait_recv()

        def item_piece(s):
            self.msg(FO, k, s).wait_recv()
            self.msg(XR, k, s).wait_recv()
            c2 = pl.ds(_al(near + lk.h * IB + s * WX, 128), WX)
            piece = pl.ds(_al(s * WX, 128), WX)
            item_final(k, s, (pi[:, c2] + self.ro[k, :, piece]) + self.rx[k, :, piece])

        def user_piece(s):
            self.msg(YR, k, s).wait_recv()
            uc = pl.ds(_al(own_u + s * WY, 128), WY)
            user_final(k, s, pu[:, uc] + self.ry[k, :, s * WY:(s + 1) * WY])

        def users_tile(t, _):
            u = t // 2
            is_far = t % 2
            own = u // 2
            base = own * own_u + (1 - own) * peer_u + (u % 2) * WY
            at = is_far * far + (1 - is_far) * near
            rows = pl.ds(_al(base, 512), WY)
            uc = pl.ds(_al(base, 128), WY)
            cols = pl.ds(_al(at, 128), 2 * IB)
            v = _dot_t(ei[k, :, cols], a[rows, cols])

            @pl.when(is_far == 0)
            def _():
                pu[:, uc] = v

            @pl.when(t == 0)
            def _():
                for s in range(SX):
                    self.msg(GF, k, s).wait_recv()

            @pl.when(is_far == 1)
            def _():
                pu[:, uc] = pu[:, uc] + v

            @pl.when(t == 1)
            def _():
                self.msg(YR, k, 0).start()

            @pl.when(t == 2)
            def _():
                item_piece(0)

            @pl.when(t == 3)
            def _():
                self.msg(YR, k, 1).start()

            @pl.when(t == 4)
            def _():
                item_piece(1)

            @pl.when(t == 6)
            def _():
                user_piece(0)
                item_piece(2)
            return 0

        lax.fori_loop(0, 8, users_tile, 0)
        user_piece(1)
        item_piece(3)

    def finish(self):
        k = STEPS - 1
        for s in range(SX):
            self.msg(FD, k, s).wait_send()
            self.msg(XR, k, s).wait_send()
            self.msg(FO, k, s).wait_send()
        for s in range(SY):
            self.msg(YR, k, s).wait_send()
        for k in range(STEPS):
            self.wait_puts(k)


class AllGather:
    def __init__(self, lk, ref, rows, ss, rs):
        self.lk, self.ref, self.rows, self.ss, self.rs = lk, ref, rows, ss, rs

    def _copy(self, i):
        lk = self.lk
        own = lk.slot
        xs, ys, ds_ = _slot_of(lk.xn), _slot_of(lk.yn), _slot_of(lk.diag)
        src_slot = (own, own, own, own, xs, ys, ds_)[i]
        dev = (lk.partner, lk.xn, lk.yn, lk.diag, lk.partner, lk.partner, lk.partner)[i]
        ref = self.ref.at[src_slot, self.rows]
        return _remote(ref, ref, self.ss.at[i], self.rs.at[i], dev)

    def start(self):
        for i in (1, 2, 0, 3):
            self._copy(i).start()

    def arrive(self, i):
        self._copy(i).wait_recv()
        if i in (1, 2, 3):
            self._copy(i + 3).start()

    def slot(self, i):
        lk = self.lk
        c, x, h = lk.c, lk.x, lk.h
        row = (2 * x + 1 - h, 2 * (1 - x) + h, lk.r, 2 * (1 - x) + h,
               2 * (1 - x) + 1 - h, 2 * x + 1 - h, 2 * (1 - x) + 1 - h)[i]
        col = (c, c, 1 - c, 1 - c, c, 1 - c, 1 - c)[i]
        return row * 2 + col

    def drain(self):
        for i in range(7):
            self._copy(i).wait_send()


ORDER = (0, 1, 2, 4, 5, 3, 6)


def _unpack_t(xt):
    n = xt.shape[1] // 2
    return jnp.concatenate([xt[:, :n], xt[:, n:]], axis=0).T


PROP_SCRATCH = [
    pltpu.VMEM((RU, CI), BF16),
    pltpu.VMEM((STEPS, D, CI), BF16),
    pltpu.VMEM((STEPS, D, RU), BF16),
    pltpu.VMEM((D, CI), F32),
    pltpu.VMEM((D, RU), F32),
    pltpu.VMEM((STEPS, D, IB), F32),
    pltpu.VMEM((STEPS, D, IB), F32),
    pltpu.VMEM((STEPS, D, IB), F32),
    pltpu.VMEM((STEPS, D, UB), F32),
    pltpu.SemaphoreType.DMA((STEPS, 8, 4)),
    pltpu.SemaphoreType.DMA((STEPS, 8, 4)),
]

CH = 64
NBUF = 4
NCH = RU // CH
AW = 8


def forward_kernel(mask, e0u, e0i, out_u, out_i, table, a_hbm,
                   a, ei, eu, pi, pu, rf, ro, rx, ry, ss, rs,
                   mbuf, msem, csum, rpart, dcol, drow, dss, drs, su, si, uacc, iacc, asem, tss, trs, iss, irs):
    lk = Links()

    def mask_copy(j):
        slot = j % NBUF
        return pltpu.make_async_copy(mask.at[pl.ds(_al(j * CH, CH), CH), :], mbuf.at[slot], msem.at[slot])

    for j in range(NBUF):
        mask_copy(j).start()
    lk.barrier()
    pr = Prop(lk, a, ei, eu, pi, pu, rf, ro, rx, ry, ss, rs)

    iacc[...] = e0i[...].astype(F32)
    for s in range(SX):
        pr.put_item(0, s, e0i[:, s * WX:(s + 1) * WX])
    uacc[...] = e0u[...].astype(F32)
    for s in range(SY):
        pr.put_user(0, s, e0u[:, s * WY:(s + 1) * WY])

    csum[...] = jnp.zeros_like(csum)

    def chunk(j, _):
        slot = j % NBUF
        mask_copy(j).wait()
        rows = pl.ds(_al(j * CH, CH), CH)

        def cols_body(w, acc):
            cols = pl.ds(_al(w * 512, 512), 512)
            v = mbuf[slot, :, cols].astype(F32)
            a[rows, cols] = v.astype(BF16)
            csum[:, cols] = csum[:, cols] + jnp.sum(v.reshape(CH // 8, 8, 512), axis=0)
            return acc + ((v[:, 0:128] + v[:, 128:256]) + (v[:, 256:384] + v[:, 384:512]))

        rpart[rows, :] = lax.fori_loop(0, CI // 512, cols_body, jnp.zeros((CH, 128), F32))

        @pl.when(j + NBUF < NCH)
        def _():
            mask_copy(j + NBUF).start()
        return 0

    lax.fori_loop(0, NCH, chunk, 0)

    ctot = jnp.sum(csum[...], axis=0, keepdims=True)
    for j in range(8):
        dcol[0, j:j + 1, :] = ctot[:, j * 1024:(j + 1) * 1024]
    drow[0] = _dot_t(jnp.ones((8, 128), BF16), rpart[...].astype(BF16))
    dcopies = [_remote(dcol.at[0], dcol.at[1 + i], dss.at[i], drs.at[i], dev)
               for i, dev in enumerate((lk.partner, lk.xn, lk.xpartner))]
    dcopies.append(_remote(drow.at[0], drow.at[1], dss.at[3], drs.at[3], lk.yn))
    for cp in dcopies:
        cp.start()
    for cp in dcopies:
        cp.wait_recv()
    ctot8 = (dcol[0] + dcol[1]) + (dcol[2] + dcol[3])
    sc8 = lax.rsqrt(jnp.maximum(ctot8, 1.0))
    for j in range(8):
        si[:, j * 1024:(j + 1) * 1024] = sc8[j:j + 1, :]
    su8 = lax.rsqrt(jnp.maximum(drow[0] + drow[1], 1.0))
    for j in range(RU // 128):
        su[j * 128:(j + 1) * 128, :] = jnp.broadcast_to(su8[0:1, j * 128:(j + 1) * 128], (128, 128)).T

    def a_copy(j):
        rows = pl.ds(_al(j * (RU // AW), RU // AW), RU // AW)
        return pltpu.make_async_copy(a.at[rows, :], a_hbm.at[rows, :], asem.at[j])

    def scale(first_col):
        def scale_rows(m, _):
            rows = pl.ds(_al(m * 64, 64), 64)
            s = su[rows, :]
            s4 = jnp.concatenate([s, s, s, s], axis=1)

            def scale_cols(w, _):
                cols = pl.ds(_al(first_col + w * 512, 512), 512)
                a[rows, cols] = a[rows, cols] * (s4 * si[:, cols]).astype(BF16)
                return 0

            lax.fori_loop(0, CI // 1024, scale_cols, 0)
            return 0

        lax.fori_loop(0, RU // 64, scale_rows, 0)

    def scale_near():
        scale(lk.x * 2 * IB)
        for j in range(AW):
            a_copy(j).start()

    scale((1 - lk.x) * 2 * IB)

    def user_final(k, s, v):
        b = v.astype(BF16)
        if k < STEPS - 1:
            pr.put_user(k + 1, s, b)
        uacc[:, s * WY:(s + 1) * WY] = uacc[:, s * WY:(s + 1) * WY] + b.astype(F32)
        if k == STEPS - 1 and s == SY - 1:
            t = uacc[...] * 0.25
            table[lk.slot, 0:PU, :] = _unpack_t(t).astype(BF16)
            ag_u.start()
            out_u[...] = t.astype(BF16)

    def item_final(k, s, v):
        b = v.astype(BF16)
        if k < STEPS - 1:
            pr.put_item(k + 1, s, b)
        iacc[:, s * WX:(s + 1) * WX] = iacc[:, s * WX:(s + 1) * WX] + b.astype(F32)
        if k == STEPS - 1 and s == SX - 1:
            t = iacc[...] * 0.25
            table[lk.slot, PU:PR, :] = _unpack_t(t).astype(BF16)
            ag_i.start()
            out_i[...] = t.astype(BF16)

    ag_u = AllGather(lk, table, pl.ds(0, PU), tss, trs)
    ag_i = AllGather(lk, table, pl.ds(PU, PI), iss, irs)
    for k in range(STEPS):
        pr.step(k, user_final, item_final, scale_near if k == 0 else None)
    for ag in (ag_u, ag_i):
        for i in ORDER:
            ag.arrive(i)
    for cp in dcopies:
        cp.wait_send()
    for j in range(AW):
        a_copy(j).wait()
    pr.finish()
    ag_u.drain()
    ag_i.drain()


def lookup_kernel(table, ru, rp, rn, out, tab, gu, gp, gn):
    def unpack(b, _):
        for lo, n, dst in ((0, PU, 0), (PU, PI, UB)):
            for o in range(0, n, 128):
                v = table[b, lo + o:lo + o + 128, :].astype(F32)
                base = b * (UB + IB) + dst + o
                tab[pl.ds(_al(base, 128), 128), :] = v
                tab[pl.ds(_al(base + n, 128), 128), :] = pltpu.roll(v, D, 1)
        return 0

    lax.fori_loop(0, 8, unpack, 0)

    def gather(g, _):
        for o in range(8):
            t = g * 8 + o
            gu[pl.ds(t, 1), :] = tab[pl.ds(ru[t], 1), :]
            gp[pl.ds(t, 1), :] = tab[pl.ds(rp[t], 1), :]
            gn[pl.ds(t, 1), :] = tab[pl.ds(rn[t], 1), :]
        return 0

    lax.fori_loop(0, TB // 8, gather, 0)

    def block(m, tot):
        rows = pl.ds(_al(m * 128, 128), 128)
        left = lax.broadcasted_iota(jnp.int32, (128, 128), 1) < D
        e_u = gu[rows, :]
        e_d = gp[rows, :] - gn[rows, :]
        x = jnp.sum(jnp.where(left, e_u * e_d, 0.0), axis=1, keepdims=True)
        z = jnp.exp(-jnp.abs(x))
        loss = jnp.maximum(-x, 0.0) + jnp.log1p(z)
        sig = jnp.where(x >= 0.0, z, 1.0) / (1.0 + z)
        coef = sig * (-1.0 / NT)
        out[rows, :] = jnp.where(left, coef * e_d, pltpu.roll(coef * e_u, D, 1))
        return tot + jnp.sum(loss, axis=0, keepdims=True)

    tot = lax.fori_loop(0, TB // 128, block, jnp.zeros((1, 1), F32))
    out[TB:TB + 8, :] = jnp.broadcast_to(tot, (8, 128))


def backward_kernel(a_hbm, g_in, uid, pid, nid, out_u, out_i, out_l,
                    a, ei, eu, pi, pu, rf, ro, rx, ry, ss, rs,
                    asem, g_all, gsem, gss, grs, wu, wi, acc_u, acc_i, su, si):
    lk = Links()
    loads = [pltpu.make_async_copy(a_hbm, a, asem)]
    gcopy = pltpu.make_async_copy(g_in, g_all.at[lk.slot], gsem)
    gcopy.start()
    loads[0].start()
    lk.barrier()
    pr = Prop(lk, a, ei, eu, pi, pu, rf, ro, rx, ry, ss, rs)
    gcopy.wait()
    ag = AllGather(lk, g_all, pl.ds(0, TB + 8), gss, grs)
    ag.start()
    acc_u[...] = jnp.zeros_like(acc_u)
    acc_i[...] = jnp.zeros_like(acc_i)
    base_u = lk.slot * UB
    base_i = (lk.c * 4 + lk.r) * IB

    def scatter(b):
        def split(m, _):
            rows = pl.ds(_al(m * 128, 128), 128)
            left = lax.broadcasted_iota(jnp.int32, (128, 128), 1) < D
            g = g_all[b, rows, :]
            hi = g.astype(BF16).astype(F32)
            r1 = g - hi
            mid = r1.astype(BF16).astype(F32)
            lo = r1 - mid
            wu[rows, 0:128] = jnp.where(left, hi, pltpu.roll(mid, D, 1)).astype(BF16)
            wu[rows, 128:256] = lo.astype(BF16)
            wi[rows, 0:128] = jnp.where(left, pltpu.roll(hi, D, 1), mid).astype(BF16)
            wi[rows, 128:256] = pltpu.roll(lo, D, 1).astype(BF16)
            return 0

        lax.fori_loop(0, TB // 128, split, 0)
        cols = pl.ds(_al(b * TB, 128), TB)
        sub = lax.broadcasted_iota(jnp.int32, (256, TB), 0).astype(F32).astype(BF16)
        one, zero = jnp.array(1.0, BF16), jnp.array(0.0, BF16)

        def lanes(ids, base):
            v = ids[:, cols] - base
            v = jnp.where((v >= 0) & (v < 256), v, -1).astype(F32)
            return jnp.broadcast_to(v, (256, TB)).astype(BF16)

        def users(m, _):
            hot = jnp.where(lanes(uid, base_u + m * 256) == sub, one, zero)
            rows = pl.ds(_al(m * 256, 256), 256)
            acc_u[rows, :] = acc_u[rows, :] + _dot(hot, wu[...])
            return 0

        def items(m, _):
            hot_p = jnp.where(lanes(pid, base_i + m * 256) == sub, one, zero)
            hot = hot_p - jnp.where(lanes(nid, base_i + m * 256) == sub, one, zero)
            rows = pl.ds(_al(m * 256, 256), 256)
            acc_i[rows, :] = acc_i[rows, :] + _dot(hot, wi[...])
            return 0

        lax.fori_loop(0, UB // 256, users, 0)
        lax.fori_loop(0, IB // 256, items, 0)

    scatter(lk.slot)
    for i in ORDER:
        ag.arrive(i)
        scatter(ag.slot(i))

    loss = g_all[0, TB:TB + 8, :]
    for b in range(1, 8):
        loss = loss + g_all[b, TB:TB + 8, :]
    out_l[...] = loss * (1.0 / NT)

    def seed(acc):
        s = (acc[:, 0:128] + pltpu.roll(acc[:, 0:128], D, 1)) + acc[:, 128:256]
        n = s.shape[0] // 2
        s = s * 0.25
        left = lax.broadcasted_iota(jnp.int32, (n, 128), 1) < D
        return jnp.where(left, s[:n], pltpu.roll(s[n:], D, 1)).T

    xi = seed(acc_i[...])
    for s in range(SX):
        src = xi[:D] if s < SX // 2 else xi[D:]
        o = (s % (SX // 2)) * WX
        v = src[:, o:o + WX]
        si[:, s * WX:(s + 1) * WX] = v
        pr.put_item(0, s, v.astype(BF16))
    xu = seed(acc_u[...])
    for s in range(SY):
        v = xu[:D] if s == 0 else xu[D:]
        su[:, s * WY:(s + 1) * WY] = v
        pr.put_user(0, s, v.astype(BF16))

    def user_final(k, s, v):
        v = su[:, s * WY:(s + 1) * WY] + v
        if k < STEPS - 1:
            pr.put_user(k + 1, s, v.astype(BF16))
        else:
            out_u[:, s * WY:(s + 1) * WY] = v

    def item_final(k, s, v):
        v = si[:, s * WX:(s + 1) * WX] + v
        if k < STEPS - 1:
            pr.put_item(k + 1, s, v.astype(BF16))
        else:
            out_i[:, s * WX:(s + 1) * WX] = v

    loads[0].wait()
    for k in range(STEPS):
        pr.step(k, user_final, item_final)
    pr.finish()
    ag.drain()


VM = pl.BlockSpec(memory_space=pltpu.VMEM)
SM = pl.BlockSpec(memory_space=pltpu.SMEM)
ANY = pl.BlockSpec(memory_space=pl.ANY)
DMA = pltpu.SemaphoreType.DMA


def _params(cid):
    return pltpu.CompilerParams(collective_id=cid, has_side_effects=True, vmem_limit_bytes=VMEM_LIMIT)


def solution(mesh):
    def local_fn(mask, e0u, e0i, triples):
        c, r, _, _ = _coords()
        slot = r * 2 + c
        out_u, out_i, table, a_hbm = pl.pallas_call(
            forward_kernel,
            name='forward',
            out_shape=(jax.ShapeDtypeStruct((D, UB), BF16), jax.ShapeDtypeStruct((D, IB), BF16),
                       jax.ShapeDtypeStruct((8, PR, 128), BF16), jax.ShapeDtypeStruct((RU, CI), BF16)),
            in_specs=[ANY, VM, VM],
            out_specs=(VM, VM, VM, ANY),
            scratch_shapes=PROP_SCRATCH + [
                pltpu.VMEM((NBUF, CH, CI), jnp.int32), DMA((NBUF,)),
                pltpu.VMEM((8, CI), F32), pltpu.VMEM((RU, 128), F32),
                pltpu.VMEM((4, 8, 1024), F32), pltpu.VMEM((2, 8, RU), F32), DMA((4,)), DMA((4,)),
                pltpu.VMEM((RU, 128), F32), pltpu.VMEM((1, CI), F32),
                pltpu.VMEM((D, UB), F32), pltpu.VMEM((D, IB), F32), DMA((AW,)),
                DMA((7,)), DMA((7,)), DMA((7,)), DMA((7,)),
            ],
            compiler_params=_params(0),
        )(mask, e0u.T, e0i.T)

        cols = triples.T
        mine = lax.dynamic_slice(cols, (0, slot * TB), (3, TB))
        per = UB + IB
        row_u = (mine[0] // UB) * per + mine[0] % UB
        blk = mine[1:] // IB
        row_i = ((blk % 4) * 2 + blk // 4) * per + UB + mine[1:] % IB
        g = pl.pallas_call(
            lookup_kernel,
            name='lookup',
            out_shape=jax.ShapeDtypeStruct((TB + 8, 128), F32),
            in_specs=[VM, SM, SM, SM],
            out_specs=VM,
            scratch_shapes=[pltpu.VMEM((8 * per, 128), F32)] + [pltpu.VMEM((TB, 128), F32)] * 3,
            compiler_params=pltpu.CompilerParams(vmem_limit_bytes=40 * 1024 * 1024),
        )(table, row_u, row_i[0], row_i[1])

        d_u, d_i, loss = pl.pallas_call(
            backward_kernel,
            name='backward',
            out_shape=(jax.ShapeDtypeStruct((D, UB), F32), jax.ShapeDtypeStruct((D, IB), F32),
                       jax.ShapeDtypeStruct((8, 128), F32)),
            in_specs=[ANY, ANY, VM, VM, VM],
            out_specs=(VM, VM, VM),
            scratch_shapes=PROP_SCRATCH + [
                DMA, pltpu.VMEM((8, TB + 8, 128), F32), DMA, DMA((7,)), DMA((7,)),
                pltpu.VMEM((TB, 256), BF16), pltpu.VMEM((TB, 256), BF16),
                pltpu.VMEM((UB, 256), F32), pltpu.VMEM((IB, 256), F32),
                pltpu.VMEM((D, UB), F32), pltpu.VMEM((D, IB), F32),
            ],
            compiler_params=_params(1),
        )(a_hbm, g, cols[0:1], cols[1:2], cols[2:3])
        return out_u.T, out_i.T, loss[0, 0], d_u.T, d_i.T

    user_spec = P(('row', 'col'), None)
    item_spec = P(('col', 'row'), None)
    return jax.shard_map(local_fn, mesh=mesh, in_specs=(P('row', 'col'), user_spec, item_spec, P()),
                         out_specs=(user_spec, item_spec, P(), user_spec, item_spec), check_vma=False)
```

```python
import jax
import jax.numpy as jnp
from jax import lax
from jax.experimental import pallas as pl
from jax.experimental.pallas import tpu as pltpu
from jax.sharding import PartitionSpec as P

MESH = pl.DeviceIdType.MESH
F32 = jnp.float32
BF16 = jnp.bfloat16

D = 64
UB = 1024
IB = 2048
RU = 2048
CI = 8192
STEPS = 3
SX = 4
WX = IB // SX
SY = 2
WY = UB // SY
TB = 1024
NT = 8192
PU = UB // 2
PI = IB // 2
PR = PU + PI

FD, XR, FO, GP, GX, GF, YR, YG = range(8)
VMEM_LIMIT = 67043328


def _coords():
    c = lax.axis_index('col')
    r = lax.axis_index('row')
    x = r // 2
    h = r % 2
    return c, r, x, h


def _dot(a, b):
    return lax.dot_general(a, b, (((1,), (0,)), ((), ())), preferred_element_type=F32)


def _dot_t(a, b):
    return lax.dot_general(a, b, (((1,), (1,)), ((), ())), preferred_element_type=F32)


def _al(v, m):
    return pl.multiple_of(v, m)


class Links:
    def __init__(self):
        self.c, self.r, self.x, self.h = _coords()
        c, r, x, h = self.c, self.r, self.x, self.h
        self.partner = (c, 2 * x + (1 - h))
        self.xn = (c, 2 * (1 - x) + h)
        self.yn = (1 - c, r)
        self.diag = (1 - c, 2 * (1 - x) + h)
        self.xpartner = (c, 2 * (1 - x) + (1 - h))
        self.slot = r * 2 + c

    def barrier(self):
        sem = pltpu.get_barrier_semaphore()
        peers = (self.partner, self.xn, self.yn, self.diag, self.xpartner)
        for p in peers:
            pl.semaphore_signal(sem, inc=1, device_id=p, device_id_type=MESH)
        pl.semaphore_wait(sem, len(peers))


def _slot_of(dev):
    return dev[1] * 2 + dev[0]


def _remote(src, dst, ss, rs, dev):
    return pltpu.make_async_remote_copy(src_ref=src, dst_ref=dst, send_sem=ss, recv_sem=rs, device_id=dev, device_id_type=MESH)


class Prop:
    def __init__(self, lk, a, ei, eu, pi, pu, rf, ro, rx, ry, ss, rs):
        self.lk = lk
        self.a, self.ei, self.eu, self.pi, self.pu = a, ei, eu, pi, pu
        self.rf, self.ro, self.rx, self.ry = rf, ro, rx, ry
        self.ss, self.rs = ss, rs

    def msg(self, kind, k, s):
        lk = self.lk
        ss, rs = self.ss.at[k, kind, s], self.rs.at[k, kind, s]
        other = 1 - lk.x
        if kind == FD:
            src = self.pi.at[:, pl.ds(_al((2 * other + 1 - lk.h) * IB + s * WX, 128), WX)]
            dst = self.rf.at[k, :, pl.ds(_al(s * WX, 128), WX)]
            return _remote(src, dst, ss, rs, lk.partner)
        if kind == XR:
            src = self.pi.at[:, pl.ds(_al((2 * other + lk.h) * IB + s * WX, 128), WX)]
            dst = self.rx.at[k, :, pl.ds(_al(s * WX, 128), WX)]
            return _remote(src, dst, ss, rs, lk.xn)
        if kind == FO:
            src = self.pi.at[:, pl.ds(_al((2 * lk.x + 1 - lk.h) * IB + s * WX, 128), WX)]
            dst = self.ro.at[k, :, pl.ds(_al(s * WX, 128), WX)]
            return _remote(src, dst, ss, rs, lk.partner)
        if kind in (GP, GX):
            ref = self.ei.at[k, :, pl.ds(_al(lk.r * IB + s * WX, 128), WX)]
            return _remote(ref, ref, ss, rs, lk.partner if kind == GP else lk.xn)
        if kind == GF:
            ref = self.ei.at[k, :, pl.ds(_al((2 * other + lk.h) * IB + s * WX, 128), WX)]
            return _remote(ref, ref, ss, rs, lk.partner)
        if kind == YR:
            src = self.pu.at[:, pl.ds(_al((1 - lk.c) * UB + s * WY, 128), WY)]
            dst = self.ry.at[k, :, pl.ds(_al(s * WY, 128), WY)]
            return _remote(src, dst, ss, rs, lk.yn)
        ref = self.eu.at[k, :, pl.ds(_al(lk.c * UB + s * WY, 128), WY)]
        return _remote(ref, ref, ss, rs, lk.yn)

    def put_item(self, k, s, value):
        self.ei[k, :, pl.ds(_al(self.lk.r * IB + s * WX, 128), WX)] = value
        self.msg(GX, k, s).start()
        self.msg(GP, k, s).start()

    def put_user(self, k, s, value):
        self.eu[k, :, pl.ds(_al(self.lk.c * UB + s * WY, 128), WY)] = value
        self.msg(YG, k, s).start()

    def wait_puts(self, k):
        for s in range(SX):
            self.msg(GX, k, s).wait_send()
            self.msg(GP, k, s).wait_send()
            if k == STEPS - 1:
                self.msg(GF, k, s).wait_send()
        for s in range(SY):
            self.msg(YG, k, s).wait_send()

    def step(self, k, user_final, item_final, between=None):
        lk = self.lk
        a, ei, eu, pi, pu = self.a, self.ei, self.eu, self.pi, self.pu
        far = (1 - lk.x) * 2 * IB
        near = lk.x * 2 * IB
        own_u = lk.c * UB
        peer_u = (1 - lk.c) * UB

        if k > 0:
            for s in range(SX):
                self.msg(FD, k - 1, s).wait_send()
                self.msg(XR, k - 1, s).wait_send()
                self.msg(FO, k - 1, s).wait_send()
                self.msg(GF, k - 1, s).wait_send()
        own_rows = pl.ds(_al(own_u, 128), UB)
        peer_rows = pl.ds(_al(peer_u, 128), UB)

        def over_own(first_col):
            def body(j, _):
                cols = pl.ds(_al(first_col + j * 1024, 128), 1024)
                pi[:, cols] = _dot(eu[k, :, own_rows], a[own_rows, cols])
                return 0

            lax.fori_loop(0, 4, body, 0)

        over_own(far)
        if between is not None:
            between()
        over_own(near)
        for s in range(SY):
            self.msg(YG, k, s).wait_recv()

        def over_peer(j, _):
            stage = j // 2
            p = j % 2
            is_far = 1 - stage % 2
            mine = stage // 2
            half = mine * lk.h + (1 - mine) * (1 - lk.h)
            cols = pl.ds(_al(is_far * far + (1 - is_far) * near + half * IB + p * 1024, 128), 1024)
            pi[:, cols] = pi[:, cols] + _dot(eu[k, :, peer_rows], a[peer_rows, cols])

            @pl.when(stage == 0)
            def _():
                for q in range(2):
                    self.msg(FD, k, 2 * p + q).start()

            @pl.when(stage == 1)
            def _():
                for q in range(2):
                    self.msg(FO, k, 2 * p + q).start()

            @pl.when(stage == 2)
            def _():
                for q in range(2):
                    s = 2 * p + q
                    self.msg(FD, k, s).wait_recv()
                    cs = pl.ds(_al(far + lk.h * IB + s * WX, 128), WX)
                    pi[:, cs] = pi[:, cs] + self.rf[k, :, pl.ds(_al(s * WX, 128), WX)]
                    self.msg(XR, k, s).start()

            @pl.when(stage == 3)
            def _():
                self.msg(GX, k, p).wait_recv()
                self.msg(GF, k, p).start()
            return 0

        lax.fori_loop(0, 8, over_peer, 0)

        if k > 0:
            for s in range(SY):
                self.msg(YR, k - 1, s).wait_send()
        for s in range(SX):
            self.msg(GP, k, s).wait_recv()

        def item_piece(s):
            self.msg(FO, k, s).wait_recv()
            self.msg(XR, k, s).wait_recv()
            c2 = pl.ds(_al(near + lk.h * IB + s * WX, 128), WX)
            piece = pl.ds(_al(s * WX, 128), WX)
            item_final(k, s, (pi[:, c2] + self.ro[k, :, piece]) + self.rx[k, :, piece])

        def user_piece(s):
            self.msg(YR, k, s).wait_recv()
            uc = pl.ds(_al(own_u + s * WY, 128), WY)
            user_final(k, s, pu[:, uc] + self.ry[k, :, s * WY:(s + 1) * WY])

        def users_tile(t, _):
            own = t // 4
            u = own * ((t // 2) % 2) + (1 - own) * (t % 2)
            is_far = own * (t % 2) + (1 - own) * ((t // 2) % 2)
            base = own * own_u + (1 - own) * peer_u + u * WY
            at = is_far * far + (1 - is_far) * near
            rows = pl.ds(_al(base, 512), WY)
            uc = pl.ds(_al(base, 128), WY)
            cols = pl.ds(_al(at, 128), 2 * IB)
            v = _dot_t(ei[k, :, cols], a[rows, cols])

            @pl.when(is_far == 0)
            def _():
                pu[:, uc] = v

            @pl.when(is_far == 1)
            def _():
                pu[:, uc] = pu[:, uc] + v

            @pl.when(t == 0)
            def _():
                for s in range(2, SX):
                    self.msg(GX, k, s).wait_recv()
                    self.msg(GF, k, s).start()

            @pl.when(t == 1)
            def _():
                for s in range(SX):
                    self.msg(GF, k, s).wait_recv()

            @pl.when((t == 2) | (t == 3))
            def _():
                self.msg(YR, k, t - 2).start()

            @pl.when(t == 3)
            def _():
                item_piece(0)

            @pl.when(t == 5)
            def _():
                item_piece(1)

            @pl.when(t == 6)
            def _():
                user_piece(0)
            return 0

        lax.fori_loop(0, 8, users_tile, 0)
        item_piece(2)
        user_piece(1)
        item_piece(3)

    def finish(self):
        k = STEPS - 1
        for s in range(SX):
            self.msg(FD, k, s).wait_send()
            self.msg(XR, k, s).wait_send()
            self.msg(FO, k, s).wait_send()
        for s in range(SY):
            self.msg(YR, k, s).wait_send()
        for k in range(STEPS):
            self.wait_puts(k)


class AllGather:
    def __init__(self, lk, ref, rows, ss, rs):
        self.lk, self.ref, self.rows, self.ss, self.rs = lk, ref, rows, ss, rs

    def _copy(self, i):
        lk = self.lk
        own = lk.slot
        xs, ys, ds_ = _slot_of(lk.xn), _slot_of(lk.yn), _slot_of(lk.diag)
        src_slot = (own, own, own, own, xs, ys, ds_)[i]
        dev = (lk.partner, lk.xn, lk.yn, lk.diag, lk.partner, lk.partner, lk.partner)[i]
        ref = self.ref.at[src_slot, self.rows]
        return _remote(ref, ref, self.ss.at[i], self.rs.at[i], dev)

    def start(self):
        for i in (1, 2, 0, 3):
            self._copy(i).start()

    def arrive(self, i):
        self._copy(i).wait_recv()
        if i in (1, 2, 3):
            self._copy(i + 3).start()

    def slot(self, i):
        lk = self.lk
        c, x, h = lk.c, lk.x, lk.h
        row = (2 * x + 1 - h, 2 * (1 - x) + h, lk.r, 2 * (1 - x) + h,
               2 * (1 - x) + 1 - h, 2 * x + 1 - h, 2 * (1 - x) + 1 - h)[i]
        col = (c, c, 1 - c, 1 - c, c, 1 - c, 1 - c)[i]
        return row * 2 + col

    def drain(self):
        for i in range(7):
            self._copy(i).wait_send()


ORDER = (0, 1, 2, 4, 5, 3, 6)


def _unpack_t(xt):
    n = xt.shape[1] // 2
    return jnp.concatenate([xt[:, :n], xt[:, n:]], axis=0).T


PROP_SCRATCH = [
    pltpu.VMEM((RU, CI), BF16),
    pltpu.VMEM((STEPS, D, CI), BF16),
    pltpu.VMEM((STEPS, D, RU), BF16),
    pltpu.VMEM((D, CI), F32),
    pltpu.VMEM((D, RU), F32),
    pltpu.VMEM((STEPS, D, IB), F32),
    pltpu.VMEM((STEPS, D, IB), F32),
    pltpu.VMEM((STEPS, D, IB), F32),
    pltpu.VMEM((STEPS, D, UB), F32),
    pltpu.SemaphoreType.DMA((STEPS, 8, 4)),
    pltpu.SemaphoreType.DMA((STEPS, 8, 4)),
]

CH = 64
NBUF = 4
NCH = RU // CH
AW = 8


def forward_kernel(mask, e0u, e0i, out_u, out_i, table, a_hbm,
                   a, ei, eu, pi, pu, rf, ro, rx, ry, ss, rs,
                   mbuf, msem, csum, rpart, dcol, drow, dss, drs, su, si, uacc, iacc, asem, tss, trs, iss, irs):
    lk = Links()

    def mask_copy(j):
        slot = j % NBUF
        return pltpu.make_async_copy(mask.at[pl.ds(_al(j * CH, CH), CH), :], mbuf.at[slot], msem.at[slot])

    for j in range(NBUF):
        mask_copy(j).start()
    lk.barrier()
    pr = Prop(lk, a, ei, eu, pi, pu, rf, ro, rx, ry, ss, rs)

    iacc[...] = e0i[...].astype(F32)
    for s in range(SX):
        pr.put_item(0, s, e0i[:, s * WX:(s + 1) * WX])
    uacc[...] = e0u[...].astype(F32)
    for s in range(SY):
        pr.put_user(0, s, e0u[:, s * WY:(s + 1) * WY])

    csum[...] = jnp.zeros_like(csum)

    def chunk(j, _):
        slot = j % NBUF
        mask_copy(j).wait()
        rows = pl.ds(_al(j * CH, CH), CH)

        def cols_body(w, acc):
            cols = pl.ds(_al(w * 512, 512), 512)
            v = mbuf[slot, :, cols].astype(F32)
            a[rows, cols] = v.astype(BF16)
            csum[:, cols] = csum[:, cols] + jnp.sum(v.reshape(CH // 8, 8, 512), axis=0)
            return acc + ((v[:, 0:128] + v[:, 128:256]) + (v[:, 256:384] + v[:, 384:512]))

        rpart[rows, :] = lax.fori_loop(0, CI // 512, cols_body, jnp.zeros((CH, 128), F32))

        @pl.when(j + NBUF < NCH)
        def _():
            mask_copy(j + NBUF).start()
        return 0

    lax.fori_loop(0, NCH, chunk, 0)

    ctot = jnp.sum(csum[...], axis=0, keepdims=True)
    for j in range(8):
        dcol[0, j:j + 1, :] = ctot[:, j * 1024:(j + 1) * 1024]
    drow[0] = _dot_t(jnp.ones((8, 128), BF16), rpart[...].astype(BF16))
    dcopies = [_remote(dcol.at[0], dcol.at[1 + i], dss.at[i], drs.at[i], dev)
               for i, dev in enumerate((lk.partner, lk.xn, lk.xpartner))]
    dcopies.append(_remote(drow.at[0], drow.at[1], dss.at[3], drs.at[3], lk.yn))
    for cp in dcopies:
        cp.start()
    for cp in dcopies:
        cp.wait_recv()
    ctot8 = (dcol[0] + dcol[1]) + (dcol[2] + dcol[3])
    sc8 = lax.rsqrt(jnp.maximum(ctot8, 1.0))
    for j in range(8):
        si[:, j * 1024:(j + 1) * 1024] = sc8[j:j + 1, :]
    su8 = lax.rsqrt(jnp.maximum(drow[0] + drow[1], 1.0))
    for j in range(RU // 128):
        su[j * 128:(j + 1) * 128, :] = jnp.broadcast_to(su8[0:1, j * 128:(j + 1) * 128], (128, 128)).T

    def a_copy(j):
        rows = pl.ds(_al(j * (RU // AW), RU // AW), RU // AW)
        return pltpu.make_async_copy(a.at[rows, :], a_hbm.at[rows, :], asem.at[j])

    def scale(first_col):
        def scale_rows(m, _):
            rows = pl.ds(_al(m * 64, 64), 64)
            s = su[rows, :]
            s4 = jnp.concatenate([s, s, s, s], axis=1)

            def scale_cols(w, _):
                cols = pl.ds(_al(first_col + w * 512, 512), 512)
                a[rows, cols] = a[rows, cols] * (s4 * si[:, cols]).astype(BF16)
                return 0

            lax.fori_loop(0, CI // 1024, scale_cols, 0)
            return 0

        lax.fori_loop(0, RU // 64, scale_rows, 0)

    def scale_near():
        scale(lk.x * 2 * IB)
        for j in range(AW):
            a_copy(j).start()

    scale((1 - lk.x) * 2 * IB)

    def user_final(k, s, v):
        b = v.astype(BF16)
        if k < STEPS - 1:
            pr.put_user(k + 1, s, b)
        uacc[:, s * WY:(s + 1) * WY] = uacc[:, s * WY:(s + 1) * WY] + b.astype(F32)
        if k == STEPS - 1 and s == SY - 1:
            t = uacc[...] * 0.25
            table[lk.slot, 0:PU, :] = _unpack_t(t).astype(BF16)
            ag_u.start()
            out_u[...] = t.astype(BF16)

    def item_final(k, s, v):
        b = v.astype(BF16)
        if k < STEPS - 1:
            pr.put_item(k + 1, s, b)
        iacc[:, s * WX:(s + 1) * WX] = iacc[:, s * WX:(s + 1) * WX] + b.astype(F32)
        if k == STEPS - 1 and s == SX - 1:
            t = iacc[...] * 0.25
            table[lk.slot, PU:PR, :] = _unpack_t(t).astype(BF16)
            ag_i.start()
            out_i[...] = t.astype(BF16)

    ag_u = AllGather(lk, table, pl.ds(0, PU), tss, trs)
    ag_i = AllGather(lk, table, pl.ds(PU, PI), iss, irs)
    for k in range(STEPS):
        pr.step(k, user_final, item_final, scale_near if k == 0 else None)
    for ag in (ag_u, ag_i):
        for i in ORDER:
            ag.arrive(i)
    for cp in dcopies:
        cp.wait_send()
    for j in range(AW):
        a_copy(j).wait()
    pr.finish()
    ag_u.drain()
    ag_i.drain()


def lookup_kernel(table, ru, rp, rn, out, tab, gu, gp, gn):
    def unpack(b, _):
        for lo, n, dst in ((0, PU, 0), (PU, PI, UB)):
            for o in range(0, n, 128):
                v = table[b, lo + o:lo + o + 128, :].astype(F32)
                base = b * (UB + IB) + dst + o
                tab[pl.ds(_al(base, 128), 128), :] = v
                tab[pl.ds(_al(base + n, 128), 128), :] = pltpu.roll(v, D, 1)
        return 0

    lax.fori_loop(0, 8, unpack, 0)

    def gather(g, _):
        for o in range(8):
            t = g * 8 + o
            gu[pl.ds(t, 1), :] = tab[pl.ds(ru[t], 1), :]
            gp[pl.ds(t, 1), :] = tab[pl.ds(rp[t], 1), :]
            gn[pl.ds(t, 1), :] = tab[pl.ds(rn[t], 1), :]
        return 0

    lax.fori_loop(0, TB // 8, gather, 0)

    def block(m, tot):
        rows = pl.ds(_al(m * 128, 128), 128)
        left = lax.broadcasted_iota(jnp.int32, (128, 128), 1) < D
        e_u = gu[rows, :]
        e_d = gp[rows, :] - gn[rows, :]
        x = jnp.sum(jnp.where(left, e_u * e_d, 0.0), axis=1, keepdims=True)
        z = jnp.exp(-jnp.abs(x))
        loss = jnp.maximum(-x, 0.0) + jnp.log1p(z)
        sig = jnp.where(x >= 0.0, z, 1.0) / (1.0 + z)
        coef = sig * (-1.0 / NT)
        out[rows, :] = jnp.where(left, coef * e_d, pltpu.roll(coef * e_u, D, 1))
        return tot + jnp.sum(loss, axis=0, keepdims=True)

    tot = lax.fori_loop(0, TB // 128, block, jnp.zeros((1, 1), F32))
    out[TB:TB + 8, :] = jnp.broadcast_to(tot, (8, 128))


def backward_kernel(a_hbm, g_in, uid, pid, nid, out_u, out_i, out_l,
                    a, ei, eu, pi, pu, rf, ro, rx, ry, ss, rs,
                    asem, g_all, gsem, gss, grs, wu, wi, acc_u, acc_i, su, si):
    lk = Links()
    loads = [pltpu.make_async_copy(a_hbm, a, asem)]
    gcopy = pltpu.make_async_copy(g_in, g_all.at[lk.slot], gsem)
    gcopy.start()
    loads[0].start()
    lk.barrier()
    pr = Prop(lk, a, ei, eu, pi, pu, rf, ro, rx, ry, ss, rs)
    gcopy.wait()
    ag = AllGather(lk, g_all, pl.ds(0, TB + 8), gss, grs)
    ag.start()
    acc_u[...] = jnp.zeros_like(acc_u)
    acc_i[...] = jnp.zeros_like(acc_i)
    base_u = lk.slot * UB
    base_i = (lk.c * 4 + lk.r) * IB

    def scatter(b):
        def split(m, _):
            rows = pl.ds(_al(m * 128, 128), 128)
            left = lax.broadcasted_iota(jnp.int32, (128, 128), 1) < D
            g = g_all[b, rows, :]
            hi = g.astype(BF16).astype(F32)
            r1 = g - hi
            mid = r1.astype(BF16).astype(F32)
            lo = r1 - mid
            wu[rows, 0:128] = jnp.where(left, hi, pltpu.roll(mid, D, 1)).astype(BF16)
            wu[rows, 128:256] = lo.astype(BF16)
            wi[rows, 0:128] = jnp.where(left, pltpu.roll(hi, D, 1), mid).astype(BF16)
            wi[rows, 128:256] = pltpu.roll(lo, D, 1).astype(BF16)
            return 0

        lax.fori_loop(0, TB // 128, split, 0)
        cols = pl.ds(_al(b * TB, 128), TB)
        sub = lax.broadcasted_iota(jnp.int32, (256, TB), 0).astype(F32).astype(BF16)
        one, zero = jnp.array(1.0, BF16), jnp.array(0.0, BF16)

        def lanes(ids, base):
            v = ids[:, cols] - base
            v = jnp.where((v >= 0) & (v < 256), v, -1).astype(F32)
            return jnp.broadcast_to(v, (256, TB)).astype(BF16)

        def users(m, _):
            hot = jnp.where(lanes(uid, base_u + m * 256) == sub, one, zero)
            rows = pl.ds(_al(m * 256, 256), 256)
            acc_u[rows, :] = acc_u[rows, :] + _dot(hot, wu[...])
            return 0

        def items(m, _):
            hot_p = jnp.where(lanes(pid, base_i + m * 256) == sub, one, zero)
            hot = hot_p - jnp.where(lanes(nid, base_i + m * 256) == sub, one, zero)
            rows = pl.ds(_al(m * 256, 256), 256)
            acc_i[rows, :] = acc_i[rows, :] + _dot(hot, wi[...])
            return 0

        lax.fori_loop(0, UB // 256, users, 0)
        lax.fori_loop(0, IB // 256, items, 0)

    scatter(lk.slot)
    for i in ORDER:
        ag.arrive(i)
        scatter(ag.slot(i))

    loss = g_all[0, TB:TB + 8, :]
    for b in range(1, 8):
        loss = loss + g_all[b, TB:TB + 8, :]
    out_l[...] = loss * (1.0 / NT)

    def seed(acc):
        s = (acc[:, 0:128] + pltpu.roll(acc[:, 0:128], D, 1)) + acc[:, 128:256]
        n = s.shape[0] // 2
        s = s * 0.25
        left = lax.broadcasted_iota(jnp.int32, (n, 128), 1) < D
        return jnp.where(left, s[:n], pltpu.roll(s[n:], D, 1)).T

    xi = seed(acc_i[...])
    for s in range(SX):
        src = xi[:D] if s < SX // 2 else xi[D:]
        o = (s % (SX // 2)) * WX
        v = src[:, o:o + WX]
        si[:, s * WX:(s + 1) * WX] = v
        pr.put_item(0, s, v.astype(BF16))
    xu = seed(acc_u[...])
    for s in range(SY):
        v = xu[:D] if s == 0 else xu[D:]
        su[:, s * WY:(s + 1) * WY] = v
        pr.put_user(0, s, v.astype(BF16))

    def user_final(k, s, v):
        v = su[:, s * WY:(s + 1) * WY] + v
        if k < STEPS - 1:
            pr.put_user(k + 1, s, v.astype(BF16))
        else:
            out_u[:, s * WY:(s + 1) * WY] = v

    def item_final(k, s, v):
        v = si[:, s * WX:(s + 1) * WX] + v
        if k < STEPS - 1:
            pr.put_item(k + 1, s, v.astype(BF16))
        else:
            out_i[:, s * WX:(s + 1) * WX] = v

    loads[0].wait()
    for k in range(STEPS):
        pr.step(k, user_final, item_final)
    pr.finish()
    ag.drain()


VM = pl.BlockSpec(memory_space=pltpu.VMEM)
SM = pl.BlockSpec(memory_space=pltpu.SMEM)
ANY = pl.BlockSpec(memory_space=pl.ANY)
DMA = pltpu.SemaphoreType.DMA


def _params(cid):
    return pltpu.CompilerParams(collective_id=cid, has_side_effects=True, vmem_limit_bytes=VMEM_LIMIT)


def solution(mesh):
    def local_fn(mask, e0u, e0i, triples):
        c, r, _, _ = _coords()
        slot = r * 2 + c
        out_u, out_i, table, a_hbm = pl.pallas_call(
            forward_kernel,
            name='forward',
            out_shape=(jax.ShapeDtypeStruct((D, UB), BF16), jax.ShapeDtypeStruct((D, IB), BF16),
                       jax.ShapeDtypeStruct((8, PR, 128), BF16), jax.ShapeDtypeStruct((RU, CI), BF16)),
            in_specs=[ANY, VM, VM],
            out_specs=(VM, VM, VM, ANY),
            scratch_shapes=PROP_SCRATCH + [
                pltpu.VMEM((NBUF, CH, CI), jnp.int32), DMA((NBUF,)),
                pltpu.VMEM((8, CI), F32), pltpu.VMEM((RU, 128), F32),
                pltpu.VMEM((4, 8, 1024), F32), pltpu.VMEM((2, 8, RU), F32), DMA((4,)), DMA((4,)),
                pltpu.VMEM((RU, 128), F32), pltpu.VMEM((1, CI), F32),
                pltpu.VMEM((D, UB), F32), pltpu.VMEM((D, IB), F32), DMA((AW,)),
                DMA((7,)), DMA((7,)), DMA((7,)), DMA((7,)),
            ],
            compiler_params=_params(0),
        )(mask, e0u.T, e0i.T)

        cols = triples.T
        mine = lax.dynamic_slice(cols, (0, slot * TB), (3, TB))
        per = UB + IB
        row_u = (mine[0] // UB) * per + mine[0] % UB
        blk = mine[1:] // IB
        row_i = ((blk % 4) * 2 + blk // 4) * per + UB + mine[1:] % IB
        g = pl.pallas_call(
            lookup_kernel,
            name='lookup',
            out_shape=jax.ShapeDtypeStruct((TB + 8, 128), F32),
            in_specs=[VM, SM, SM, SM],
            out_specs=VM,
            scratch_shapes=[pltpu.VMEM((8 * per, 128), F32)] + [pltpu.VMEM((TB, 128), F32)] * 3,
            compiler_params=pltpu.CompilerParams(vmem_limit_bytes=40 * 1024 * 1024),
        )(table, row_u, row_i[0], row_i[1])

        d_u, d_i, loss = pl.pallas_call(
            backward_kernel,
            name='backward',
            out_shape=(jax.ShapeDtypeStruct((D, UB), F32), jax.ShapeDtypeStruct((D, IB), F32),
                       jax.ShapeDtypeStruct((8, 128), F32)),
            in_specs=[ANY, ANY, VM, VM, VM],
            out_specs=(VM, VM, VM),
            scratch_shapes=PROP_SCRATCH + [
                DMA, pltpu.VMEM((8, TB + 8, 128), F32), DMA, DMA((7,)), DMA((7,)),
                pltpu.VMEM((TB, 256), BF16), pltpu.VMEM((TB, 256), BF16),
                pltpu.VMEM((UB, 256), F32), pltpu.VMEM((IB, 256), F32),
                pltpu.VMEM((D, UB), F32), pltpu.VMEM((D, IB), F32),
            ],
            compiler_params=_params(1),
        )(a_hbm, g, cols[0:1], cols[1:2], cols[2:3])
        return out_u.T, out_i.T, loss[0, 0], d_u.T, d_i.T

    user_spec = P(('row', 'col'), None)
    item_spec = P(('col', 'row'), None)
    return jax.shard_map(local_fn, mesh=mesh, in_specs=(P('row', 'col'), user_spec, item_spec, P()),
                         out_specs=(user_spec, item_spec, P(), user_spec, item_spec), check_vma=False)
```

```python
import jax
import jax.numpy as jnp
from jax import lax
from jax.experimental import pallas as pl
from jax.experimental.pallas import tpu as pltpu
from jax.sharding import PartitionSpec as P

MESH = pl.DeviceIdType.MESH
F32 = jnp.float32
BF16 = jnp.bfloat16

D = 64
UB = 1024
IB = 2048
RU = 2048
CI = 8192
STEPS = 3
SX = 4
WX = IB // SX
SY = 2
WY = UB // SY
TB = 1024
NT = 8192
PU = UB // 2
PI = IB // 2
PR = PU + PI

FD, XR, FO, GP, GX, GF, YR, YG = range(8)
VMEM_LIMIT = 67043328


def _coords():
    c = lax.axis_index('col')
    r = lax.axis_index('row')
    x = r // 2
    h = r % 2
    return c, r, x, h


def _dot(a, b):
    return lax.dot_general(a, b, (((1,), (0,)), ((), ())), preferred_element_type=F32)


def _dot_t(a, b):
    return lax.dot_general(a, b, (((1,), (1,)), ((), ())), preferred_element_type=F32)


def _al(v, m):
    return pl.multiple_of(v, m)


class Links:
    def __init__(self):
        self.c, self.r, self.x, self.h = _coords()
        c, r, x, h = self.c, self.r, self.x, self.h
        self.partner = (c, 2 * x + (1 - h))
        self.xn = (c, 2 * (1 - x) + h)
        self.yn = (1 - c, r)
        self.diag = (1 - c, 2 * (1 - x) + h)
        self.xpartner = (c, 2 * (1 - x) + (1 - h))
        self.slot = r * 2 + c

    def barrier(self):
        sem = pltpu.get_barrier_semaphore()
        peers = (self.partner, self.xn, self.yn, self.diag, self.xpartner)
        for p in peers:
            pl.semaphore_signal(sem, inc=1, device_id=p, device_id_type=MESH)
        pl.semaphore_wait(sem, len(peers))


def _slot_of(dev):
    return dev[1] * 2 + dev[0]


def _remote(src, dst, ss, rs, dev):
    return pltpu.make_async_remote_copy(src_ref=src, dst_ref=dst, send_sem=ss, recv_sem=rs, device_id=dev, device_id_type=MESH)


class Prop:
    def __init__(self, lk, a, ei, eu, pi, pu, rf, ro, rx, ry, ss, rs):
        self.lk = lk
        self.a, self.ei, self.eu, self.pi, self.pu = a, ei, eu, pi, pu
        self.rf, self.ro, self.rx, self.ry = rf, ro, rx, ry
        self.ss, self.rs = ss, rs

    def msg(self, kind, k, s):
        lk = self.lk
        ss, rs = self.ss.at[k, kind, s], self.rs.at[k, kind, s]
        other = 1 - lk.x
        if kind == FD:
            src = self.pi.at[:, pl.ds(_al((2 * other + 1 - lk.h) * IB + s * WX, 128), WX)]
            dst = self.rf.at[k, :, pl.ds(_al(s * WX, 128), WX)]
            return _remote(src, dst, ss, rs, lk.partner)
        if kind == XR:
            src = self.pi.at[:, pl.ds(_al((2 * other + lk.h) * IB + s * WX, 128), WX)]
            dst = self.rx.at[k, :, pl.ds(_al(s * WX, 128), WX)]
            return _remote(src, dst, ss, rs, lk.xn)
        if kind == FO:
            src = self.pi.at[:, pl.ds(_al((2 * lk.x + 1 - lk.h) * IB + s * WX, 128), WX)]
            dst = self.ro.at[k, :, pl.ds(_al(s * WX, 128), WX)]
            return _remote(src, dst, ss, rs, lk.partner)
        if kind in (GP, GX):
            ref = self.ei.at[k, :, pl.ds(_al(lk.r * IB + s * WX, 128), WX)]
            return _remote(ref, ref, ss, rs, lk.partner if kind == GP else lk.xn)
        if kind == GF:
            ref = self.ei.at[k, :, pl.ds(_al((2 * other + lk.h) * IB + s * WX, 128), WX)]
            return _remote(ref, ref, ss, rs, lk.partner)
        if kind == YR:
            src = self.pu.at[:, pl.ds(_al((1 - lk.c) * UB + s * WY, 128), WY)]
            dst = self.ry.at[k, :, pl.ds(_al(s * WY, 128), WY)]
            return _remote(src, dst, ss, rs, lk.yn)
        ref = self.eu.at[k, :, pl.ds(_al(lk.c * UB + s * WY, 128), WY)]
        return _remote(ref, ref, ss, rs, lk.yn)

    def put_item(self, k, s, value):
        self.ei[k, :, pl.ds(_al(self.lk.r * IB + s * WX, 128), WX)] = value
        self.msg(GX, k, s).start()
        self.msg(GP, k, s).start()

    def put_user(self, k, s, value):
        self.eu[k, :, pl.ds(_al(self.lk.c * UB + s * WY, 128), WY)] = value
        self.msg(YG, k, s).start()

    def wait_puts(self, k):
        for s in range(SX):
            self.msg(GX, k, s).wait_send()
            self.msg(GP, k, s).wait_send()
            if k == STEPS - 1:
                self.msg(GF, k, s).wait_send()
        for s in range(SY):
            self.msg(YG, k, s).wait_send()

    def step(self, k, user_final, item_final, between=None):
        lk = self.lk
        a, ei, eu, pi, pu = self.a, self.ei, self.eu, self.pi, self.pu
        far = (1 - lk.x) * 2 * IB
        near = lk.x * 2 * IB
        own_u = lk.c * UB
        peer_u = (1 - lk.c) * UB

        if k > 0:
            for s in range(SX):
                self.msg(FD, k - 1, s).wait_send()
                self.msg(XR, k - 1, s).wait_send()
                self.msg(FO, k - 1, s).wait_send()
                self.msg(GF, k - 1, s).wait_send()
        own_rows = pl.ds(_al(own_u, 128), UB)
        peer_rows = pl.ds(_al(peer_u, 128), UB)

        def over_own(first_col):
            cols = pl.ds(_al(first_col, 128), 2 * IB)
            pi[:, cols] = _dot(eu[k, :, own_rows], a[own_rows, cols])

        over_own(far)
        if between is not None:
            between()
        over_own(near)
        for s in range(SY):
            self.msg(YG, k, s).wait_recv()

        def over_peer(stage, _):
            is_far = 1 - stage % 2
            mine = stage // 2
            half = mine * lk.h + (1 - mine) * (1 - lk.h)
            cols = pl.ds(_al(is_far * far + (1 - is_far) * near + half * IB, 128), IB)
            pi[:, cols] = pi[:, cols] + _dot(eu[k, :, peer_rows], a[peer_rows, cols])

            @pl.when(stage == 0)
            def _():
                for s in range(SX):
                    self.msg(FD, k, s).start()

            @pl.when(stage == 1)
            def _():
                for s in range(SX):
                    self.msg(FO, k, s).start()

            @pl.when(stage == 2)
            def _():
                for s in range(SX):
                    self.msg(FD, k, s).wait_recv()
                    cs = pl.ds(_al(far + lk.h * IB + s * WX, 128), WX)
                    pi[:, cs] = pi[:, cs] + self.rf[k, :, s * WX:(s + 1) * WX]
                    self.msg(XR, k, s).start()

            @pl.when(stage == 3)
            def _():
                for s in range(2):
                    self.msg(GX, k, s).wait_recv()
                    self.msg(GF, k, s).start()
            return 0

        lax.fori_loop(0, 4, over_peer, 0)

        if k > 0:
            for s in range(SY):
                self.msg(YR, k - 1, s).wait_send()
        for s in range(SX):
            self.msg(GP, k, s).wait_recv()

        def item_piece(s):
            self.msg(FO, k, s).wait_recv()
            self.msg(XR, k, s).wait_recv()
            c2 = pl.ds(_al(near + lk.h * IB + s * WX, 128), WX)
            piece = pl.ds(_al(s * WX, 128), WX)
            item_final(k, s, (pi[:, c2] + self.ro[k, :, piece]) + self.rx[k, :, piece])

        def user_piece(s):
            self.msg(YR, k, s).wait_recv()
            uc = pl.ds(_al(own_u + s * WY, 128), WY)
            user_final(k, s, pu[:, uc] + self.ry[k, :, s * WY:(s + 1) * WY])

        def users_tile(t, _):
            own = t // 4
            u = own * ((t // 2) % 2) + (1 - own) * (t % 2)
            is_far = own * (t % 2) + (1 - own) * ((t // 2) % 2)
            base = own * own_u + (1 - own) * peer_u + u * WY
            at = is_far * far + (1 - is_far) * near
            rows = pl.ds(_al(base, 512), WY)
            uc = pl.ds(_al(base, 128), WY)
            cols = pl.ds(_al(at, 128), 2 * IB)
            v = _dot_t(ei[k, :, cols], a[rows, cols])

            @pl.when(is_far == 0)
            def _():
                pu[:, uc] = v

            @pl.when(is_far == 1)
            def _():
                pu[:, uc] = pu[:, uc] + v

            @pl.when(t == 0)
            def _():
                for s in range(2, SX):
                    self.msg(GX, k, s).wait_recv()
                    self.msg(GF, k, s).start()

            @pl.when(t == 1)
            def _():
                for s in range(SX):
                    self.msg(GF, k, s).wait_recv()

            @pl.when((t == 2) | (t == 3))
            def _():
                self.msg(YR, k, t - 2).start()

            @pl.when(t == 3)
            def _():
                item_piece(0)

            @pl.when(t == 5)
            def _():
                item_piece(1)

            @pl.when(t == 6)
            def _():
                user_piece(0)
            return 0

        lax.fori_loop(0, 8, users_tile, 0)
        item_piece(2)
        user_piece(1)
        item_piece(3)

    def finish(self):
        k = STEPS - 1
        for s in range(SX):
            self.msg(FD, k, s).wait_send()
            self.msg(XR, k, s).wait_send()
            self.msg(FO, k, s).wait_send()
        for s in range(SY):
            self.msg(YR, k, s).wait_send()
        for k in range(STEPS):
            self.wait_puts(k)


class AllGather:
    def __init__(self, lk, ref, start, n_lo, n_hi, ss, rs):
        self.lk, self.ref, self.ss, self.rs = lk, ref, ss, rs
        self.full, self.lo, self.hi = pl.ds(start, n_lo + n_hi), pl.ds(start, n_lo), pl.ds(start + n_lo, n_hi)
        self.two = n_hi > 0

    def _copy(self, i):
        lk = self.lk
        xs, ys, ds_ = _slot_of(lk.xn), _slot_of(lk.yn), _slot_of(lk.diag)
        src_slot = (lk.slot, lk.slot, lk.slot, xs, ys, xs, ys, ds_, ds_)[i]
        dev = (lk.partner, lk.xn, lk.yn, lk.yn, lk.xn, lk.partner, lk.partner, lk.partner, lk.partner)[i]
        rows = (self.full, self.full, self.full, self.lo, self.hi, self.full, self.full, self.lo, self.hi)[i]
        ref = self.ref.at[src_slot, rows]
        return _remote(ref, ref, self.ss.at[i], self.rs.at[i], dev)

    def _used(self, i):
        return self.two or i not in (4, 8)

    def start(self):
        for i in (1, 2, 0):
            self._copy(i).start()

    def arrive(self, i):
        if not self._used(i):
            return
        self._copy(i).wait_recv()
        for j in {1: (3, 5), 2: (4, 6), 3: (7,), 4: (8,)}.get(i, ()):
            if self._used(j):
                self._copy(j).start()

    def slot(self, i):
        lk = self.lk
        c, x, h = lk.c, lk.x, lk.h
        row = {0: 2 * x + 1 - h, 1: 2 * (1 - x) + h, 2: lk.r, 4: 2 * (1 - x) + h,
               5: 2 * (1 - x) + 1 - h, 6: 2 * x + 1 - h, 8: 2 * (1 - x) + 1 - h}[i]
        col = {0: c, 1: c, 2: 1 - c, 4: 1 - c, 5: c, 6: 1 - c, 8: 1 - c}[i]
        return row * 2 + col

    def drain(self):
        for i in range(9):
            if self._used(i):
                self._copy(i).wait_send()


def _unpack_t(xt):
    n = xt.shape[1] // 2
    return jnp.concatenate([xt[:, :n], xt[:, n:]], axis=0).T


PROP_SCRATCH = [
    pltpu.VMEM((RU, CI), BF16),
    pltpu.VMEM((STEPS, D, CI), BF16),
    pltpu.VMEM((STEPS, D, RU), BF16),
    pltpu.VMEM((D, CI), F32),
    pltpu.VMEM((D, RU), F32),
    pltpu.VMEM((STEPS, D, IB), F32),
    pltpu.VMEM((STEPS, D, IB), F32),
    pltpu.VMEM((STEPS, D, IB), F32),
    pltpu.VMEM((STEPS, D, UB), F32),
    pltpu.SemaphoreType.DMA((STEPS, 8, 4)),
    pltpu.SemaphoreType.DMA((STEPS, 8, 4)),
]

CH = 64
NBUF = 4
NCH = RU // CH
AW = 8


def forward_kernel(mask, e0u, e0i, out_u, out_i, table, a_hbm,
                   a, ei, eu, pi, pu, rf, ro, rx, ry, ss, rs,
                   mbuf, msem, csum, rpart, dcol, drow, dss, drs, su, si, uacc, iacc, asem, iss, irs):
    lk = Links()

    def mask_copy(j):
        slot = j % NBUF
        return pltpu.make_async_copy(mask.at[pl.ds(_al(j * CH, CH), CH), :], mbuf.at[slot], msem.at[slot])

    for j in range(NBUF):
        mask_copy(j).start()
    lk.barrier()
    pr = Prop(lk, a, ei, eu, pi, pu, rf, ro, rx, ry, ss, rs)

    iacc[...] = e0i[...].astype(F32)
    for s in range(SX):
        pr.put_item(0, s, e0i[:, s * WX:(s + 1) * WX])
    uacc[...] = e0u[...].astype(F32)
    for s in range(SY):
        pr.put_user(0, s, e0u[:, s * WY:(s + 1) * WY])

    csum[...] = jnp.zeros_like(csum)

    def chunk(j, _):
        slot = j % NBUF
        mask_copy(j).wait()
        rows = pl.ds(_al(j * CH, CH), CH)

        def cols_body(w, acc):
            cols = pl.ds(_al(w * 512, 512), 512)
            v = mbuf[slot, :, cols].astype(F32)
            a[rows, cols] = v.astype(BF16)
            csum[:, cols] = csum[:, cols] + jnp.sum(v.reshape(CH // 8, 8, 512), axis=0)
            return acc + ((v[:, 0:128] + v[:, 128:256]) + (v[:, 256:384] + v[:, 384:512]))

        rpart[rows, :] = lax.fori_loop(0, CI // 512, cols_body, jnp.zeros((CH, 128), F32))

        @pl.when(j + NBUF < NCH)
        def _():
            mask_copy(j + NBUF).start()
        return 0

    lax.fori_loop(0, NCH, chunk, 0)

    ctot = jnp.sum(csum[...], axis=0, keepdims=True)
    for j in range(8):
        dcol[0, j:j + 1, :] = ctot[:, j * 1024:(j + 1) * 1024]
    drow[0] = _dot_t(jnp.ones((8, 128), BF16), rpart[...].astype(BF16))
    dcopies = [_remote(dcol.at[0], dcol.at[1 + i], dss.at[i], drs.at[i], dev)
               for i, dev in enumerate((lk.partner, lk.xn, lk.xpartner))]
    dcopies.append(_remote(drow.at[0], drow.at[1], dss.at[3], drs.at[3], lk.yn))
    for cp in dcopies:
        cp.start()
    for cp in dcopies:
        cp.wait_recv()
    ctot8 = (dcol[0] + dcol[1]) + (dcol[2] + dcol[3])
    sc8 = lax.rsqrt(jnp.maximum(ctot8, 1.0))
    for j in range(8):
        si[:, j * 1024:(j + 1) * 1024] = sc8[j:j + 1, :]
    su8 = lax.rsqrt(jnp.maximum(drow[0] + drow[1], 1.0))
    for j in range(RU // 128):
        su[j * 128:(j + 1) * 128, :] = jnp.broadcast_to(su8[0:1, j * 128:(j + 1) * 128], (128, 128)).T

    def a_copy(j):
        rows = pl.ds(_al(j * (RU // AW), RU // AW), RU // AW)
        return pltpu.make_async_copy(a.at[rows, :], a_hbm.at[rows, :], asem.at[j])

    def scale(first_col):
        def scale_rows(m, _):
            rows = pl.ds(_al(m * 64, 64), 64)
            s = su[rows, :]
            s4 = jnp.concatenate([s, s, s, s], axis=1)

            def scale_cols(w, _):
                cols = pl.ds(_al(first_col + w * 512, 512), 512)
                a[rows, cols] = a[rows, cols] * (s4 * si[:, cols]).astype(BF16)
                return 0

            lax.fori_loop(0, CI // 1024, scale_cols, 0)
            return 0

        lax.fori_loop(0, RU // 64, scale_rows, 0)

    def scale_near():
        scale(lk.x * 2 * IB)
        for j in range(AW):
            a_copy(j).start()

    scale((1 - lk.x) * 2 * IB)

    def user_final(k, s, v):
        b = v.astype(BF16)
        if k < STEPS - 1:
            pr.put_user(k + 1, s, b)
        uacc[:, s * WY:(s + 1) * WY] = uacc[:, s * WY:(s + 1) * WY] + b.astype(F32)
        if k == STEPS - 1 and s == SY - 1:
            t = uacc[...] * 0.25
            table[lk.slot, 0:PU, :] = _unpack_t(t).astype(BF16)
            ag_u.start()
            out_u[...] = t.astype(BF16)

    def item_final(k, s, v):
        b = v.astype(BF16)
        if k < STEPS - 1:
            pr.put_item(k + 1, s, b)
        iacc[:, s * WX:(s + 1) * WX] = iacc[:, s * WX:(s + 1) * WX] + b.astype(F32)
        if k == STEPS - 1:
            t = iacc[:, s * WX:(s + 1) * WX] * 0.25
            table[lk.slot, PU + s * WX // 2:PU + (s + 1) * WX // 2, :] = _unpack_t(t).astype(BF16)
            ags[s].start()
            out_i[:, s * WX:(s + 1) * WX] = t.astype(BF16)

    ags = [AllGather(lk, table, PU + s * WX // 2, WX // 2, 0, iss.at[s], irs.at[s]) for s in range(SX)]
    ag_u = AllGather(lk, table, 0, PU, 0, iss.at[SX], irs.at[SX])
    ags.append(ag_u)
    for k in range(STEPS):
        pr.step(k, user_final, item_final, scale_near if k == 0 else None)
    for group in ((1, 2), (3,), (0, 5, 6, 7)):
        for s in (SX, 0, 1, 2, 3):
            for i in group:
                ags[s].arrive(i)
    for cp in dcopies:
        cp.wait_send()
    for j in range(AW):
        a_copy(j).wait()
    pr.finish()
    for ag in ags:
        ag.drain()


def lookup_kernel(table, ru, rp, rn, out, tab, gu, gp, gn):
    def unpack(b, _):
        for lo, n, dst in [(0, PU, 0)] + [(PU + s * WX // 2, WX // 2, UB + s * WX) for s in range(SX)]:
            for o in range(0, n, 128):
                v = table[b, lo + o:lo + o + 128, :].astype(F32)
                base = b * (UB + IB) + dst + o
                tab[pl.ds(_al(base, 128), 128), :] = v
                tab[pl.ds(_al(base + n, 128), 128), :] = pltpu.roll(v, D, 1)
        return 0

    lax.fori_loop(0, 8, unpack, 0)

    def gather(g, _):
        for o in range(8):
            t = g * 8 + o
            gu[pl.ds(t, 1), :] = tab[pl.ds(ru[t], 1), :]
            gp[pl.ds(t, 1), :] = tab[pl.ds(rp[t], 1), :]
            gn[pl.ds(t, 1), :] = tab[pl.ds(rn[t], 1), :]
        return 0

    lax.fori_loop(0, TB // 8, gather, 0)

    def block(m, tot):
        rows = pl.ds(_al(m * 128, 128), 128)
        left = lax.broadcasted_iota(jnp.int32, (128, 128), 1) < D
        e_u = gu[rows, :]
        e_d = gp[rows, :] - gn[rows, :]
        x = jnp.sum(jnp.where(left, e_u * e_d, 0.0), axis=1, keepdims=True)
        z = jnp.exp(-jnp.abs(x))
        loss = jnp.maximum(-x, 0.0) + jnp.log1p(z)
        sig = jnp.where(x >= 0.0, z, 1.0) / (1.0 + z)
        coef = sig * (-1.0 / NT)
        out[rows, :] = jnp.where(left, coef * e_d, pltpu.roll(coef * e_u, D, 1))
        return tot + jnp.sum(loss, axis=0, keepdims=True)

    tot = lax.fori_loop(0, TB // 128, block, jnp.zeros((1, 1), F32))
    out[TB:TB + 8, :] = jnp.broadcast_to(tot, (8, 128))


def backward_kernel(a_hbm, g_in, uid, pid, nid, out_u, out_i, out_l,
                    a, ei, eu, pi, pu, rf, ro, rx, ry, ss, rs,
                    asem, g_all, gsem, gss, grs, wu, wi, acc_u, acc_i, su, si):
    lk = Links()
    loads = [pltpu.make_async_copy(a_hbm, a, asem)]
    gcopy = pltpu.make_async_copy(g_in, g_all.at[lk.slot], gsem)
    gcopy.start()
    loads[0].start()
    lk.barrier()
    pr = Prop(lk, a, ei, eu, pi, pu, rf, ro, rx, ry, ss, rs)
    gcopy.wait()
    ag = AllGather(lk, g_all, 0, TB // 2, TB // 2 + 8, gss, grs)
    ag.start()
    acc_u[...] = jnp.zeros_like(acc_u)
    acc_i[...] = jnp.zeros_like(acc_i)
    base_u = lk.slot * UB
    base_i = (lk.c * 4 + lk.r) * IB

    def scatter(b):
        def split(m, _):
            rows = pl.ds(_al(m * 256, 256), 256)
            left = lax.broadcasted_iota(jnp.int32, (256, 128), 1) < D
            g = g_all[b, rows, :]
            hi = g.astype(BF16).astype(F32)
            r1 = g - hi
            mid = r1.astype(BF16).astype(F32)
            lo = r1 - mid
            wu[rows, 0:128] = jnp.where(left, hi, pltpu.roll(mid, D, 1)).astype(BF16)
            wu[rows, 128:256] = lo.astype(BF16)
            wi[rows, 0:128] = jnp.where(left, pltpu.roll(hi, D, 1), mid).astype(BF16)
            wi[rows, 128:256] = pltpu.roll(lo, D, 1).astype(BF16)
            return 0

        lax.fori_loop(0, TB // 256, split, 0)
        cols = pl.ds(_al(b * TB, 128), TB)
        sub = lax.broadcasted_iota(jnp.int32, (256, TB), 0).astype(F32).astype(BF16)
        one, zero = jnp.array(1.0, BF16), jnp.array(0.0, BF16)

        def lanes(ids, base):
            v = ids[:, cols] - base
            v = jnp.where((v >= 0) & (v < 256), v, -1).astype(F32)
            return jnp.broadcast_to(v, (256, TB)).astype(BF16)

        def hot(ids, base):
            return jnp.concatenate([jnp.where(lanes(ids, base + m * 256) == sub, one, zero) for m in range(4)], axis=0)

        acc_u[...] = acc_u[...] + _dot(hot(uid, base_u), wu[...])

        def items(m, _):
            rows = pl.ds(_al(m * 1024, 1024), 1024)
            acc_i[rows, :] = acc_i[rows, :] + _dot(hot(pid, base_i + m * 1024) - hot(nid, base_i + m * 1024), wi[...])
            return 0

        lax.fori_loop(0, IB // 1024, items, 0)

    scatter(lk.slot)
    for group in ((0,), (1,), (2,), (5,), (6,), (3, 4), (7, 8)):
        for i in group:
            ag.arrive(i)
        scatter(ag.slot(group[-1]))

    loss = g_all[0, TB:TB + 8, :]
    for b in range(1, 8):
        loss = loss + g_all[b, TB:TB + 8, :]
    out_l[...] = loss * (1.0 / NT)

    def seed(acc):
        s = (acc[:, 0:128] + pltpu.roll(acc[:, 0:128], D, 1)) + acc[:, 128:256]
        n = s.shape[0] // 2
        s = s * 0.25
        left = lax.broadcasted_iota(jnp.int32, (n, 128), 1) < D
        return jnp.where(left, s[:n], pltpu.roll(s[n:], D, 1)).T

    xi = seed(acc_i[...])
    for s in range(SX):
        src = xi[:D] if s < SX // 2 else xi[D:]
        o = (s % (SX // 2)) * WX
        v = src[:, o:o + WX]
        si[:, s * WX:(s + 1) * WX] = v
        pr.put_item(0, s, v.astype(BF16))
    xu = seed(acc_u[...])
    for s in range(SY):
        v = xu[:D] if s == 0 else xu[D:]
        su[:, s * WY:(s + 1) * WY] = v
        pr.put_user(0, s, v.astype(BF16))

    def user_final(k, s, v):
        v = su[:, s * WY:(s + 1) * WY] + v
        if k < STEPS - 1:
            pr.put_user(k + 1, s, v.astype(BF16))
        else:
            out_u[:, s * WY:(s + 1) * WY] = v

    def item_final(k, s, v):
        v = si[:, s * WX:(s + 1) * WX] + v
        if k < STEPS - 1:
            pr.put_item(k + 1, s, v.astype(BF16))
        else:
            out_i[:, s * WX:(s + 1) * WX] = v

    loads[0].wait()
    for k in range(STEPS):
        pr.step(k, user_final, item_final)
    pr.finish()
    ag.drain()


def finish_kernel(*refs):
    for src, dst in zip(refs[:4], refs[4:]):
        dst[...] = src[...]


VM = pl.BlockSpec(memory_space=pltpu.VMEM)
SM = pl.BlockSpec(memory_space=pltpu.SMEM)
ANY = pl.BlockSpec(memory_space=pl.ANY)
DMA = pltpu.SemaphoreType.DMA


def _params(cid):
    return pltpu.CompilerParams(collective_id=cid, has_side_effects=True, vmem_limit_bytes=VMEM_LIMIT)


def solution(mesh):
    def local_fn(mask, e0u, e0i, triples):
        c, r, _, _ = _coords()
        slot = r * 2 + c
        out_u, out_i, table, a_hbm = pl.pallas_call(
            forward_kernel,
            name='forward',
            out_shape=(jax.ShapeDtypeStruct((D, UB), BF16), jax.ShapeDtypeStruct((D, IB), BF16),
                       jax.ShapeDtypeStruct((8, PR, 128), BF16), jax.ShapeDtypeStruct((RU, CI), BF16)),
            in_specs=[ANY, VM, VM],
            out_specs=(VM, VM, VM, ANY),
            scratch_shapes=PROP_SCRATCH + [
                pltpu.VMEM((NBUF, CH, CI), jnp.int32), DMA((NBUF,)),
                pltpu.VMEM((8, CI), F32), pltpu.VMEM((RU, 128), F32),
                pltpu.VMEM((4, 8, 1024), F32), pltpu.VMEM((2, 8, RU), F32), DMA((4,)), DMA((4,)),
                pltpu.VMEM((RU, 128), F32), pltpu.VMEM((1, CI), F32),
                pltpu.VMEM((D, UB), F32), pltpu.VMEM((D, IB), F32), DMA((AW,)),
                DMA((SX + 1, 9)), DMA((SX + 1, 9)),
            ],
            compiler_params=_params(0),
        )(mask, e0u.T, e0i.T)

        cols = triples.T
        mine = lax.dynamic_slice(cols, (0, slot * TB), (3, TB))
        per = UB + IB
        row_u = (mine[0] // UB) * per + mine[0] % UB
        blk = mine[1:] // IB
        row_i = ((blk % 4) * 2 + blk // 4) * per + UB + mine[1:] % IB
        g = pl.pallas_call(
            lookup_kernel,
            name='lookup',
            out_shape=jax.ShapeDtypeStruct((TB + 8, 128), F32),
            in_specs=[VM, SM, SM, SM],
            out_specs=VM,
            scratch_shapes=[pltpu.VMEM((8 * per, 128), F32)] + [pltpu.VMEM((TB, 128), F32)] * 3,
            compiler_params=pltpu.CompilerParams(vmem_limit_bytes=40 * 1024 * 1024),
        )(table, row_u, row_i[0], row_i[1])

        d_u, d_i, loss = pl.pallas_call(
            backward_kernel,
            name='backward',
            out_shape=(jax.ShapeDtypeStruct((D, UB), F32), jax.ShapeDtypeStruct((D, IB), F32),
                       jax.ShapeDtypeStruct((8, 128), F32)),
            in_specs=[ANY, ANY, VM, VM, VM],
            out_specs=(VM, VM, VM),
            scratch_shapes=PROP_SCRATCH + [
                DMA, pltpu.VMEM((8, TB + 8, 128), F32), DMA, DMA((9,)), DMA((9,)),
                pltpu.VMEM((TB, 256), BF16), pltpu.VMEM((TB, 256), BF16),
                pltpu.VMEM((UB, 256), F32), pltpu.VMEM((IB, 256), F32),
                pltpu.VMEM((D, UB), F32), pltpu.VMEM((D, IB), F32),
            ],
            compiler_params=_params(1),
        )(a_hbm, g, cols[0:1], cols[1:2], cols[2:3])
        outs = (out_u, out_i, d_u, d_i)
        out_u, out_i, d_u, d_i = pl.pallas_call(
            finish_kernel,
            name='finish',
            out_shape=tuple(jax.ShapeDtypeStruct(o.shape, o.dtype) for o in outs),
            in_specs=[VM] * 4,
            out_specs=(VM,) * 4,
        )(*outs)
        return out_u.T, out_i.T, loss[0, 0], d_u.T, d_i.T

    user_spec = P(('row', 'col'), None)
    item_spec = P(('col', 'row'), None)
    return jax.shard_map(local_fn, mesh=mesh, in_specs=(P('row', 'col'), user_spec, item_spec, P()),
                         out_specs=(user_spec, item_spec, P(), user_spec, item_spec), check_vma=False)
```

```python
import jax
import jax.numpy as jnp
from jax import lax
from jax.experimental import pallas as pl
from jax.experimental.pallas import tpu as pltpu
from jax.sharding import PartitionSpec as P

MESH = pl.DeviceIdType.MESH
F32 = jnp.float32
BF16 = jnp.bfloat16

D = 64
UB = 1024
IB = 2048
RU = 2048
CI = 8192
STEPS = 3
SX = 4
WX = IB // SX
SY = 2
WY = UB // SY
TB = 1024
NT = 8192
PU = UB // 2
PI = IB // 2
PR = PU + PI

FD, XR, FO, GP, GX, GF, YR, YG = range(8)
VMEM_LIMIT = 67043328


def _coords():
    c = lax.axis_index('col')
    r = lax.axis_index('row')
    x = r // 2
    h = r % 2
    return c, r, x, h


def _dot(a, b):
    return lax.dot_general(a, b, (((1,), (0,)), ((), ())), preferred_element_type=F32)


def _dot_t(a, b):
    return lax.dot_general(a, b, (((1,), (1,)), ((), ())), preferred_element_type=F32)


def _al(v, m):
    return pl.multiple_of(v, m)


class Links:
    def __init__(self):
        self.c, self.r, self.x, self.h = _coords()
        c, r, x, h = self.c, self.r, self.x, self.h
        self.partner = (c, 2 * x + (1 - h))
        self.xn = (c, 2 * (1 - x) + h)
        self.yn = (1 - c, r)
        self.diag = (1 - c, 2 * (1 - x) + h)
        self.xpartner = (c, 2 * (1 - x) + (1 - h))
        self.slot = r * 2 + c

    def barrier(self):
        sem = pltpu.get_barrier_semaphore()
        peers = (self.partner, self.xn, self.yn, self.diag, self.xpartner)
        for p in peers:
            pl.semaphore_signal(sem, inc=1, device_id=p, device_id_type=MESH)
        pl.semaphore_wait(sem, len(peers))


def _slot_of(dev):
    return dev[1] * 2 + dev[0]


def _remote(src, dst, ss, rs, dev):
    return pltpu.make_async_remote_copy(src_ref=src, dst_ref=dst, send_sem=ss, recv_sem=rs, device_id=dev, device_id_type=MESH)


class Prop:
    def __init__(self, lk, a, ei, eu, pi, pu, rf, ro, rx, ry, ss, rs):
        self.lk = lk
        self.a, self.ei, self.eu, self.pi, self.pu = a, ei, eu, pi, pu
        self.rf, self.ro, self.rx, self.ry = rf, ro, rx, ry
        self.ss, self.rs = ss, rs

    def msg(self, kind, k, s):
        lk = self.lk
        ss, rs = self.ss.at[k, kind, s], self.rs.at[k, kind, s]
        other = 1 - lk.x
        if kind == FD:
            src = self.pi.at[:, pl.ds(_al((2 * other + 1 - lk.h) * IB + s * WX, 128), WX)]
            dst = self.rf.at[k, :, pl.ds(_al(s * WX, 128), WX)]
            return _remote(src, dst, ss, rs, lk.partner)
        if kind == XR:
            src = self.pi.at[:, pl.ds(_al((2 * other + lk.h) * IB + s * WX, 128), WX)]
            dst = self.rx.at[k, :, pl.ds(_al(s * WX, 128), WX)]
            return _remote(src, dst, ss, rs, lk.xn)
        if kind == FO:
            src = self.pi.at[:, pl.ds(_al((2 * lk.x + 1 - lk.h) * IB + s * WX, 128), WX)]
            dst = self.ro.at[k, :, pl.ds(_al(s * WX, 128), WX)]
            return _remote(src, dst, ss, rs, lk.partner)
        if kind in (GP, GX):
            ref = self.ei.at[k, :, pl.ds(_al(lk.r * IB + s * WX, 128), WX)]
            return _remote(ref, ref, ss, rs, lk.partner if kind == GP else lk.xn)
        if kind == GF:
            ref = self.ei.at[k, :, pl.ds(_al((2 * other + lk.h) * IB + s * WX, 128), WX)]
            return _remote(ref, ref, ss, rs, lk.partner)
        if kind == YR:
            src = self.pu.at[:, pl.ds(_al((1 - lk.c) * UB + s * WY, 128), WY)]
            dst = self.ry.at[k, :, pl.ds(_al(s * WY, 128), WY)]
            return _remote(src, dst, ss, rs, lk.yn)
        ref = self.eu.at[k, :, pl.ds(_al(lk.c * UB + s * WY, 128), WY)]
        return _remote(ref, ref, ss, rs, lk.yn)

    def put_item(self, k, s, value):
        self.ei[k, :, pl.ds(_al(self.lk.r * IB + s * WX, 128), WX)] = value
        self.msg(GX, k, s).start()
        self.msg(GP, k, s).start()

    def put_user(self, k, s, value):
        self.eu[k, :, pl.ds(_al(self.lk.c * UB + s * WY, 128), WY)] = value
        self.msg(YG, k, s).start()

    def wait_puts(self, k):
        for s in range(SX):
            self.msg(GX, k, s).wait_send()
            self.msg(GP, k, s).wait_send()
            if k == STEPS - 1:
                self.msg(GF, k, s).wait_send()
        for s in range(SY):
            self.msg(YG, k, s).wait_send()

    def step(self, k, user_final, item_final, between=None):
        lk = self.lk
        a, ei, eu, pi, pu = self.a, self.ei, self.eu, self.pi, self.pu
        far = (1 - lk.x) * 2 * IB
        near = lk.x * 2 * IB
        own_u = lk.c * UB
        peer_u = (1 - lk.c) * UB

        if k > 0:
            for s in range(SX):
                self.msg(FD, k - 1, s).wait_send()
                self.msg(XR, k - 1, s).wait_send()
                self.msg(FO, k - 1, s).wait_send()
                self.msg(GF, k - 1, s).wait_send()
        own_rows = pl.ds(_al(own_u, 128), UB)
        peer_rows = pl.ds(_al(peer_u, 128), UB)

        def over_own(j, _):
            cols = pl.ds(_al(far + j * (near - far), 128), 2 * IB)
            pi[:, cols] = _dot(eu[k, :, own_rows], a[own_rows, cols])
            return 0

        late_near = between is not None
        lax.fori_loop(0, 1 if late_near else 2, over_own, 0)
        for s in range(SY):
            self.msg(YG, k, s).wait_recv()

        def over_peer(stage, _):
            is_far = 1 - (stage // 2 if late_near else stage % 2)
            mine = stage % 2 if late_near else stage // 2
            half = mine * lk.h + (1 - mine) * (1 - lk.h)
            cols = pl.ds(_al(is_far * far + (1 - is_far) * near + half * IB, 128), IB)
            pi[:, cols] = pi[:, cols] + _dot(eu[k, :, peer_rows], a[peer_rows, cols])

            @pl.when(is_far * (1 - mine) == 1)
            def _():
                for s in range(SX):
                    self.msg(FD, k, s).start()

            @pl.when((1 - is_far) * (1 - mine) == 1)
            def _():
                for s in range(SX):
                    self.msg(FO, k, s).start()

            @pl.when(is_far * mine == 1)
            def _():
                for s in range(SX):
                    self.msg(FD, k, s).wait_recv()
                    cs = pl.ds(_al(far + lk.h * IB + s * WX, 128), WX)
                    pi[:, cs] = pi[:, cs] + self.rf[k, :, s * WX:(s + 1) * WX]
                    self.msg(XR, k, s).start()

            @pl.when((1 - is_far) * mine == 1)
            def _():
                for s in range(2):
                    self.msg(GX, k, s).wait_recv()
                    self.msg(GF, k, s).start()
            return 0

        if late_near:
            lax.fori_loop(0, 2, over_peer, 0)
            between()
            lax.fori_loop(1, 2, over_own, 0)
            lax.fori_loop(2, 4, over_peer, 0)
        else:
            lax.fori_loop(0, 4, over_peer, 0)

        if k > 0:
            for s in range(SY):
                self.msg(YR, k - 1, s).wait_send()
        for s in range(SX):
            self.msg(GP, k, s).wait_recv()

        def item_piece(s):
            self.msg(FO, k, s).wait_recv()
            self.msg(XR, k, s).wait_recv()
            c2 = pl.ds(_al(near + lk.h * IB + s * WX, 128), WX)
            piece = pl.ds(_al(s * WX, 128), WX)
            item_final(k, s, (pi[:, c2] + self.ro[k, :, piece]) + self.rx[k, :, piece])

        def user_piece(s):
            self.msg(YR, k, s).wait_recv()
            uc = pl.ds(_al(own_u + s * WY, 128), WY)
            user_final(k, s, pu[:, uc] + self.ry[k, :, s * WY:(s + 1) * WY])

        def users_tile(t, _):
            own = t // 4
            u = own * ((t // 2) % 2) + (1 - own) * (t % 2)
            is_far = own * (t % 2) + (1 - own) * ((t // 2) % 2)
            base = own * own_u + (1 - own) * peer_u + u * WY
            at = is_far * far + (1 - is_far) * near
            rows = pl.ds(_al(base, 512), WY)
            uc = pl.ds(_al(base, 128), WY)
            cols = pl.ds(_al(at, 128), 2 * IB)
            v = _dot_t(ei[k, :, cols], a[rows, cols])

            @pl.when(is_far == 0)
            def _():
                pu[:, uc] = v

            @pl.when(is_far == 1)
            def _():
                pu[:, uc] = pu[:, uc] + v

            @pl.when(t == 0)
            def _():
                for s in range(2, SX):
                    self.msg(GX, k, s).wait_recv()
                    self.msg(GF, k, s).start()

            @pl.when(t == 1)
            def _():
                for s in range(SX):
                    self.msg(GF, k, s).wait_recv()

            @pl.when((t == 2) | (t == 3))
            def _():
                self.msg(YR, k, t - 2).start()

            @pl.when(t == 3)
            def _():
                item_piece(0)

            @pl.when(t == 5)
            def _():
                item_piece(1)

            @pl.when(t == 6)
            def _():
                user_piece(0)
            return 0

        lax.fori_loop(0, 8, users_tile, 0)
        item_piece(2)
        user_piece(1)
        item_piece(3)

    def finish(self):
        k = STEPS - 1
        for s in range(SX):
            self.msg(FD, k, s).wait_send()
            self.msg(XR, k, s).wait_send()
            self.msg(FO, k, s).wait_send()
        for s in range(SY):
            self.msg(YR, k, s).wait_send()
        for k in range(STEPS):
            self.wait_puts(k)


class AllGather:
    def __init__(self, lk, ref, start, n_lo, n_hi, ss, rs):
        self.lk, self.ref, self.ss, self.rs = lk, ref, ss, rs
        self.full, self.lo, self.hi = pl.ds(start, n_lo + n_hi), pl.ds(start, n_lo), pl.ds(start + n_lo, n_hi)
        self.two = n_hi > 0

    def _copy(self, i):
        lk = self.lk
        xs, ys, ds_ = _slot_of(lk.xn), _slot_of(lk.yn), _slot_of(lk.diag)
        src_slot = (lk.slot, lk.slot, lk.slot, xs, ys, xs, ys, ds_, ds_)[i]
        dev = (lk.partner, lk.xn, lk.yn, lk.yn, lk.xn, lk.partner, lk.partner, lk.partner, lk.partner)[i]
        rows = (self.full, self.full, self.full, self.lo, self.hi, self.full, self.full, self.lo, self.hi)[i]
        ref = self.ref.at[src_slot, rows]
        return _remote(ref, ref, self.ss.at[i], self.rs.at[i], dev)

    def _used(self, i):
        return self.two or i not in (4, 8)

    def start(self):
        for i in (1, 2, 0):
            self._copy(i).start()

    def arrive(self, i):
        if not self._used(i):
            return
        self._copy(i).wait_recv()
        for j in {1: (3, 5), 2: (4, 6), 3: (7,), 4: (8,)}.get(i, ()):
            if self._used(j):
                self._copy(j).start()

    def slot(self, i):
        lk = self.lk
        c, x, h = lk.c, lk.x, lk.h
        row = {0: 2 * x + 1 - h, 1: 2 * (1 - x) + h, 2: lk.r, 4: 2 * (1 - x) + h,
               5: 2 * (1 - x) + 1 - h, 6: 2 * x + 1 - h, 8: 2 * (1 - x) + 1 - h}[i]
        col = {0: c, 1: c, 2: 1 - c, 4: 1 - c, 5: c, 6: 1 - c, 8: 1 - c}[i]
        return row * 2 + col

    def drain(self):
        for i in range(9):
            if self._used(i):
                self._copy(i).wait_send()


def _unpack_t(xt):
    n = xt.shape[1] // 2
    return jnp.concatenate([xt[:, :n], xt[:, n:]], axis=0).T


PROP_SCRATCH = [
    pltpu.VMEM((RU, CI), BF16),
    pltpu.VMEM((STEPS, D, CI), BF16),
    pltpu.VMEM((STEPS, D, RU), BF16),
    pltpu.VMEM((D, CI), F32),
    pltpu.VMEM((D, RU), F32),
    pltpu.VMEM((STEPS, D, IB), F32),
    pltpu.VMEM((STEPS, D, IB), F32),
    pltpu.VMEM((STEPS, D, IB), F32),
    pltpu.VMEM((STEPS, D, UB), F32),
    pltpu.SemaphoreType.DMA((STEPS, 8, 4)),
    pltpu.SemaphoreType.DMA((STEPS, 8, 4)),
]

CH = 64
NBUF = 4
NCH = RU // CH
AW = 8


def forward_kernel(mask, e0u, e0i, out_u, out_i, table, a_hbm,
                   a, ei, eu, pi, pu, rf, ro, rx, ry, ss, rs,
                   mbuf, msem, csum, rpart, dcol, drow, dss, drs, su, si, uacc, iacc, asem, iss, irs):
    lk = Links()

    def mask_copy(j):
        slot = j % NBUF
        return pltpu.make_async_copy(mask.at[pl.ds(_al(j * CH, CH), CH), :], mbuf.at[slot], msem.at[slot])

    for j in range(NBUF):
        mask_copy(j).start()
    lk.barrier()
    pr = Prop(lk, a, ei, eu, pi, pu, rf, ro, rx, ry, ss, rs)

    iacc[...] = e0i[...].astype(F32)
    for s in range(SX):
        pr.put_item(0, s, e0i[:, s * WX:(s + 1) * WX])
    uacc[...] = e0u[...].astype(F32)
    for s in range(SY):
        pr.put_user(0, s, e0u[:, s * WY:(s + 1) * WY])

    csum[...] = jnp.zeros_like(csum)

    def chunk(j, _):
        slot = j % NBUF
        mask_copy(j).wait()
        rows = pl.ds(_al(j * CH, CH), CH)

        def cols_body(w, acc):
            cols = pl.ds(_al(w * 512, 512), 512)
            v = mbuf[slot, :, cols].astype(F32)
            a[rows, cols] = v.astype(BF16)
            csum[:, cols] = csum[:, cols] + jnp.sum(v.reshape(CH // 8, 8, 512), axis=0)
            return acc + ((v[:, 0:128] + v[:, 128:256]) + (v[:, 256:384] + v[:, 384:512]))

        rpart[rows, :] = lax.fori_loop(0, CI // 512, cols_body, jnp.zeros((CH, 128), F32))

        @pl.when(j + NBUF < NCH)
        def _():
            mask_copy(j + NBUF).start()
        return 0

    lax.fori_loop(0, NCH, chunk, 0)

    ctot = jnp.sum(csum[...], axis=0, keepdims=True)
    for j in range(8):
        dcol[0, j:j + 1, :] = ctot[:, j * 1024:(j + 1) * 1024]
    drow[0] = _dot_t(jnp.ones((8, 128), BF16), rpart[...].astype(BF16))
    dcopies = [_remote(dcol.at[0], dcol.at[1 + i], dss.at[i], drs.at[i], dev)
               for i, dev in enumerate((lk.partner, lk.xn, lk.xpartner))]
    dcopies.append(_remote(drow.at[0], drow.at[1], dss.at[3], drs.at[3], lk.yn))
    for cp in dcopies:
        cp.start()
    for cp in dcopies:
        cp.wait_recv()
    ctot8 = (dcol[0] + dcol[1]) + (dcol[2] + dcol[3])
    sc8 = lax.rsqrt(jnp.maximum(ctot8, 1.0))
    for j in range(8):
        si[:, j * 1024:(j + 1) * 1024] = sc8[j:j + 1, :]
    su8 = lax.rsqrt(jnp.maximum(drow[0] + drow[1], 1.0))
    for j in range(RU // 128):
        su[j * 128:(j + 1) * 128, :] = jnp.broadcast_to(su8[0:1, j * 128:(j + 1) * 128], (128, 128)).T

    def a_copy(j):
        rows = pl.ds(_al(j * (RU // AW), RU // AW), RU // AW)
        return pltpu.make_async_copy(a.at[rows, :], a_hbm.at[rows, :], asem.at[j])

    def scale(first_col):
        def scale_rows(m, _):
            rows = pl.ds(_al(m * 64, 64), 64)
            s = su[rows, :]
            s4 = jnp.concatenate([s, s, s, s], axis=1)

            def scale_cols(w, _):
                cols = pl.ds(_al(first_col + w * 512, 512), 512)
                a[rows, cols] = a[rows, cols] * (s4 * si[:, cols]).astype(BF16)
                return 0

            lax.fori_loop(0, CI // 1024, scale_cols, 0)
            return 0

        lax.fori_loop(0, RU // 64, scale_rows, 0)

    def scale_near():
        scale(lk.x * 2 * IB)
        for j in range(AW):
            a_copy(j).start()

    scale((1 - lk.x) * 2 * IB)

    def user_final(k, s, v):
        b = v.astype(BF16)
        if k < STEPS - 1:
            pr.put_user(k + 1, s, b)
        uacc[:, s * WY:(s + 1) * WY] = uacc[:, s * WY:(s + 1) * WY] + b.astype(F32)
        if k == STEPS - 1 and s == SY - 1:
            t = uacc[...] * 0.25
            table[lk.slot, 0:PU, :] = _unpack_t(t).astype(BF16)
            ag_u.start()
            out_u[...] = t.astype(BF16)

    def item_final(k, s, v):
        b = v.astype(BF16)
        if k < STEPS - 1:
            pr.put_item(k + 1, s, b)
        iacc[:, s * WX:(s + 1) * WX] = iacc[:, s * WX:(s + 1) * WX] + b.astype(F32)
        if k == STEPS - 1:
            t = iacc[:, s * WX:(s + 1) * WX] * 0.25
            table[lk.slot, PU + s * WX // 2:PU + (s + 1) * WX // 2, :] = _unpack_t(t).astype(BF16)
            ags[s].start()
            out_i[:, s * WX:(s + 1) * WX] = t.astype(BF16)

    ags = [AllGather(lk, table, PU + s * WX // 2, WX // 2, 0, iss.at[s], irs.at[s]) for s in range(SX)]
    ag_u = AllGather(lk, table, 0, PU, 0, iss.at[SX], irs.at[SX])
    ags.append(ag_u)
    for k in range(STEPS):
        pr.step(k, user_final, item_final, scale_near if k == 0 else None)
    for group in ((1, 2), (3,), (0, 5, 6, 7)):
        for s in (SX, 0, 1, 2, 3):
            for i in group:
                ags[s].arrive(i)
    for cp in dcopies:
        cp.wait_send()
    for j in range(AW):
        a_copy(j).wait()
    pr.finish()
    for ag in ags:
        ag.drain()


def lookup_kernel(table_hbm, ids, out, table, tsem, tab, gu, gp, gn):
    def load(b):
        return pltpu.make_async_copy(table_hbm.at[b], table.at[b], tsem.at[b])

    for b in range(8):
        load(b).start()

    def unpack(b, _):
        load(b).wait()
        for lo, n, dst in [(0, PU, 0)] + [(PU + s * WX // 2, WX // 2, UB + s * WX) for s in range(SX)]:
            for o in range(0, n, 128):
                v = table[b, lo + o:lo + o + 128, :].astype(F32)
                base = b * (UB + IB) + dst + o
                tab[pl.ds(_al(base, 128), 128), :] = v
                tab[pl.ds(_al(base + n, 128), 128), :] = pltpu.roll(v, D, 1)
        return 0

    lax.fori_loop(0, 8, unpack, 0)

    def gather(g, _):
        for o in range(8):
            t = g * 8 + o
            gu[pl.ds(t, 1), :] = tab[pl.ds(ids[0, t], 1), :]
            gp[pl.ds(t, 1), :] = tab[pl.ds(ids[1, t], 1), :]
            gn[pl.ds(t, 1), :] = tab[pl.ds(ids[2, t], 1), :]
        return 0

    lax.fori_loop(0, TB // 8, gather, 0)

    def block(m, tot):
        rows = pl.ds(_al(m * 128, 128), 128)
        left = lax.broadcasted_iota(jnp.int32, (128, 128), 1) < D
        e_u = gu[rows, :]
        e_d = gp[rows, :] - gn[rows, :]
        x = jnp.sum(jnp.where(left, e_u * e_d, 0.0), axis=1, keepdims=True)
        z = jnp.exp(-jnp.abs(x))
        loss = jnp.maximum(-x, 0.0) + jnp.log1p(z)
        sig = jnp.where(x >= 0.0, z, 1.0) / (1.0 + z)
        coef = sig * (-1.0 / NT)
        out[rows, :] = jnp.where(left, coef * e_d, pltpu.roll(coef * e_u, D, 1))
        return tot + jnp.sum(loss, axis=0, keepdims=True)

    tot = lax.fori_loop(0, TB // 128, block, jnp.zeros((1, 1), F32))
    out[TB:TB + 8, :] = jnp.broadcast_to(tot, (8, 128))


def backward_kernel(a_hbm, g_in, ids, out_u, out_i, out_l,
                    a, ei, eu, pi, pu, rf, ro, rx, ry, ss, rs,
                    asem, g_all, gsem, gss, grs, wu, wi, acc_u, acc_i, su, si):
    lk = Links()
    loads = [pltpu.make_async_copy(a_hbm, a, asem)]
    gcopy = pltpu.make_async_copy(g_in, g_all.at[lk.slot], gsem)
    gcopy.start()
    loads[0].start()
    lk.barrier()
    pr = Prop(lk, a, ei, eu, pi, pu, rf, ro, rx, ry, ss, rs)
    gcopy.wait()
    ag = AllGather(lk, g_all, 0, TB // 2, TB // 2 + 8, gss, grs)
    ag.start()
    acc_u[...] = jnp.zeros_like(acc_u)
    acc_i[...] = jnp.zeros_like(acc_i)
    base_u = lk.slot * UB
    base_i = (lk.c * 4 + lk.r) * IB

    def scatter(b):
        def split(m, _):
            rows = pl.ds(_al(m * 256, 256), 256)
            left = lax.broadcasted_iota(jnp.int32, (256, 128), 1) < D
            g = g_all[b, rows, :]
            hi = g.astype(BF16).astype(F32)
            r1 = g - hi
            mid = r1.astype(BF16).astype(F32)
            lo = r1 - mid
            wu[rows, 0:128] = jnp.where(left, hi, pltpu.roll(mid, D, 1)).astype(BF16)
            wu[rows, 128:256] = lo.astype(BF16)
            wi[rows, 0:128] = jnp.where(left, pltpu.roll(hi, D, 1), mid).astype(BF16)
            wi[rows, 128:256] = pltpu.roll(lo, D, 1).astype(BF16)
            return 0

        lax.fori_loop(0, TB // 256, split, 0)
        cols = pl.ds(_al(b * TB, 128), TB)
        sub = lax.broadcasted_iota(jnp.int32, (256, TB), 0).astype(F32).astype(BF16)
        one, zero = jnp.array(1.0, BF16), jnp.array(0.0, BF16)

        def lanes(which, base):
            v = ids[which:which + 1, cols] - base
            v = jnp.where((v >= 0) & (v < 256), v, -1).astype(F32)
            return jnp.broadcast_to(v, (256, TB)).astype(BF16)

        def hot(which, base):
            return jnp.concatenate([jnp.where(lanes(which, base + m * 256) == sub, one, zero) for m in range(4)], axis=0)

        acc_u[...] = acc_u[...] + _dot(hot(0, base_u), wu[...])

        def items(m, _):
            rows = pl.ds(_al(m * 1024, 1024), 1024)
            acc_i[rows, :] = acc_i[rows, :] + _dot(hot(1, base_i + m * 1024) - hot(2, base_i + m * 1024), wi[...])
            return 0

        lax.fori_loop(0, IB // 1024, items, 0)

    scatter(lk.slot)
    for group in ((0,), (1,), (2,), (5,), (6,), (3, 4), (7, 8)):
        for i in group:
            ag.arrive(i)
        scatter(ag.slot(group[-1]))

    loss = g_all[0, TB:TB + 8, :]
    for b in range(1, 8):
        loss = loss + g_all[b, TB:TB + 8, :]
    out_l[...] = loss * (1.0 / NT)

    def seed(acc):
        s = (acc[:, 0:128] + pltpu.roll(acc[:, 0:128], D, 1)) + acc[:, 128:256]
        n = s.shape[0] // 2
        s = s * 0.25
        left = lax.broadcasted_iota(jnp.int32, (n, 128), 1) < D
        return jnp.where(left, s[:n], pltpu.roll(s[n:], D, 1)).T

    xi = seed(acc_i[...])
    for s in range(SX):
        src = xi[:D] if s < SX // 2 else xi[D:]
        o = (s % (SX // 2)) * WX
        v = src[:, o:o + WX]
        si[:, s * WX:(s + 1) * WX] = v
        pr.put_item(0, s, v.astype(BF16))
    xu = seed(acc_u[...])
    for s in range(SY):
        v = xu[:D] if s == 0 else xu[D:]
        su[:, s * WY:(s + 1) * WY] = v
        pr.put_user(0, s, v.astype(BF16))

    def user_final(k, s, v):
        v = su[:, s * WY:(s + 1) * WY] + v
        if k < STEPS - 1:
            pr.put_user(k + 1, s, v.astype(BF16))
        else:
            out_u[:, s * WY:(s + 1) * WY] = v

    def item_final(k, s, v):
        v = si[:, s * WX:(s + 1) * WX] + v
        if k < STEPS - 1:
            pr.put_item(k + 1, s, v.astype(BF16))
        else:
            out_i[:, s * WX:(s + 1) * WX] = v

    loads[0].wait()
    for k in range(STEPS):
        pr.step(k, user_final, item_final)
    pr.finish()
    ag.drain()


def finish_kernel(*refs):
    for src, dst in zip(refs[:4], refs[4:]):
        dst[...] = src[...]


VM = pl.BlockSpec(memory_space=pltpu.VMEM)
SM = pl.BlockSpec(memory_space=pltpu.SMEM)
ANY = pl.BlockSpec(memory_space=pl.ANY)
DMA = pltpu.SemaphoreType.DMA


def _params(cid):
    return pltpu.CompilerParams(collective_id=cid, has_side_effects=True, vmem_limit_bytes=VMEM_LIMIT)


def solution(mesh):
    def local_fn(mask, e0u, e0i, triples):
        c, r, _, _ = _coords()
        slot = r * 2 + c
        out_u, out_i, table, a_hbm = pl.pallas_call(
            forward_kernel,
            name='forward',
            out_shape=(jax.ShapeDtypeStruct((D, UB), BF16), jax.ShapeDtypeStruct((D, IB), BF16),
                       jax.ShapeDtypeStruct((8, PR, 128), BF16), jax.ShapeDtypeStruct((RU, CI), BF16)),
            in_specs=[ANY, VM, VM],
            out_specs=(VM, VM, VM, ANY),
            scratch_shapes=PROP_SCRATCH + [
                pltpu.VMEM((NBUF, CH, CI), jnp.int32), DMA((NBUF,)),
                pltpu.VMEM((8, CI), F32), pltpu.VMEM((RU, 128), F32),
                pltpu.VMEM((4, 8, 1024), F32), pltpu.VMEM((2, 8, RU), F32), DMA((4,)), DMA((4,)),
                pltpu.VMEM((RU, 128), F32), pltpu.VMEM((1, CI), F32),
                pltpu.VMEM((D, UB), F32), pltpu.VMEM((D, IB), F32), DMA((AW,)),
                DMA((SX + 1, 9)), DMA((SX + 1, 9)),
            ],
            compiler_params=_params(0),
        )(mask, e0u.T, e0i.T)

        cols = triples.T
        mine = lax.dynamic_slice(cols, (0, slot * TB), (3, TB))
        per = UB + IB
        blk = mine // IB
        row_i = ((blk % 4) * 2 + blk // 4) * per + UB + mine % IB
        row_u = (mine // UB) * per + mine % UB
        ids = jnp.where(lax.broadcasted_iota(jnp.int32, (3, TB), 0) == 0, row_u, row_i)
        g = pl.pallas_call(
            lookup_kernel,
            name='lookup',
            out_shape=jax.ShapeDtypeStruct((TB + 8, 128), F32),
            in_specs=[ANY, SM],
            out_specs=VM,
            scratch_shapes=[pltpu.VMEM((8, PR, 128), BF16), DMA((8,)), pltpu.VMEM((8 * per, 128), F32)] + [pltpu.VMEM((TB, 128), F32)] * 3,
            compiler_params=pltpu.CompilerParams(vmem_limit_bytes=VMEM_LIMIT),
        )(table, ids)

        d_u, d_i, loss = pl.pallas_call(
            backward_kernel,
            name='backward',
            out_shape=(jax.ShapeDtypeStruct((D, UB), F32), jax.ShapeDtypeStruct((D, IB), F32),
                       jax.ShapeDtypeStruct((8, 128), F32)),
            in_specs=[ANY, ANY, VM],
            out_specs=(VM, VM, VM),
            scratch_shapes=PROP_SCRATCH + [
                DMA, pltpu.VMEM((8, TB + 8, 128), F32), DMA, DMA((9,)), DMA((9,)),
                pltpu.VMEM((TB, 256), BF16), pltpu.VMEM((TB, 256), BF16),
                pltpu.VMEM((UB, 256), F32), pltpu.VMEM((IB, 256), F32),
                pltpu.VMEM((D, UB), F32), pltpu.VMEM((D, IB), F32),
            ],
            compiler_params=_params(1),
        )(a_hbm, g, cols)
        outs = (out_u, out_i, d_u, d_i)
        out_u, out_i, d_u, d_i = pl.pallas_call(
            finish_kernel,
            name='finish',
            out_shape=tuple(jax.ShapeDtypeStruct(o.shape, o.dtype) for o in outs),
            in_specs=[VM] * 4,
            out_specs=(VM,) * 4,
        )(*outs)
        return out_u.T, out_i.T, loss[0, 0], d_u.T, d_i.T

    user_spec = P(('row', 'col'), None)
    item_spec = P(('col', 'row'), None)
    return jax.shard_map(local_fn, mesh=mesh, in_specs=(P('row', 'col'), user_spec, item_spec, P()),
                         out_specs=(user_spec, item_spec, P(), user_spec, item_spec), check_vma=False)
```

```python
import jax
import jax.numpy as jnp
from jax import lax
from jax.experimental import pallas as pl
from jax.experimental.pallas import tpu as pltpu
from jax.sharding import PartitionSpec as P

MESH = pl.DeviceIdType.MESH
F32 = jnp.float32
BF16 = jnp.bfloat16

D = 64
UB = 1024
IB = 2048
RU = 2048
CI = 8192
STEPS = 3
SX = 4
WX = IB // SX
SY = 2
WY = UB // SY
TB = 1024
NT = 8192
PU = UB // 2
PI = IB // 2
PR = PU + PI

FD, XR, FO, GP, GX, GF, YR, YG = range(8)
VMEM_LIMIT = 67043328


def _coords():
    c = lax.axis_index('col')
    r = lax.axis_index('row')
    x = r // 2
    h = r % 2
    return c, r, x, h


def _dot(a, b):
    return lax.dot_general(a, b, (((1,), (0,)), ((), ())), preferred_element_type=F32)


def _dot_t(a, b):
    return lax.dot_general(a, b, (((1,), (1,)), ((), ())), preferred_element_type=F32)


def _al(v, m):
    return pl.multiple_of(v, m)


class Links:
    def __init__(self):
        self.c, self.r, self.x, self.h = _coords()
        c, r, x, h = self.c, self.r, self.x, self.h
        self.partner = (c, 2 * x + (1 - h))
        self.xn = (c, 2 * (1 - x) + h)
        self.yn = (1 - c, r)
        self.diag = (1 - c, 2 * (1 - x) + h)
        self.xpartner = (c, 2 * (1 - x) + (1 - h))
        self.slot = r * 2 + c

    def barrier(self):
        sem = pltpu.get_barrier_semaphore()
        peers = (self.partner, self.xn, self.yn, self.diag, self.xpartner)
        for p in peers:
            pl.semaphore_signal(sem, inc=1, device_id=p, device_id_type=MESH)
        pl.semaphore_wait(sem, len(peers))


def _slot_of(dev):
    return dev[1] * 2 + dev[0]


def _remote(src, dst, ss, rs, dev):
    return pltpu.make_async_remote_copy(src_ref=src, dst_ref=dst, send_sem=ss, recv_sem=rs, device_id=dev, device_id_type=MESH)


class Prop:
    def __init__(self, lk, a, ei, eu, pi, pu, rf, ro, rx, ry, ss, rs):
        self.lk = lk
        self.a, self.ei, self.eu, self.pi, self.pu = a, ei, eu, pi, pu
        self.rf, self.ro, self.rx, self.ry = rf, ro, rx, ry
        self.ss, self.rs = ss, rs
        pu[...] = jnp.zeros_like(pu)

    def msg(self, kind, k, s):
        lk = self.lk
        ss, rs = self.ss.at[k, kind, s], self.rs.at[k, kind, s]
        other = 1 - lk.x
        if kind == FD:
            src = self.pi.at[:, pl.ds(_al((2 * other + 1 - lk.h) * IB + s * WX, 128), WX)]
            dst = self.rf.at[k, :, pl.ds(_al(s * WX, 128), WX)]
            return _remote(src, dst, ss, rs, lk.partner)
        if kind == XR:
            src = self.pi.at[:, pl.ds(_al((2 * other + lk.h) * IB + s * WX, 128), WX)]
            dst = self.rx.at[k, :, pl.ds(_al(s * WX, 128), WX)]
            return _remote(src, dst, ss, rs, lk.xn)
        if kind == FO:
            src = self.pi.at[:, pl.ds(_al((2 * lk.x + 1 - lk.h) * IB + s * WX, 128), WX)]
            dst = self.ro.at[k, :, pl.ds(_al(s * WX, 128), WX)]
            return _remote(src, dst, ss, rs, lk.partner)
        if kind in (GP, GX):
            ref = self.ei.at[k, :, pl.ds(_al(lk.r * IB + s * WX, 128), WX)]
            return _remote(ref, ref, ss, rs, lk.partner if kind == GP else lk.xn)
        if kind == GF:
            ref = self.ei.at[k, :, pl.ds(_al((2 * other + lk.h) * IB + s * WX, 128), WX)]
            return _remote(ref, ref, ss, rs, lk.partner)
        if kind == YR:
            src = self.pu.at[:, pl.ds(_al((1 - lk.c) * UB + s * WY, 128), WY)]
            dst = self.ry.at[k, :, pl.ds(_al(s * WY, 128), WY)]
            return _remote(src, dst, ss, rs, lk.yn)
        ref = self.eu.at[k, :, pl.ds(_al(lk.c * UB + s * WY, 128), WY)]
        return _remote(ref, ref, ss, rs, lk.yn)

    def put_item(self, k, s, value):
        self.ei[k, :, pl.ds(_al(self.lk.r * IB + s * WX, 128), WX)] = value
        self.msg(GX, k, s).start()
        self.msg(GP, k, s).start()

    def put_user(self, k, s, value):
        self.eu[k, :, pl.ds(_al(self.lk.c * UB + s * WY, 128), WY)] = value
        self.msg(YG, k, s).start()

    def wait_puts(self, k):
        for s in range(SX):
            self.msg(GX, k, s).wait_send()
            self.msg(GP, k, s).wait_send()
            if k == STEPS - 1:
                self.msg(GF, k, s).wait_send()
        for s in range(SY):
            self.msg(YG, k, s).wait_send()

    def step(self, k, user_final, item_final, between=None):
        lk = self.lk
        a, ei, eu, pi, pu = self.a, self.ei, self.eu, self.pi, self.pu
        far = (1 - lk.x) * 2 * IB
        near = lk.x * 2 * IB
        own_u = lk.c * UB
        peer_u = (1 - lk.c) * UB

        if k > 0:
            for s in range(SX):
                self.msg(FD, k - 1, s).wait_send()
                self.msg(XR, k - 1, s).wait_send()
                self.msg(FO, k - 1, s).wait_send()
                self.msg(GF, k - 1, s).wait_send()
        own_rows = pl.ds(_al(own_u, 128), UB)
        peer_rows = pl.ds(_al(peer_u, 128), UB)

        def over_own(j, _):
            cols = pl.ds(_al(far + j * (near - far), 128), 2 * IB)
            pi[:, cols] = _dot(eu[k, :, own_rows], a[own_rows, cols])
            return 0

        late_near = between is not None
        lax.fori_loop(0, 1 if late_near else 2, over_own, 0)
        for s in range(SY):
            self.msg(YG, k, s).wait_recv()

        def over_peer(stage, _):
            is_far = 1 - (stage // 2 if late_near else stage % 2)
            mine = stage % 2 if late_near else stage // 2
            half = mine * lk.h + (1 - mine) * (1 - lk.h)
            cols = pl.ds(_al(is_far * far + (1 - is_far) * near + half * IB, 128), IB)
            pi[:, cols] = pi[:, cols] + _dot(eu[k, :, peer_rows], a[peer_rows, cols])

            @pl.when(is_far * (1 - mine) == 1)
            def _():
                for s in range(SX):
                    self.msg(FD, k, s).start()

            @pl.when((1 - is_far) * (1 - mine) == 1)
            def _():
                for s in range(SX):
                    self.msg(FO, k, s).start()

            @pl.when(is_far * mine == 1)
            def _():
                for s in range(SX):
                    self.msg(FD, k, s).wait_recv()
                    cs = pl.ds(_al(far + lk.h * IB + s * WX, 128), WX)
                    pi[:, cs] = pi[:, cs] + self.rf[k, :, s * WX:(s + 1) * WX]
                    self.msg(XR, k, s).start()

            @pl.when((1 - is_far) * mine == 1)
            def _():
                for s in range(2):
                    self.msg(GX, k, s).wait_recv()
                    self.msg(GF, k, s).start()
            return 0

        if late_near:
            lax.fori_loop(0, 2, over_peer, 0)
            between()
            lax.fori_loop(1, 2, over_own, 0)
            lax.fori_loop(2, 4, over_peer, 0)
        else:
            lax.fori_loop(0, 4, over_peer, 0)

        if k > 0:
            for s in range(SY):
                self.msg(YR, k - 1, s).wait_send()
        for s in range(SX):
            self.msg(GP, k, s).wait_recv()

        def item_piece(s):
            self.msg(FO, k, s).wait_recv()
            self.msg(XR, k, s).wait_recv()
            c2 = pl.ds(_al(near + lk.h * IB + s * WX, 128), WX)
            piece = pl.ds(_al(s * WX, 128), WX)
            item_final(k, s, (pi[:, c2] + self.ro[k, :, piece]) + self.rx[k, :, piece])

        def user_piece(s):
            self.msg(YR, k, s).wait_recv()
            uc = pl.ds(_al(own_u + s * WY, 128), WY)
            user_final(k, s, pu[:, uc] + self.ry[k, :, s * WY:(s + 1) * WY])

        def users_tile(t, _):
            own = t // 4
            u = own * ((t // 2) % 2) + (1 - own) * (t % 2)
            is_far = own * (t % 2) + (1 - own) * ((t // 2) % 2)
            base = own * own_u + (1 - own) * peer_u + u * WY
            at = is_far * far + (1 - is_far) * near
            rows = pl.ds(_al(base, 512), WY)
            uc = pl.ds(_al(base, 128), WY)
            cols = pl.ds(_al(at, 128), 2 * IB)
            v = _dot_t(ei[k, :, cols], a[rows, cols])
            pu[:, uc] = v + jnp.where(is_far == 1, pu[:, uc], 0.0)

            @pl.when(t == 0)
            def _():
                for s in range(2, SX):
                    self.msg(GX, k, s).wait_recv()
                    self.msg(GF, k, s).start()

            @pl.when(t == 1)
            def _():
                for s in range(SX):
                    self.msg(GF, k, s).wait_recv()

            @pl.when((t == 2) | (t == 3))
            def _():
                self.msg(YR, k, t - 2).start()

            @pl.when(t == 3)
            def _():
                item_piece(0)

            @pl.when(t == 5)
            def _():
                item_piece(1)

            @pl.when(t == 6)
            def _():
                user_piece(0)
            return 0

        lax.fori_loop(0, 8, users_tile, 0)
        item_piece(2)
        user_piece(1)
        item_piece(3)

    def finish(self):
        k = STEPS - 1
        for s in range(SX):
            self.msg(FD, k, s).wait_send()
            self.msg(XR, k, s).wait_send()
            self.msg(FO, k, s).wait_send()
        for s in range(SY):
            self.msg(YR, k, s).wait_send()
        for k in range(STEPS):
            self.wait_puts(k)


class AllGather:
    def __init__(self, lk, ref, start, n_lo, n_hi, ss, rs):
        self.lk, self.ref, self.ss, self.rs = lk, ref, ss, rs
        self.full, self.lo, self.hi = pl.ds(start, n_lo + n_hi), pl.ds(start, n_lo), pl.ds(start + n_lo, n_hi)
        self.two = n_hi > 0

    def _copy(self, i):
        lk = self.lk
        xs, ys, ds_ = _slot_of(lk.xn), _slot_of(lk.yn), _slot_of(lk.diag)
        src_slot = (lk.slot, lk.slot, lk.slot, xs, ys, xs, ys, ds_, ds_)[i]
        dev = (lk.partner, lk.xn, lk.yn, lk.yn, lk.xn, lk.partner, lk.partner, lk.partner, lk.partner)[i]
        rows = (self.full, self.full, self.full, self.lo, self.hi, self.full, self.full, self.lo, self.hi)[i]
        ref = self.ref.at[src_slot, rows]
        return _remote(ref, ref, self.ss.at[i], self.rs.at[i], dev)

    def _used(self, i):
        return self.two or i not in (4, 8)

    def start(self):
        for i in (1, 2, 0):
            self._copy(i).start()

    def arrive(self, i):
        if not self._used(i):
            return
        self._copy(i).wait_recv()
        for j in {1: (3, 5), 2: (4, 6), 3: (7,), 4: (8,)}.get(i, ()):
            if self._used(j):
                self._copy(j).start()

    def slot(self, i):
        lk = self.lk
        c, x, h = lk.c, lk.x, lk.h
        row = {0: 2 * x + 1 - h, 1: 2 * (1 - x) + h, 2: lk.r, 4: 2 * (1 - x) + h,
               5: 2 * (1 - x) + 1 - h, 6: 2 * x + 1 - h, 8: 2 * (1 - x) + 1 - h}[i]
        col = {0: c, 1: c, 2: 1 - c, 4: 1 - c, 5: c, 6: 1 - c, 8: 1 - c}[i]
        return row * 2 + col

    def drain(self):
        for i in range(9):
            if self._used(i):
                self._copy(i).wait_send()


def _unpack_t(xt):
    n = xt.shape[1] // 2
    return jnp.concatenate([xt[:, :n], xt[:, n:]], axis=0).T


PROP_SCRATCH = [
    pltpu.VMEM((RU, CI), BF16),
    pltpu.VMEM((STEPS, D, CI), BF16),
    pltpu.VMEM((STEPS, D, RU), BF16),
    pltpu.VMEM((D, CI), F32),
    pltpu.VMEM((D, RU), F32),
    pltpu.VMEM((STEPS, D, IB), F32),
    pltpu.VMEM((STEPS, D, IB), F32),
    pltpu.VMEM((STEPS, D, IB), F32),
    pltpu.VMEM((STEPS, D, UB), F32),
    pltpu.SemaphoreType.DMA((STEPS, 8, 4)),
    pltpu.SemaphoreType.DMA((STEPS, 8, 4)),
]

CH = 64
NBUF = 4
NCH = RU // CH
AW = 8


def forward_kernel(mask, e0u, e0i, out_u, out_i, table, a_hbm,
                   a, ei, eu, pi, pu, rf, ro, rx, ry, ss, rs,
                   mbuf, msem, csum, rpart, dcol, drow, dss, drs, su, si, uacc, iacc, asem, iss, irs):
    lk = Links()

    def mask_copy(j):
        slot = j % NBUF
        return pltpu.make_async_copy(mask.at[pl.ds(_al(j * CH, CH), CH), :], mbuf.at[slot], msem.at[slot])

    for j in range(NBUF):
        mask_copy(j).start()
    lk.barrier()
    pr = Prop(lk, a, ei, eu, pi, pu, rf, ro, rx, ry, ss, rs)

    iacc[...] = e0i[...].astype(F32)
    for s in range(SX):
        pr.put_item(0, s, e0i[:, s * WX:(s + 1) * WX])
    uacc[...] = e0u[...].astype(F32)
    for s in range(SY):
        pr.put_user(0, s, e0u[:, s * WY:(s + 1) * WY])

    csum[...] = jnp.zeros_like(csum)

    def chunk(j, _):
        slot = j % NBUF
        mask_copy(j).wait()
        rows = pl.ds(_al(j * CH, CH), CH)

        def cols_body(w, acc):
            cols = pl.ds(_al(w * 512, 512), 512)
            v = mbuf[slot, :, cols].astype(F32)
            a[rows, cols] = v.astype(BF16)
            csum[:, cols] = csum[:, cols] + jnp.sum(v.reshape(CH // 8, 8, 512), axis=0)
            return acc + ((v[:, 0:128] + v[:, 128:256]) + (v[:, 256:384] + v[:, 384:512]))

        rpart[rows, :] = lax.fori_loop(0, CI // 512, cols_body, jnp.zeros((CH, 128), F32))

        @pl.when(j + NBUF < NCH)
        def _():
            mask_copy(j + NBUF).start()
        return 0

    lax.fori_loop(0, NCH, chunk, 0)

    ctot = jnp.sum(csum[...], axis=0, keepdims=True)
    for j in range(8):
        dcol[0, j:j + 1, :] = ctot[:, j * 1024:(j + 1) * 1024]
    drow[0] = _dot_t(jnp.ones((8, 128), BF16), rpart[...].astype(BF16))
    dcopies = [_remote(dcol.at[0], dcol.at[1 + i], dss.at[i], drs.at[i], dev)
               for i, dev in enumerate((lk.partner, lk.xn, lk.xpartner))]
    dcopies.append(_remote(drow.at[0], drow.at[1], dss.at[3], drs.at[3], lk.yn))
    for cp in dcopies:
        cp.start()
    for cp in dcopies:
        cp.wait_recv()
    ctot8 = (dcol[0] + dcol[1]) + (dcol[2] + dcol[3])
    sc8 = lax.rsqrt(jnp.maximum(ctot8, 1.0))
    for j in range(8):
        si[:, j * 1024:(j + 1) * 1024] = sc8[j:j + 1, :]
    su8 = lax.rsqrt(jnp.maximum(drow[0] + drow[1], 1.0))
    for j in range(RU // 128):
        su[j * 128:(j + 1) * 128, :] = jnp.broadcast_to(su8[0:1, j * 128:(j + 1) * 128], (128, 128)).T

    def a_copy(j):
        rows = pl.ds(_al(j * (RU // AW), RU // AW), RU // AW)
        return pltpu.make_async_copy(a.at[rows, :], a_hbm.at[rows, :], asem.at[j])

    def scale(first_col):
        def scale_rows(m, _):
            rows = pl.ds(_al(m * 64, 64), 64)
            s = su[rows, :]
            s4 = jnp.concatenate([s, s, s, s], axis=1)

            def scale_cols(w, _):
                cols = pl.ds(_al(first_col + w * 512, 512), 512)
                a[rows, cols] = a[rows, cols] * (s4 * si[:, cols]).astype(BF16)
                return 0

            lax.fori_loop(0, CI // 1024, scale_cols, 0)
            return 0

        lax.fori_loop(0, RU // 64, scale_rows, 0)

    def scale_near():
        scale(lk.x * 2 * IB)
        for j in range(AW):
            a_copy(j).start()

    scale((1 - lk.x) * 2 * IB)

    def user_final(k, s, v):
        b = v.astype(BF16)
        if k < STEPS - 1:
            pr.put_user(k + 1, s, b)
        uacc[:, s * WY:(s + 1) * WY] = uacc[:, s * WY:(s + 1) * WY] + b.astype(F32)
        if k == STEPS - 1 and s == SY - 1:
            t = uacc[...] * 0.25
            table[lk.slot, 0:PU, :] = _unpack_t(t).astype(BF16)
            ag_u.start()
            out_u[...] = t.astype(BF16)

    def item_final(k, s, v):
        b = v.astype(BF16)
        if k < STEPS - 1:
            pr.put_item(k + 1, s, b)
        iacc[:, s * WX:(s + 1) * WX] = iacc[:, s * WX:(s + 1) * WX] + b.astype(F32)
        if k == STEPS - 1:
            t = iacc[:, s * WX:(s + 1) * WX] * 0.25
            table[lk.slot, PU + s * WX // 2:PU + (s + 1) * WX // 2, :] = _unpack_t(t).astype(BF16)
            ags[s].start()
            out_i[:, s * WX:(s + 1) * WX] = t.astype(BF16)

    ags = [AllGather(lk, table, PU + s * WX // 2, WX // 2, 0, iss.at[s], irs.at[s]) for s in range(SX)]
    ag_u = AllGather(lk, table, 0, PU, 0, iss.at[SX], irs.at[SX])
    ags.append(ag_u)
    for k in range(STEPS):
        pr.step(k, user_final, item_final, scale_near if k == 0 else None)
    for group in ((1, 2), (3,), (0, 5, 6, 7)):
        for s in (SX, 0, 1, 2, 3):
            for i in group:
                ags[s].arrive(i)
    for cp in dcopies:
        cp.wait_send()
    for j in range(AW):
        a_copy(j).wait()
    pr.finish()
    for ag in ags:
        ag.drain()


def lookup_kernel(table_hbm, ids, out, table, tsem, tab, gu, gp, gn):
    def load(b):
        return pltpu.make_async_copy(table_hbm.at[b], table.at[b], tsem.at[b])

    for b in range(8):
        load(b).start()

    def unpack(b, _):
        load(b).wait()
        for lo, n, dst in [(0, PU, 0)] + [(PU + s * WX // 2, WX // 2, UB + s * WX) for s in range(SX)]:
            for o in range(0, n, 128):
                v = table[b, lo + o:lo + o + 128, :].astype(F32)
                base = b * (UB + IB) + dst + o
                tab[pl.ds(_al(base, 128), 128), :] = v
                tab[pl.ds(_al(base + n, 128), 128), :] = pltpu.roll(v, D, 1)
        return 0

    lax.fori_loop(0, 8, unpack, 0)

    def gather(g, _):
        for o in range(8):
            t = g * 8 + o
            gu[pl.ds(t, 1), :] = tab[pl.ds(ids[t], 1), :]
            gp[pl.ds(t, 1), :] = tab[pl.ds(ids[TB + t], 1), :]
            gn[pl.ds(t, 1), :] = tab[pl.ds(ids[2 * TB + t], 1), :]
        return 0

    lax.fori_loop(0, TB // 8, gather, 0)

    def block(m, tot):
        rows = pl.ds(_al(m * 256, 256), 256)
        left = lax.broadcasted_iota(jnp.int32, (256, 128), 1) < D
        e_u = gu[rows, :]
        e_d = gp[rows, :] - gn[rows, :]
        x = jnp.sum(jnp.where(left, e_u * e_d, 0.0), axis=1, keepdims=True)
        z = jnp.exp(-jnp.abs(x))
        loss = jnp.maximum(-x, 0.0) + jnp.log1p(z)
        sig = jnp.where(x >= 0.0, z, 1.0) / (1.0 + z)
        coef = sig * (-1.0 / NT)
        out[rows, :] = jnp.where(left, coef * e_d, pltpu.roll(coef * e_u, D, 1))
        return tot + jnp.sum(loss, axis=0, keepdims=True)

    tot = lax.fori_loop(0, TB // 256, block, jnp.zeros((1, 1), F32))
    out[TB:TB + 8, :] = jnp.broadcast_to(tot, (8, 128))


def backward_kernel(a_hbm, g_in, ids, out_u, out_i, out_l,
                    a, ei, eu, pi, pu, rf, ro, rx, ry, ss, rs,
                    asem, g_all, gsem, gss, grs, wu, wi, acc_u, acc_i, su, si):
    lk = Links()
    loads = [pltpu.make_async_copy(a_hbm, a, asem)]
    gcopy = pltpu.make_async_copy(g_in, g_all.at[lk.slot], gsem)
    gcopy.start()
    loads[0].start()
    lk.barrier()
    pr = Prop(lk, a, ei, eu, pi, pu, rf, ro, rx, ry, ss, rs)
    gcopy.wait()
    ag = AllGather(lk, g_all, 0, TB // 2, TB // 2 + 8, gss, grs)
    ag.start()
    acc_u[...] = jnp.zeros_like(acc_u)
    acc_i[...] = jnp.zeros_like(acc_i)
    base_u = lk.slot * UB
    base_i = (lk.c * 4 + lk.r) * IB

    def scatter(b):
        def split(m, _):
            rows = pl.ds(_al(m * 256, 256), 256)
            left = lax.broadcasted_iota(jnp.int32, (256, 128), 1) < D
            g = g_all[b, rows, :]
            hi = g.astype(BF16).astype(F32)
            r1 = g - hi
            mid = r1.astype(BF16).astype(F32)
            lo = r1 - mid
            wu[rows, 0:128] = jnp.where(left, hi, pltpu.roll(mid, D, 1)).astype(BF16)
            wu[rows, 128:256] = lo.astype(BF16)
            wi[rows, 0:128] = jnp.where(left, pltpu.roll(hi, D, 1), mid).astype(BF16)
            wi[rows, 128:256] = pltpu.roll(lo, D, 1).astype(BF16)
            return 0

        lax.fori_loop(0, TB // 256, split, 0)
        cols = pl.ds(_al(b * TB, 128), TB)
        sub = lax.broadcasted_iota(jnp.int32, (256, TB), 0).astype(F32).astype(BF16)
        one, zero = jnp.array(1.0, BF16), jnp.array(0.0, BF16)

        def lanes(which, base):
            v = ids[which:which + 1, cols] - base
            v = jnp.where((v >= 0) & (v < 256), v, -1).astype(F32)
            return jnp.broadcast_to(v, (256, TB)).astype(BF16)

        def hot(which, base):
            return jnp.concatenate([jnp.where(lanes(which, base + m * 256) == sub, one, zero) for m in range(4)], axis=0)

        acc_u[...] = acc_u[...] + _dot(hot(0, base_u), wu[...])

        def items(m, _):
            rows = pl.ds(_al(m * 1024, 1024), 1024)
            acc_i[rows, :] = acc_i[rows, :] + _dot(hot(1, base_i + m * 1024) - hot(2, base_i + m * 1024), wi[...])
            return 0

        lax.fori_loop(0, IB // 1024, items, 0)

    scatter(lk.slot)
    for group in ((0,), (1,), (2,), (5,), (6,), (3, 4), (7, 8)):
        for i in group:
            ag.arrive(i)
        scatter(ag.slot(group[-1]))

    loss = g_all[0, TB:TB + 8, :]
    for b in range(1, 8):
        loss = loss + g_all[b, TB:TB + 8, :]
    out_l[...] = loss * (1.0 / NT)

    def seed(acc):
        s = (acc[:, 0:128] + pltpu.roll(acc[:, 0:128], D, 1)) + acc[:, 128:256]
        n = s.shape[0] // 2
        s = s * 0.25
        left = lax.broadcasted_iota(jnp.int32, (n, 128), 1) < D
        return jnp.where(left, s[:n], pltpu.roll(s[n:], D, 1)).T

    xi = seed(acc_i[...])
    for s in range(SX):
        src = xi[:D] if s < SX // 2 else xi[D:]
        o = (s % (SX // 2)) * WX
        v = src[:, o:o + WX]
        si[:, s * WX:(s + 1) * WX] = v
        pr.put_item(0, s, v.astype(BF16))
    xu = seed(acc_u[...])
    for s in range(SY):
        v = xu[:D] if s == 0 else xu[D:]
        su[:, s * WY:(s + 1) * WY] = v
        pr.put_user(0, s, v.astype(BF16))

    def user_final(k, s, v):
        v = su[:, s * WY:(s + 1) * WY] + v
        if k < STEPS - 1:
            pr.put_user(k + 1, s, v.astype(BF16))
        else:
            out_u[:, s * WY:(s + 1) * WY] = v

    def item_final(k, s, v):
        v = si[:, s * WX:(s + 1) * WX] + v
        if k < STEPS - 1:
            pr.put_item(k + 1, s, v.astype(BF16))
        else:
            out_i[:, s * WX:(s + 1) * WX] = v

    loads[0].wait()
    for k in range(STEPS):
        pr.step(k, user_final, item_final)
    pr.finish()
    ag.drain()


def finish_kernel(*refs):
    for src, dst in zip(refs[:4], refs[5:9]):
        dst[...] = src[...]
    refs[9][...] = refs[4][0:1, 0:1]


VM = pl.BlockSpec(memory_space=pltpu.VMEM)
SM = pl.BlockSpec(memory_space=pltpu.SMEM)
ANY = pl.BlockSpec(memory_space=pl.ANY)
DMA = pltpu.SemaphoreType.DMA


def _params(cid):
    return pltpu.CompilerParams(collective_id=cid, has_side_effects=True, vmem_limit_bytes=VMEM_LIMIT)


def solution(mesh):
    def local_fn(mask, e0u, e0i, triples):
        c, r, _, _ = _coords()
        slot = r * 2 + c
        out_u, out_i, table, a_hbm = pl.pallas_call(
            forward_kernel,
            name='forward',
            out_shape=(jax.ShapeDtypeStruct((D, UB), BF16), jax.ShapeDtypeStruct((D, IB), BF16),
                       jax.ShapeDtypeStruct((8, PR, 128), BF16), jax.ShapeDtypeStruct((RU, CI), BF16)),
            in_specs=[ANY, VM, VM],
            out_specs=(VM, VM, VM, ANY),
            scratch_shapes=PROP_SCRATCH + [
                pltpu.VMEM((NBUF, CH, CI), jnp.int32), DMA((NBUF,)),
                pltpu.VMEM((8, CI), F32), pltpu.VMEM((RU, 128), F32),
                pltpu.VMEM((4, 8, 1024), F32), pltpu.VMEM((2, 8, RU), F32), DMA((4,)), DMA((4,)),
                pltpu.VMEM((RU, 128), F32), pltpu.VMEM((1, CI), F32),
                pltpu.VMEM((D, UB), F32), pltpu.VMEM((D, IB), F32), DMA((AW,)),
                DMA((SX + 1, 9)), DMA((SX + 1, 9)),
            ],
            compiler_params=_params(0),
        )(mask, e0u.T, e0i.T)

        cols = triples.T
        mine = lax.dynamic_slice(cols, (0, slot * TB), (3, TB))
        per = UB + IB
        blk = mine // IB
        row_i = ((blk % 4) * 2 + blk // 4) * per + UB + mine % IB
        row_u = (mine // UB) * per + mine % UB
        ids = jnp.where(lax.broadcasted_iota(jnp.int32, (3, TB), 0) == 0, row_u, row_i)
        g = pl.pallas_call(
            lookup_kernel,
            name='lookup',
            out_shape=jax.ShapeDtypeStruct((TB + 8, 128), F32),
            in_specs=[ANY, SM],
            out_specs=VM,
            scratch_shapes=[pltpu.VMEM((8, PR, 128), BF16), DMA((8,)), pltpu.VMEM((8 * per, 128), F32)] + [pltpu.VMEM((TB, 128), F32)] * 3,
            compiler_params=pltpu.CompilerParams(vmem_limit_bytes=VMEM_LIMIT),
        )(table, ids.reshape(-1))

        d_u, d_i, loss = pl.pallas_call(
            backward_kernel,
            name='backward',
            out_shape=(jax.ShapeDtypeStruct((D, UB), F32), jax.ShapeDtypeStruct((D, IB), F32),
                       jax.ShapeDtypeStruct((8, 128), F32)),
            in_specs=[ANY, ANY, VM],
            out_specs=(VM, VM, VM),
            scratch_shapes=PROP_SCRATCH + [
                DMA, pltpu.VMEM((8, TB + 8, 128), F32), DMA, DMA((9,)), DMA((9,)),
                pltpu.VMEM((TB, 256), BF16), pltpu.VMEM((TB, 256), BF16),
                pltpu.VMEM((UB, 256), F32), pltpu.VMEM((IB, 256), F32),
                pltpu.VMEM((D, UB), F32), pltpu.VMEM((D, IB), F32),
            ],
            compiler_params=_params(1),
        )(a_hbm, g, cols)
        outs = (out_u, out_i, d_u, d_i)
        out_u, out_i, d_u, d_i, loss = pl.pallas_call(
            finish_kernel,
            name='finish',
            out_shape=tuple(jax.ShapeDtypeStruct(o.shape, o.dtype) for o in outs) + (jax.ShapeDtypeStruct((1, 1), F32),),
            in_specs=[VM] * 5,
            out_specs=(VM,) * 5,
        )(*outs, loss)
        return out_u.T, out_i.T, loss.reshape(()), d_u.T, d_i.T

    user_spec = P(('row', 'col'), None)
    item_spec = P(('col', 'row'), None)
    return jax.shard_map(local_fn, mesh=mesh, in_specs=(P('row', 'col'), user_spec, item_spec, P()),
                         out_specs=(user_spec, item_spec, P(), user_spec, item_spec), check_vma=False)
```

```python
import jax
import jax.numpy as jnp
from jax import lax
from jax.experimental import pallas as pl
from jax.experimental.pallas import tpu as pltpu
from jax.sharding import PartitionSpec as P

MESH = pl.DeviceIdType.MESH
F32 = jnp.float32
BF16 = jnp.bfloat16

D = 64
UB = 1024
IB = 2048
RU = 2048
CI = 8192
STEPS = 3
SX = 4
WX = IB // SX
SY = 2
WY = UB // SY
TB = 1024
NT = 8192
PU = UB // 2
PI = IB // 2
PR = PU + PI

FD, XR, FO, GP, GX, GF, YR, YG = range(8)
VMEM_LIMIT = 67043328


def _coords():
    c = lax.axis_index('col')
    r = lax.axis_index('row')
    x = r // 2
    h = r % 2
    return c, r, x, h


def _dot(a, b):
    return lax.dot_general(a, b, (((1,), (0,)), ((), ())), preferred_element_type=F32)


def _dot_t(a, b):
    return lax.dot_general(a, b, (((1,), (1,)), ((), ())), preferred_element_type=F32)


def _al(v, m):
    return pl.multiple_of(v, m)


class Links:
    def __init__(self):
        self.c, self.r, self.x, self.h = _coords()
        c, r, x, h = self.c, self.r, self.x, self.h
        self.partner = (c, 2 * x + (1 - h))
        self.xn = (c, 2 * (1 - x) + h)
        self.yn = (1 - c, r)
        self.diag = (1 - c, 2 * (1 - x) + h)
        self.xpartner = (c, 2 * (1 - x) + (1 - h))
        self.slot = r * 2 + c

    def barrier(self):
        sem = pltpu.get_barrier_semaphore()
        peers = (self.partner, self.xn, self.yn, self.diag, self.xpartner)
        for p in peers:
            pl.semaphore_signal(sem, inc=1, device_id=p, device_id_type=MESH)
        pl.semaphore_wait(sem, len(peers))


def _slot_of(dev):
    return dev[1] * 2 + dev[0]


def _remote(src, dst, ss, rs, dev):
    return pltpu.make_async_remote_copy(src_ref=src, dst_ref=dst, send_sem=ss, recv_sem=rs, device_id=dev, device_id_type=MESH)


class Prop:
    def __init__(self, lk, a, ei, eu, pi, pu, rf, ro, rx, ry, ss, rs):
        self.lk = lk
        self.a, self.ei, self.eu, self.pi, self.pu = a, ei, eu, pi, pu
        self.rf, self.ro, self.rx, self.ry = rf, ro, rx, ry
        self.ss, self.rs = ss, rs
        pu[...] = jnp.zeros_like(pu)

    def msg(self, kind, k, s):
        lk = self.lk
        ss, rs = self.ss.at[k, kind, s], self.rs.at[k, kind, s]
        other = 1 - lk.x
        if kind == FD:
            src = self.pi.at[:, pl.ds(_al((2 * other + 1 - lk.h) * IB + s * WX, 128), WX)]
            dst = self.rf.at[k, :, pl.ds(_al(s * WX, 128), WX)]
            return _remote(src, dst, ss, rs, lk.partner)
        if kind == XR:
            src = self.pi.at[:, pl.ds(_al((2 * other + lk.h) * IB + s * WX, 128), WX)]
            dst = self.rx.at[k, :, pl.ds(_al(s * WX, 128), WX)]
            return _remote(src, dst, ss, rs, lk.xn)
        if kind == FO:
            src = self.pi.at[:, pl.ds(_al((2 * lk.x + 1 - lk.h) * IB + s * WX, 128), WX)]
            dst = self.ro.at[k, :, pl.ds(_al(s * WX, 128), WX)]
            return _remote(src, dst, ss, rs, lk.partner)
        if kind in (GP, GX):
            ref = self.ei.at[k, :, pl.ds(_al(lk.r * IB + s * WX, 128), WX)]
            return _remote(ref, ref, ss, rs, lk.partner if kind == GP else lk.xn)
        if kind == GF:
            ref = self.ei.at[k, :, pl.ds(_al((2 * other + lk.h) * IB + s * WX, 128), WX)]
            return _remote(ref, ref, ss, rs, lk.partner)
        if kind == YR:
            src = self.pu.at[:, pl.ds(_al((1 - lk.c) * UB + s * WY, 128), WY)]
            dst = self.ry.at[k, :, pl.ds(_al(s * WY, 128), WY)]
            return _remote(src, dst, ss, rs, lk.yn)
        ref = self.eu.at[k, :, pl.ds(_al(lk.c * UB + s * WY, 128), WY)]
        return _remote(ref, ref, ss, rs, lk.yn)

    def put_item(self, k, s, value):
        self.ei[k, :, pl.ds(_al(self.lk.r * IB + s * WX, 128), WX)] = value
        self.msg(GX, k, s).start()
        self.msg(GP, k, s).start()

    def put_user(self, k, s, value):
        self.eu[k, :, pl.ds(_al(self.lk.c * UB + s * WY, 128), WY)] = value
        self.msg(YG, k, s).start()

    def wait_puts(self, k):
        for s in range(SX):
            self.msg(GX, k, s).wait_send()
            self.msg(GP, k, s).wait_send()
            if k == STEPS - 1:
                self.msg(GF, k, s).wait_send()
        for s in range(SY):
            self.msg(YG, k, s).wait_send()

    def step(self, k, user_final, item_final, between=None):
        lk = self.lk
        a, ei, eu, pi, pu = self.a, self.ei, self.eu, self.pi, self.pu
        far = (1 - lk.x) * 2 * IB
        near = lk.x * 2 * IB
        own_u = lk.c * UB
        peer_u = (1 - lk.c) * UB

        if k > 0:
            for s in range(SX):
                self.msg(FD, k - 1, s).wait_send()
                self.msg(XR, k - 1, s).wait_send()
                self.msg(FO, k - 1, s).wait_send()
                self.msg(GF, k - 1, s).wait_send()
        own_rows = pl.ds(_al(own_u, 128), UB)
        peer_rows = pl.ds(_al(peer_u, 128), UB)

        def over_own(j, _):
            cols = pl.ds(_al(far + j * (near - far), 128), 2 * IB)
            pi[:, cols] = _dot(eu[k, :, own_rows], a[own_rows, cols])
            return 0

        late_near = between is not None
        lax.fori_loop(0, 1 if late_near else 2, over_own, 0)
        for s in range(SY):
            self.msg(YG, k, s).wait_recv()

        def over_peer(stage, _):
            is_far = 1 - (stage // 2 if late_near else stage % 2)
            mine = stage % 2 if late_near else stage // 2
            half = mine * lk.h + (1 - mine) * (1 - lk.h)
            cols = pl.ds(_al(is_far * far + (1 - is_far) * near + half * IB, 128), IB)
            pi[:, cols] = pi[:, cols] + _dot(eu[k, :, peer_rows], a[peer_rows, cols])

            @pl.when(is_far * (1 - mine) == 1)
            def _():
                for s in range(SX):
                    self.msg(FD, k, s).start()

            @pl.when((1 - is_far) * (1 - mine) == 1)
            def _():
                for s in range(SX):
                    self.msg(FO, k, s).start()

            @pl.when(is_far * mine == 1)
            def _():
                for s in range(SX):
                    self.msg(FD, k, s).wait_recv()
                    cs = pl.ds(_al(far + lk.h * IB + s * WX, 128), WX)
                    pi[:, cs] = pi[:, cs] + self.rf[k, :, s * WX:(s + 1) * WX]
                    self.msg(XR, k, s).start()

            @pl.when((1 - is_far) * mine == 1)
            def _():
                for s in range(2):
                    self.msg(GX, k, s).wait_recv()
                    self.msg(GF, k, s).start()
            return 0

        if late_near:
            lax.fori_loop(0, 2, over_peer, 0)
            between()
            lax.fori_loop(1, 2, over_own, 0)
            lax.fori_loop(2, 4, over_peer, 0)
        else:
            lax.fori_loop(0, 4, over_peer, 0)

        if k > 0:
            for s in range(SY):
                self.msg(YR, k - 1, s).wait_send()
        for s in range(SX):
            self.msg(GP, k, s).wait_recv()

        def item_piece(s):
            self.msg(FO, k, s).wait_recv()
            self.msg(XR, k, s).wait_recv()
            c2 = pl.ds(_al(near + lk.h * IB + s * WX, 128), WX)
            piece = pl.ds(_al(s * WX, 128), WX)
            item_final(k, s, (pi[:, c2] + self.ro[k, :, piece]) + self.rx[k, :, piece])

        def user_piece(s):
            self.msg(YR, k, s).wait_recv()
            uc = pl.ds(_al(own_u + s * WY, 128), WY)
            user_final(k, s, pu[:, uc] + self.ry[k, :, s * WY:(s + 1) * WY])

        def users_tile(t, _):
            own = t // 4
            u = own * ((t // 2) % 2) + (1 - own) * (t % 2)
            is_far = own * (t % 2) + (1 - own) * ((t // 2) % 2)
            base = own * own_u + (1 - own) * peer_u + u * WY
            at = is_far * far + (1 - is_far) * near
            rows = pl.ds(_al(base, 512), WY)
            uc = pl.ds(_al(base, 128), WY)
            cols = pl.ds(_al(at, 128), 2 * IB)
            v = _dot_t(ei[k, :, cols], a[rows, cols])
            pu[:, uc] = v + jnp.where(is_far == 1, pu[:, uc], 0.0)

            @pl.when(t == 0)
            def _():
                for s in range(2, SX):
                    self.msg(GX, k, s).wait_recv()
                    self.msg(GF, k, s).start()

            @pl.when(t == 1)
            def _():
                for s in range(SX):
                    self.msg(GF, k, s).wait_recv()

            @pl.when((t == 2) | (t == 3))
            def _():
                self.msg(YR, k, t - 2).start()

            @pl.when(t == 3)
            def _():
                item_piece(0)

            @pl.when(t == 5)
            def _():
                item_piece(1)

            @pl.when(t == 6)
            def _():
                user_piece(0)
            return 0

        lax.fori_loop(0, 8, users_tile, 0)
        item_piece(2)
        user_piece(1)
        item_piece(3)

    def finish(self):
        k = STEPS - 1
        for s in range(SX):
            self.msg(FD, k, s).wait_send()
            self.msg(XR, k, s).wait_send()
            self.msg(FO, k, s).wait_send()
        for s in range(SY):
            self.msg(YR, k, s).wait_send()
        for k in range(STEPS):
            self.wait_puts(k)


class AllGather:
    def __init__(self, lk, ref, start, n_lo, n_hi, ss, rs):
        self.lk, self.ref, self.ss, self.rs = lk, ref, ss, rs
        self.full, self.lo, self.hi = pl.ds(start, n_lo + n_hi), pl.ds(start, n_lo), pl.ds(start + n_lo, n_hi)
        self.two = n_hi > 0

    def _copy(self, i):
        lk = self.lk
        xs, ys, ds_ = _slot_of(lk.xn), _slot_of(lk.yn), _slot_of(lk.diag)
        src_slot = (lk.slot, lk.slot, lk.slot, xs, ys, xs, ys, ds_, ds_)[i]
        dev = (lk.partner, lk.xn, lk.yn, lk.yn, lk.xn, lk.partner, lk.partner, lk.partner, lk.partner)[i]
        rows = (self.full, self.full, self.full, self.lo, self.hi, self.full, self.full, self.lo, self.hi)[i]
        ref = self.ref.at[src_slot, rows]
        return _remote(ref, ref, self.ss.at[i], self.rs.at[i], dev)

    def _used(self, i):
        return self.two or i not in (4, 8)

    def start(self):
        for i in (1, 2, 0):
            self._copy(i).start()

    def arrive(self, i):
        if not self._used(i):
            return
        self._copy(i).wait_recv()
        for j in {1: (3, 5), 2: (4, 6), 3: (7,), 4: (8,)}.get(i, ()):
            if self._used(j):
                self._copy(j).start()

    def slot(self, i):
        lk = self.lk
        c, x, h = lk.c, lk.x, lk.h
        row = {0: 2 * x + 1 - h, 1: 2 * (1 - x) + h, 2: lk.r, 4: 2 * (1 - x) + h,
               5: 2 * (1 - x) + 1 - h, 6: 2 * x + 1 - h, 8: 2 * (1 - x) + 1 - h}[i]
        col = {0: c, 1: c, 2: 1 - c, 4: 1 - c, 5: c, 6: 1 - c, 8: 1 - c}[i]
        return row * 2 + col

    def drain(self):
        for i in range(9):
            if self._used(i):
                self._copy(i).wait_send()


def _unpack_t(xt):
    n = xt.shape[1] // 2
    return jnp.concatenate([xt[:, :n], xt[:, n:]], axis=0).T


PROP_SCRATCH = [
    pltpu.VMEM((RU, CI), BF16),
    pltpu.VMEM((STEPS, D, CI), BF16),
    pltpu.VMEM((STEPS, D, RU), BF16),
    pltpu.VMEM((D, CI), F32),
    pltpu.VMEM((D, RU), F32),
    pltpu.VMEM((STEPS, D, IB), F32),
    pltpu.VMEM((STEPS, D, IB), F32),
    pltpu.VMEM((STEPS, D, IB), F32),
    pltpu.VMEM((STEPS, D, UB), F32),
    pltpu.SemaphoreType.DMA((STEPS, 8, 4)),
    pltpu.SemaphoreType.DMA((STEPS, 8, 4)),
]

CH = 64
NBUF = 4
NCH = RU // CH
AW = 8


def forward_kernel(mask, e0u, e0i, out_u, out_i, table, a_hbm,
                   a, ei, eu, pi, pu, rf, ro, rx, ry, ss, rs,
                   mbuf, msem, csum, rpart, dcol, drow, dss, drs, su, si, uacc, iacc, asem, iss, irs):
    lk = Links()

    def mask_copy(j):
        slot = j % NBUF
        return pltpu.make_async_copy(mask.at[pl.ds(_al(j * CH, CH), CH), :], mbuf.at[slot], msem.at[slot])

    for j in range(NBUF):
        mask_copy(j).start()
    lk.barrier()
    pr = Prop(lk, a, ei, eu, pi, pu, rf, ro, rx, ry, ss, rs)

    iacc[...] = e0i[...].astype(F32)
    for s in range(SX):
        pr.put_item(0, s, e0i[:, s * WX:(s + 1) * WX])
    uacc[...] = e0u[...].astype(F32)
    for s in range(SY):
        pr.put_user(0, s, e0u[:, s * WY:(s + 1) * WY])

    csum[...] = jnp.zeros_like(csum)

    def chunk(j, _):
        slot = j % NBUF
        mask_copy(j).wait()
        rows = pl.ds(_al(j * CH, CH), CH)

        def cols_body(w, acc):
            cols = pl.ds(_al(w * 512, 512), 512)
            v = mbuf[slot, :, cols].astype(F32)
            a[rows, cols] = v.astype(BF16)
            csum[:, cols] = csum[:, cols] + jnp.sum(v.reshape(CH // 8, 8, 512), axis=0)
            return acc + ((v[:, 0:128] + v[:, 128:256]) + (v[:, 256:384] + v[:, 384:512]))

        rpart[rows, :] = lax.fori_loop(0, CI // 512, cols_body, jnp.zeros((CH, 128), F32))

        @pl.when(j + NBUF < NCH)
        def _():
            mask_copy(j + NBUF).start()
        return 0

    lax.fori_loop(0, NCH, chunk, 0)

    ctot = jnp.sum(csum[...], axis=0, keepdims=True)
    for j in range(8):
        dcol[0, j:j + 1, :] = ctot[:, j * 1024:(j + 1) * 1024]
    drow[0] = _dot_t(jnp.ones((8, 128), BF16), rpart[...].astype(BF16))
    dcopies = [_remote(dcol.at[0], dcol.at[1 + i], dss.at[i], drs.at[i], dev)
               for i, dev in enumerate((lk.partner, lk.xn, lk.xpartner))]
    dcopies.append(_remote(drow.at[0], drow.at[1], dss.at[3], drs.at[3], lk.yn))
    for cp in dcopies:
        cp.start()
    for cp in dcopies:
        cp.wait_recv()
    ctot8 = (dcol[0] + dcol[1]) + (dcol[2] + dcol[3])
    sc8 = lax.rsqrt(jnp.maximum(ctot8, 1.0))
    for j in range(8):
        si[:, j * 1024:(j + 1) * 1024] = sc8[j:j + 1, :]
    su8 = lax.rsqrt(jnp.maximum(drow[0] + drow[1], 1.0))
    for j in range(RU // 128):
        su[j * 128:(j + 1) * 128, :] = jnp.broadcast_to(su8[0:1, j * 128:(j + 1) * 128], (128, 128)).T

    def a_copy(j):
        rows = pl.ds(_al(j * (RU // AW), RU // AW), RU // AW)
        return pltpu.make_async_copy(a.at[rows, :], a_hbm.at[rows, :], asem.at[j])

    def scale(first_col):
        def scale_rows(m, _):
            rows = pl.ds(_al(m * 64, 64), 64)
            s = su[rows, :]
            s4 = jnp.concatenate([s, s, s, s], axis=1)

            def scale_cols(w, _):
                cols = pl.ds(_al(first_col + w * 512, 512), 512)
                a[rows, cols] = a[rows, cols] * (s4 * si[:, cols]).astype(BF16)
                return 0

            lax.fori_loop(0, CI // 1024, scale_cols, 0)
            return 0

        lax.fori_loop(0, RU // 64, scale_rows, 0)

    def scale_near():
        scale(lk.x * 2 * IB)
        for j in range(AW):
            a_copy(j).start()

    scale((1 - lk.x) * 2 * IB)

    def user_final(k, s, v):
        b = v.astype(BF16)
        if k < STEPS - 1:
            pr.put_user(k + 1, s, b)
        uacc[:, s * WY:(s + 1) * WY] = uacc[:, s * WY:(s + 1) * WY] + b.astype(F32)
        if k == STEPS - 1 and s == SY - 1:
            t = uacc[...] * 0.25
            table[lk.slot, 0:PU, :] = _unpack_t(t).astype(BF16)
            ag_u.start()
            out_u[...] = t.astype(BF16)

    def item_final(k, s, v):
        b = v.astype(BF16)
        if k < STEPS - 1:
            pr.put_item(k + 1, s, b)
        iacc[:, s * WX:(s + 1) * WX] = iacc[:, s * WX:(s + 1) * WX] + b.astype(F32)
        if k == STEPS - 1:
            t = iacc[:, s * WX:(s + 1) * WX] * 0.25
            table[lk.slot, PU + s * WX // 2:PU + (s + 1) * WX // 2, :] = _unpack_t(t).astype(BF16)
            ags[s].start()
            out_i[:, s * WX:(s + 1) * WX] = t.astype(BF16)

    ags = [AllGather(lk, table, PU + s * WX // 2, WX // 4, WX // 4, iss.at[s], irs.at[s]) for s in range(SX)]
    ag_u = AllGather(lk, table, 0, PU // 2, PU // 2, iss.at[SX], irs.at[SX])
    ags.append(ag_u)
    for k in range(STEPS):
        pr.step(k, user_final, item_final, scale_near if k == 0 else None)
    for group in ((1, 2), (3, 4), (0, 5, 6, 7, 8)):
        for s in (SX, 0, 1, 2, 3):
            for i in group:
                ags[s].arrive(i)
    for cp in dcopies:
        cp.wait_send()
    for j in range(AW):
        a_copy(j).wait()
    pr.finish()
    for ag in ags:
        ag.drain()


def lookup_kernel(table_hbm, ids, out, table, tsem, tab, gu, gp, gn):
    def load(b):
        return pltpu.make_async_copy(table_hbm.at[b], table.at[b], tsem.at[b])

    for b in range(8):
        load(b).start()

    def unpack(b, _):
        load(b).wait()
        for lo, n, dst in [(0, PU, 0)] + [(PU + s * WX // 2, WX // 2, UB + s * WX) for s in range(SX)]:
            for o in range(0, n, 128):
                v = table[b, lo + o:lo + o + 128, :].astype(F32)
                base = b * (UB + IB) + dst + o
                tab[pl.ds(_al(base, 128), 128), :] = v
                tab[pl.ds(_al(base + n, 128), 128), :] = pltpu.roll(v, D, 1)
        return 0

    lax.fori_loop(0, 8, unpack, 0)

    def gather(g, _):
        for o in range(8):
            t = g * 8 + o
            gu[pl.ds(t, 1), :] = tab[pl.ds(ids[t], 1), :]
            gp[pl.ds(t, 1), :] = tab[pl.ds(ids[TB + t], 1), :]
            gn[pl.ds(t, 1), :] = tab[pl.ds(ids[2 * TB + t], 1), :]
        return 0

    lax.fori_loop(0, TB // 8, gather, 0)

    def block(m, tot):
        rows = pl.ds(_al(m * 256, 256), 256)
        left = lax.broadcasted_iota(jnp.int32, (256, 128), 1) < D
        e_u = gu[rows, :]
        e_d = gp[rows, :] - gn[rows, :]
        x = jnp.sum(jnp.where(left, e_u * e_d, 0.0), axis=1, keepdims=True)
        z = jnp.exp(-jnp.abs(x))
        loss = jnp.maximum(-x, 0.0) + jnp.log1p(z)
        sig = jnp.where(x >= 0.0, z, 1.0) / (1.0 + z)
        coef = sig * (-1.0 / NT)
        out[rows, :] = jnp.where(left, coef * e_d, pltpu.roll(coef * e_u, D, 1))
        return tot + jnp.sum(loss, axis=0, keepdims=True)

    tot = lax.fori_loop(0, TB // 256, block, jnp.zeros((1, 1), F32))
    out[TB:TB + 8, :] = jnp.broadcast_to(tot, (8, 128))


def backward_kernel(a_hbm, g_in, ids, out_u, out_i, out_l,
                    a, ei, eu, pi, pu, rf, ro, rx, ry, ss, rs,
                    asem, g_all, gsem, gss, grs, wu, wi, acc_u, acc_i, su, si):
    lk = Links()
    loads = [pltpu.make_async_copy(a_hbm, a, asem)]
    gcopy = pltpu.make_async_copy(g_in, g_all.at[lk.slot], gsem)
    gcopy.start()
    loads[0].start()
    lk.barrier()
    pr = Prop(lk, a, ei, eu, pi, pu, rf, ro, rx, ry, ss, rs)
    gcopy.wait()
    ag = AllGather(lk, g_all, 0, TB // 2, TB // 2 + 8, gss, grs)
    ag.start()
    acc_u[...] = jnp.zeros_like(acc_u)
    acc_i[...] = jnp.zeros_like(acc_i)
    base_u = lk.slot * UB
    base_i = (lk.c * 4 + lk.r) * IB

    def scatter(b):
        def split(m, _):
            rows = pl.ds(_al(m * 256, 256), 256)
            left = lax.broadcasted_iota(jnp.int32, (256, 128), 1) < D
            g = g_all[b, rows, :]
            hi = g.astype(BF16).astype(F32)
            r1 = g - hi
            mid = r1.astype(BF16).astype(F32)
            lo = r1 - mid
            wu[rows, 0:128] = jnp.where(left, hi, pltpu.roll(mid, D, 1)).astype(BF16)
            wu[rows, 128:256] = lo.astype(BF16)
            wi[rows, 0:128] = jnp.where(left, pltpu.roll(hi, D, 1), mid).astype(BF16)
            wi[rows, 128:256] = pltpu.roll(lo, D, 1).astype(BF16)
            return 0

        lax.fori_loop(0, TB // 256, split, 0)
        cols = pl.ds(_al(b * TB, 128), TB)
        sub = lax.broadcasted_iota(jnp.int32, (256, TB), 0).astype(F32).astype(BF16)
        one, zero = jnp.array(1.0, BF16), jnp.array(0.0, BF16)

        def lanes(which, base):
            v = ids[which:which + 1, cols] - base
            v = jnp.where((v >= 0) & (v < 256), v, -1).astype(F32)
            return jnp.broadcast_to(v, (256, TB)).astype(BF16)

        def hot(which, base):
            return jnp.concatenate([jnp.where(lanes(which, base + m * 256) == sub, one, zero) for m in range(4)], axis=0)

        acc_u[...] = acc_u[...] + _dot(hot(0, base_u), wu[...])

        def items(m, _):
            rows = pl.ds(_al(m * 1024, 1024), 1024)
            acc_i[rows, :] = acc_i[rows, :] + _dot(hot(1, base_i + m * 1024) - hot(2, base_i + m * 1024), wi[...])
            return 0

        lax.fori_loop(0, IB // 1024, items, 0)

    scatter(lk.slot)
    for group, done in (((0,), 0), ((1, 2), 1), ((), 2), ((5,), 5), ((3, 4, 6), 6), ((), 4), ((7, 8), 8)):
        for i in group:
            ag.arrive(i)
        scatter(ag.slot(done))

    loss = g_all[0, TB:TB + 8, :]
    for b in range(1, 8):
        loss = loss + g_all[b, TB:TB + 8, :]
    out_l[...] = loss * (1.0 / NT)

    def seed(acc):
        s = (acc[:, 0:128] + pltpu.roll(acc[:, 0:128], D, 1)) + acc[:, 128:256]
        n = s.shape[0] // 2
        s = s * 0.25
        left = lax.broadcasted_iota(jnp.int32, (n, 128), 1) < D
        return jnp.where(left, s[:n], pltpu.roll(s[n:], D, 1)).T

    xi = seed(acc_i[...])
    for s in range(SX):
        src = xi[:D] if s < SX // 2 else xi[D:]
        o = (s % (SX // 2)) * WX
        v = src[:, o:o + WX]
        si[:, s * WX:(s + 1) * WX] = v
        pr.put_item(0, s, v.astype(BF16))
    xu = seed(acc_u[...])
    for s in range(SY):
        v = xu[:D] if s == 0 else xu[D:]
        su[:, s * WY:(s + 1) * WY] = v
        pr.put_user(0, s, v.astype(BF16))

    def user_final(k, s, v):
        v = su[:, s * WY:(s + 1) * WY] + v
        if k < STEPS - 1:
            pr.put_user(k + 1, s, v.astype(BF16))
        else:
            out_u[:, s * WY:(s + 1) * WY] = v

    def item_final(k, s, v):
        v = si[:, s * WX:(s + 1) * WX] + v
        if k < STEPS - 1:
            pr.put_item(k + 1, s, v.astype(BF16))
        else:
            out_i[:, s * WX:(s + 1) * WX] = v

    loads[0].wait()
    for k in range(STEPS):
        pr.step(k, user_final, item_final)
    pr.finish()
    ag.drain()


def finish_kernel(*refs):
    for src, dst in zip(refs[:4], refs[5:9]):
        dst[...] = src[...]
    refs[9][...] = refs[4][0:1, 0:1]


VM = pl.BlockSpec(memory_space=pltpu.VMEM)
SM = pl.BlockSpec(memory_space=pltpu.SMEM)
ANY = pl.BlockSpec(memory_space=pl.ANY)
DMA = pltpu.SemaphoreType.DMA


def _params(cid):
    return pltpu.CompilerParams(collective_id=cid, has_side_effects=True, vmem_limit_bytes=VMEM_LIMIT)


def solution(mesh):
    def local_fn(mask, e0u, e0i, triples):
        c, r, _, _ = _coords()
        slot = r * 2 + c
        out_u, out_i, table, a_hbm = pl.pallas_call(
            forward_kernel,
            name='forward',
            out_shape=(jax.ShapeDtypeStruct((D, UB), BF16), jax.ShapeDtypeStruct((D, IB), BF16),
                       jax.ShapeDtypeStruct((8, PR, 128), BF16), jax.ShapeDtypeStruct((RU, CI), BF16)),
            in_specs=[ANY, VM, VM],
            out_specs=(VM, VM, VM, ANY),
            scratch_shapes=PROP_SCRATCH + [
                pltpu.VMEM((NBUF, CH, CI), jnp.int32), DMA((NBUF,)),
                pltpu.VMEM((8, CI), F32), pltpu.VMEM((RU, 128), F32),
                pltpu.VMEM((4, 8, 1024), F32), pltpu.VMEM((2, 8, RU), F32), DMA((4,)), DMA((4,)),
                pltpu.VMEM((RU, 128), F32), pltpu.VMEM((1, CI), F32),
                pltpu.VMEM((D, UB), F32), pltpu.VMEM((D, IB), F32), DMA((AW,)),
                DMA((SX + 1, 9)), DMA((SX + 1, 9)),
            ],
            compiler_params=_params(0),
        )(mask, e0u.T, e0i.T)

        cols = triples.T
        mine = lax.dynamic_slice(cols, (0, slot * TB), (3, TB))
        per = UB + IB
        blk = mine // IB
        row_i = ((blk % 4) * 2 + blk // 4) * per + UB + mine % IB
        row_u = (mine // UB) * per + mine % UB
        ids = jnp.where(lax.broadcasted_iota(jnp.int32, (3, TB), 0) == 0, row_u, row_i)
        g = pl.pallas_call(
            lookup_kernel,
            name='lookup',
            out_shape=jax.ShapeDtypeStruct((TB + 8, 128), F32),
            in_specs=[ANY, SM],
            out_specs=VM,
            scratch_shapes=[pltpu.VMEM((8, PR, 128), BF16), DMA((8,)), pltpu.VMEM((8 * per, 128), F32)] + [pltpu.VMEM((TB, 128), F32)] * 3,
            compiler_params=pltpu.CompilerParams(vmem_limit_bytes=VMEM_LIMIT),
        )(table, ids.reshape(-1))

        d_u, d_i, loss = pl.pallas_call(
            backward_kernel,
            name='backward',
            out_shape=(jax.ShapeDtypeStruct((D, UB), F32), jax.ShapeDtypeStruct((D, IB), F32),
                       jax.ShapeDtypeStruct((8, 128), F32)),
            in_specs=[ANY, ANY, VM],
            out_specs=(VM, VM, VM),
            scratch_shapes=PROP_SCRATCH + [
                DMA, pltpu.VMEM((8, TB + 8, 128), F32), DMA, DMA((9,)), DMA((9,)),
                pltpu.VMEM((TB, 256), BF16), pltpu.VMEM((TB, 256), BF16),
                pltpu.VMEM((UB, 256), F32), pltpu.VMEM((IB, 256), F32),
                pltpu.VMEM((D, UB), F32), pltpu.VMEM((D, IB), F32),
            ],
            compiler_params=_params(1),
        )(a_hbm, g, cols)
        outs = (out_u, out_i, d_u, d_i)
        out_u, out_i, d_u, d_i, loss = pl.pallas_call(
            finish_kernel,
            name='finish',
            out_shape=tuple(jax.ShapeDtypeStruct(o.shape, o.dtype) for o in outs) + (jax.ShapeDtypeStruct((1, 1), F32),),
            in_specs=[VM] * 5,
            out_specs=(VM,) * 5,
        )(*outs, loss)
        return out_u.T, out_i.T, loss.reshape(()), d_u.T, d_i.T

    user_spec = P(('row', 'col'), None)
    item_spec = P(('col', 'row'), None)
    return jax.shard_map(local_fn, mesh=mesh, in_specs=(P('row', 'col'), user_spec, item_spec, P()),
                         out_specs=(user_spec, item_spec, P(), user_spec, item_spec), check_vma=False)
```

```python
import jax
import jax.numpy as jnp
from jax import lax
from jax.experimental import pallas as pl
from jax.experimental.pallas import tpu as pltpu
from jax.sharding import PartitionSpec as P

MESH = pl.DeviceIdType.MESH
F32 = jnp.float32
BF16 = jnp.bfloat16

D = 64
UB = 1024
IB = 2048
RU = 2048
CI = 8192
STEPS = 3
SX = 4
WX = IB // SX
SY = 2
WY = UB // SY
TB = 1024
NT = 8192
PU = UB // 2
PI = IB // 2
PR = PU + PI

FD, XR, FO, GP, GX, GF, YR, YG = range(8)
VMEM_LIMIT = 67043328


def _coords():
    c = lax.axis_index('col')
    r = lax.axis_index('row')
    x = r // 2
    h = r % 2
    return c, r, x, h


def _dot(a, b):
    return lax.dot_general(a, b, (((1,), (0,)), ((), ())), preferred_element_type=F32)


def _dot_t(a, b):
    return lax.dot_general(a, b, (((1,), (1,)), ((), ())), preferred_element_type=F32)


def _al(v, m):
    return pl.multiple_of(v, m)


class Links:
    def __init__(self):
        self.c, self.r, self.x, self.h = _coords()
        c, r, x, h = self.c, self.r, self.x, self.h
        self.partner = (c, 2 * x + (1 - h))
        self.xn = (c, 2 * (1 - x) + h)
        self.yn = (1 - c, r)
        self.diag = (1 - c, 2 * (1 - x) + h)
        self.xpartner = (c, 2 * (1 - x) + (1 - h))
        self.slot = r * 2 + c

    def barrier(self):
        sem = pltpu.get_barrier_semaphore()
        peers = (self.partner, self.xn, self.yn, self.diag, self.xpartner)
        for p in peers:
            pl.semaphore_signal(sem, inc=1, device_id=p, device_id_type=MESH)
        pl.semaphore_wait(sem, len(peers))


def _slot_of(dev):
    return dev[1] * 2 + dev[0]


def _remote(src, dst, ss, rs, dev):
    return pltpu.make_async_remote_copy(src_ref=src, dst_ref=dst, send_sem=ss, recv_sem=rs, device_id=dev, device_id_type=MESH)


class Prop:
    def __init__(self, lk, a, ei, eu, pi, pu, rf, ro, rx, ry, ss, rs):
        self.lk = lk
        self.a, self.ei, self.eu, self.pi, self.pu = a, ei, eu, pi, pu
        self.rf, self.ro, self.rx, self.ry = rf, ro, rx, ry
        self.ss, self.rs = ss, rs
        pu[...] = jnp.zeros_like(pu)

    def msg(self, kind, k, s):
        lk = self.lk
        ss, rs = self.ss.at[k, kind, s], self.rs.at[k, kind, s]
        other = 1 - lk.x
        if kind == FD:
            src = self.pi.at[:, pl.ds(_al((2 * other + 1 - lk.h) * IB + s * WX, 128), WX)]
            dst = self.rf.at[k, :, pl.ds(_al(s * WX, 128), WX)]
            return _remote(src, dst, ss, rs, lk.partner)
        if kind == XR:
            src = self.pi.at[:, pl.ds(_al((2 * other + lk.h) * IB + s * WX, 128), WX)]
            dst = self.rx.at[k, :, pl.ds(_al(s * WX, 128), WX)]
            return _remote(src, dst, ss, rs, lk.xn)
        if kind == FO:
            src = self.pi.at[:, pl.ds(_al((2 * lk.x + 1 - lk.h) * IB + s * WX, 128), WX)]
            dst = self.ro.at[k, :, pl.ds(_al(s * WX, 128), WX)]
            return _remote(src, dst, ss, rs, lk.partner)
        if kind in (GP, GX):
            ref = self.ei.at[k, :, pl.ds(_al(lk.r * IB + s * WX, 128), WX)]
            return _remote(ref, ref, ss, rs, lk.partner if kind == GP else lk.xn)
        if kind == GF:
            ref = self.ei.at[k, :, pl.ds(_al((2 * other + lk.h) * IB + s * WX, 128), WX)]
            return _remote(ref, ref, ss, rs, lk.partner)
        if kind == YR:
            src = self.pu.at[:, pl.ds(_al((1 - lk.c) * UB + s * WY, 128), WY)]
            dst = self.ry.at[k, :, pl.ds(_al(s * WY, 128), WY)]
            return _remote(src, dst, ss, rs, lk.yn)
        ref = self.eu.at[k, :, pl.ds(_al(lk.c * UB + s * WY, 128), WY)]
        return _remote(ref, ref, ss, rs, lk.yn)

    def put_item(self, k, s, value):
        self.ei[k, :, pl.ds(_al(self.lk.r * IB + s * WX, 128), WX)] = value
        self.msg(GX, k, s).start()
        self.msg(GP, k, s).start()

    def put_user(self, k, s, value):
        self.eu[k, :, pl.ds(_al(self.lk.c * UB + s * WY, 128), WY)] = value
        self.msg(YG, k, s).start()

    def wait_puts(self, k):
        for s in range(SX):
            self.msg(GX, k, s).wait_send()
            self.msg(GP, k, s).wait_send()
            if k == STEPS - 1:
                self.msg(GF, k, s).wait_send()
        for s in range(SY):
            self.msg(YG, k, s).wait_send()

    def step(self, k, user_final, item_final, between=None):
        lk = self.lk
        a, ei, eu, pi, pu = self.a, self.ei, self.eu, self.pi, self.pu
        far = (1 - lk.x) * 2 * IB
        near = lk.x * 2 * IB
        own_u = lk.c * UB
        peer_u = (1 - lk.c) * UB

        if k > 0:
            for s in range(SX):
                self.msg(FD, k - 1, s).wait_send()
                self.msg(XR, k - 1, s).wait_send()
                self.msg(FO, k - 1, s).wait_send()
                self.msg(GF, k - 1, s).wait_send()
        own_rows = pl.ds(_al(own_u, 128), UB)
        peer_rows = pl.ds(_al(peer_u, 128), UB)

        def over_own(j, _):
            cols = pl.ds(_al(far + j * (near - far), 128), 2 * IB)
            pi[:, cols] = _dot(eu[k, :, own_rows], a[own_rows, cols])
            return 0

        late_near = between is not None
        lax.fori_loop(0, 1 if late_near else 2, over_own, 0)
        for s in range(SY):
            self.msg(YG, k, s).wait_recv()

        def over_peer(stage, _):
            is_far = 1 - (stage // 2 if late_near else stage % 2)
            mine = stage % 2 if late_near else stage // 2
            half = mine * lk.h + (1 - mine) * (1 - lk.h)
            cols = pl.ds(_al(is_far * far + (1 - is_far) * near + half * IB, 128), IB)
            pi[:, cols] = pi[:, cols] + _dot(eu[k, :, peer_rows], a[peer_rows, cols])

            @pl.when(is_far * (1 - mine) == 1)
            def _():
                for s in range(SX):
                    self.msg(FD, k, s).start()

            @pl.when((1 - is_far) * (1 - mine) == 1)
            def _():
                for s in range(SX):
                    self.msg(FO, k, s).start()

            @pl.when(is_far * mine == 1)
            def _():
                for s in range(SX):
                    self.msg(FD, k, s).wait_recv()
                    cs = pl.ds(_al(far + lk.h * IB + s * WX, 128), WX)
                    pi[:, cs] = pi[:, cs] + self.rf[k, :, s * WX:(s + 1) * WX]
                    self.msg(XR, k, s).start()

            @pl.when((1 - is_far) * mine == 1)
            def _():
                for s in range(2):
                    self.msg(GX, k, s).wait_recv()
                    self.msg(GF, k, s).start()
            return 0

        if late_near:
            lax.fori_loop(0, 2, over_peer, 0)
            between()
            lax.fori_loop(1, 2, over_own, 0)
            lax.fori_loop(2, 4, over_peer, 0)
        else:
            lax.fori_loop(0, 4, over_peer, 0)

        if k > 0:
            for s in range(SY):
                self.msg(YR, k - 1, s).wait_send()
        for s in range(SX):
            self.msg(GP, k, s).wait_recv()

        def item_piece(s):
            self.msg(FO, k, s).wait_recv()
            self.msg(XR, k, s).wait_recv()
            c2 = pl.ds(_al(near + lk.h * IB + s * WX, 128), WX)
            piece = pl.ds(_al(s * WX, 128), WX)
            item_final(k, s, (pi[:, c2] + self.ro[k, :, piece]) + self.rx[k, :, piece])

        def user_piece(s):
            self.msg(YR, k, s).wait_recv()
            uc = pl.ds(_al(own_u + s * WY, 128), WY)
            user_final(k, s, pu[:, uc] + self.ry[k, :, s * WY:(s + 1) * WY])

        def users_tile(t, _):
            own = t // 4
            u = own * ((t // 2) % 2) + (1 - own) * (t % 2)
            is_far = own * (t % 2) + (1 - own) * ((t // 2) % 2)
            base = own * own_u + (1 - own) * peer_u + u * WY
            at = is_far * far + (1 - is_far) * near
            rows = pl.ds(_al(base, 512), WY)
            uc = pl.ds(_al(base, 128), WY)
            cols = pl.ds(_al(at, 128), 2 * IB)
            v = _dot_t(ei[k, :, cols], a[rows, cols])
            pu[:, uc] = v + jnp.where(is_far == 1, pu[:, uc], 0.0)

            @pl.when(t == 0)
            def _():
                for s in range(2, SX):
                    self.msg(GX, k, s).wait_recv()
                    self.msg(GF, k, s).start()

            @pl.when(t == 1)
            def _():
                for s in range(SX):
                    self.msg(GF, k, s).wait_recv()

            @pl.when((t == 2) | (t == 3))
            def _():
                self.msg(YR, k, t - 2).start()

            @pl.when(t == 3)
            def _():
                item_piece(0)

            @pl.when(t == 5)
            def _():
                item_piece(1)

            @pl.when(t == 6)
            def _():
                user_piece(0)
            return 0

        lax.fori_loop(0, 8, users_tile, 0)
        item_piece(2)
        user_piece(1)
        item_piece(3)

    def finish(self):
        k = STEPS - 1
        for s in range(SX):
            self.msg(FD, k, s).wait_send()
            self.msg(XR, k, s).wait_send()
            self.msg(FO, k, s).wait_send()
        for s in range(SY):
            self.msg(YR, k, s).wait_send()
        for k in range(STEPS):
            self.wait_puts(k)


class AllGather:
    def __init__(self, lk, ref, start, n_lo, n_hi, ss, rs):
        self.lk, self.ref, self.ss, self.rs = lk, ref, ss, rs
        self.full, self.lo, self.hi = pl.ds(start, n_lo + n_hi), pl.ds(start, n_lo), pl.ds(start + n_lo, n_hi)
        self.two = n_hi > 0

    def _copy(self, i):
        lk = self.lk
        xs, ys, ds_ = _slot_of(lk.xn), _slot_of(lk.yn), _slot_of(lk.diag)
        src_slot = (lk.slot, lk.slot, lk.slot, xs, ys, xs, ys, ds_, ds_)[i]
        dev = (lk.partner, lk.xn, lk.yn, lk.yn, lk.xn, lk.partner, lk.partner, lk.partner, lk.partner)[i]
        rows = (self.full, self.full, self.full, self.lo, self.hi, self.full, self.full, self.lo, self.hi)[i]
        ref = self.ref.at[src_slot, rows]
        return _remote(ref, ref, self.ss.at[i], self.rs.at[i], dev)

    def _used(self, i):
        return self.two or i not in (4, 8)

    def start(self):
        for i in (1, 2, 0):
            self._copy(i).start()

    def arrive(self, i):
        if not self._used(i):
            return
        self._copy(i).wait_recv()
        for j in {1: (3, 5), 2: (4, 6), 3: (7,), 4: (8,)}.get(i, ()):
            if self._used(j):
                self._copy(j).start()

    def slot(self, i):
        lk = self.lk
        c, x, h = lk.c, lk.x, lk.h
        row = {0: 2 * x + 1 - h, 1: 2 * (1 - x) + h, 2: lk.r, 4: 2 * (1 - x) + h,
               5: 2 * (1 - x) + 1 - h, 6: 2 * x + 1 - h, 8: 2 * (1 - x) + 1 - h}[i]
        col = {0: c, 1: c, 2: 1 - c, 4: 1 - c, 5: c, 6: 1 - c, 8: 1 - c}[i]
        return row * 2 + col

    def drain(self):
        for i in range(9):
            if self._used(i):
                self._copy(i).wait_send()


def _unpack_t(xt):
    n = xt.shape[1] // 2
    return jnp.concatenate([xt[:, :n], xt[:, n:]], axis=0).T


PROP_SCRATCH = [
    pltpu.VMEM((RU, CI), BF16),
    pltpu.VMEM((STEPS, D, CI), BF16),
    pltpu.VMEM((STEPS, D, RU), BF16),
    pltpu.VMEM((D, CI), F32),
    pltpu.VMEM((D, RU), F32),
    pltpu.VMEM((STEPS, D, IB), F32),
    pltpu.VMEM((STEPS, D, IB), F32),
    pltpu.VMEM((STEPS, D, IB), F32),
    pltpu.VMEM((STEPS, D, UB), F32),
    pltpu.SemaphoreType.DMA((STEPS, 8, 4)),
    pltpu.SemaphoreType.DMA((STEPS, 8, 4)),
]

CH = 64
NBUF = 4
NCH = RU // CH
AW = 8


def forward_kernel(mask, e0u, e0i, out_u, out_i, table, a_hbm,
                   a, ei, eu, pi, pu, rf, ro, rx, ry, ss, rs,
                   mbuf, msem, csum, rpart, dcol, drow, dss, drs, su, si, uacc, iacc, asem, iss, irs):
    lk = Links()

    def mask_copy(j):
        slot = j % NBUF
        return pltpu.make_async_copy(mask.at[pl.ds(_al(j * CH, CH), CH), :], mbuf.at[slot], msem.at[slot])

    for j in range(NBUF):
        mask_copy(j).start()
    lk.barrier()
    pr = Prop(lk, a, ei, eu, pi, pu, rf, ro, rx, ry, ss, rs)

    iacc[...] = e0i[...].astype(F32)
    for s in range(SX):
        pr.put_item(0, s, e0i[:, s * WX:(s + 1) * WX])
    uacc[...] = e0u[...].astype(F32)
    for s in range(SY):
        pr.put_user(0, s, e0u[:, s * WY:(s + 1) * WY])

    csum[...] = jnp.zeros_like(csum)

    def chunk(j, _):
        slot = j % NBUF
        mask_copy(j).wait()
        rows = pl.ds(_al(j * CH, CH), CH)

        def cols_body(w, acc):
            cols = pl.ds(_al(w * 512, 512), 512)
            v = mbuf[slot, :, cols].astype(F32)
            a[rows, cols] = v.astype(BF16)
            csum[:, cols] = csum[:, cols] + jnp.sum(v.reshape(CH // 8, 8, 512), axis=0)
            return acc + ((v[:, 0:128] + v[:, 128:256]) + (v[:, 256:384] + v[:, 384:512]))

        rpart[rows, :] = lax.fori_loop(0, CI // 512, cols_body, jnp.zeros((CH, 128), F32))

        @pl.when(j + NBUF < NCH)
        def _():
            mask_copy(j + NBUF).start()
        return 0

    lax.fori_loop(0, NCH, chunk, 0)

    ctot = jnp.sum(csum[...], axis=0, keepdims=True)
    for j in range(8):
        dcol[0, j:j + 1, :] = ctot[:, j * 1024:(j + 1) * 1024]
    drow[0] = _dot_t(jnp.ones((8, 128), BF16), rpart[...].astype(BF16))
    dcopies = [_remote(dcol.at[0], dcol.at[1 + i], dss.at[i], drs.at[i], dev)
               for i, dev in enumerate((lk.partner, lk.xn, lk.xpartner))]
    dcopies.append(_remote(drow.at[0], drow.at[1], dss.at[3], drs.at[3], lk.yn))
    for cp in dcopies:
        cp.start()
    for cp in dcopies:
        cp.wait_recv()
    ctot8 = (dcol[0] + dcol[1]) + (dcol[2] + dcol[3])
    sc8 = lax.rsqrt(jnp.maximum(ctot8, 1.0))
    for j in range(8):
        si[:, j * 1024:(j + 1) * 1024] = sc8[j:j + 1, :]
    su8 = lax.rsqrt(jnp.maximum(drow[0] + drow[1], 1.0))
    for j in range(RU // 128):
        su[j * 128:(j + 1) * 128, :] = jnp.broadcast_to(su8[0:1, j * 128:(j + 1) * 128], (128, 128)).T

    def a_copy(j):
        rows = pl.ds(_al(j * (RU // AW), RU // AW), RU // AW)
        return pltpu.make_async_copy(a.at[rows, :], a_hbm.at[rows, :], asem.at[j])

    def scale(first_col):
        def scale_rows(m, _):
            rows = pl.ds(_al(m * 64, 64), 64)
            s = su[rows, :]
            s4 = jnp.concatenate([s, s, s, s], axis=1)

            def scale_cols(w, _):
                cols = pl.ds(_al(first_col + w * 512, 512), 512)
                a[rows, cols] = a[rows, cols] * (s4 * si[:, cols]).astype(BF16)
                return 0

            lax.fori_loop(0, CI // 1024, scale_cols, 0)
            return 0

        lax.fori_loop(0, RU // 64, scale_rows, 0)

    def scale_near():
        scale(lk.x * 2 * IB)
        for j in range(AW):
            a_copy(j).start()

    scale((1 - lk.x) * 2 * IB)

    def user_final(k, s, v):
        b = v.astype(BF16)
        if k < STEPS - 1:
            pr.put_user(k + 1, s, b)
        uacc[:, s * WY:(s + 1) * WY] = uacc[:, s * WY:(s + 1) * WY] + b.astype(F32)
        if k == STEPS - 1 and s == SY - 1:
            t = uacc[...] * 0.25
            table[lk.slot, 0:PU, :] = _unpack_t(t).astype(BF16)
            ag_u.start()
            out_u[...] = t.astype(BF16)

    def item_final(k, s, v):
        b = v.astype(BF16)
        if k < STEPS - 1:
            pr.put_item(k + 1, s, b)
        iacc[:, s * WX:(s + 1) * WX] = iacc[:, s * WX:(s + 1) * WX] + b.astype(F32)
        if k == STEPS - 1:
            t = iacc[:, s * WX:(s + 1) * WX] * 0.25
            table[lk.slot, PU + s * WX // 2:PU + (s + 1) * WX // 2, :] = _unpack_t(t).astype(BF16)
            ags[s].start()
            out_i[:, s * WX:(s + 1) * WX] = t.astype(BF16)

    ags = [AllGather(lk, table, PU + s * WX // 2, WX // 4, WX // 4, iss.at[s], irs.at[s]) for s in range(SX)]
    ag_u = AllGather(lk, table, 0, PU // 2, PU // 2, iss.at[SX], irs.at[SX])
    ags.append(ag_u)
    for k in range(STEPS):
        pr.step(k, user_final, item_final, scale_near if k == 0 else None)
    for group in ((1, 2), (3, 4), (0, 5, 6, 7, 8)):
        for s in (SX, 0, 1, 2, 3):
            for i in group:
                ags[s].arrive(i)
    for cp in dcopies:
        cp.wait_send()
    for j in range(AW):
        a_copy(j).wait()
    pr.finish()
    for ag in ags:
        ag.drain()


def lookup_kernel(table_hbm, ids, out, table, tsem, tab, gu, gp, gn):
    def load(b):
        return pltpu.make_async_copy(table_hbm.at[b], table.at[b], tsem.at[b])

    for b in range(8):
        load(b).start()

    def unpack(b, _):
        load(b).wait()
        for lo, n, dst in [(0, PU, 0)] + [(PU + s * WX // 2, WX // 2, UB + s * WX) for s in range(SX)]:
            for o in range(0, n, 128):
                v = table[b, lo + o:lo + o + 128, :].astype(F32)
                base = b * (UB + IB) + dst + o
                tab[pl.ds(_al(base, 128), 128), :] = v
                tab[pl.ds(_al(base + n, 128), 128), :] = pltpu.roll(v, D, 1)
        return 0

    lax.fori_loop(0, 8, unpack, 0)

    def gather(g, _):
        for o in range(16):
            t = g * 16 + o
            gu[pl.ds(t, 1), :] = tab[pl.ds(ids[t], 1), :]
            gp[pl.ds(t, 1), :] = tab[pl.ds(ids[TB + t], 1), :]
            gn[pl.ds(t, 1), :] = tab[pl.ds(ids[2 * TB + t], 1), :]
        return 0

    lax.fori_loop(0, TB // 16, gather, 0)

    def block(m, tot):
        rows = pl.ds(_al(m * 256, 256), 256)
        left = lax.broadcasted_iota(jnp.int32, (256, 128), 1) < D
        e_u = gu[rows, :]
        e_d = gp[rows, :] - gn[rows, :]
        x = jnp.sum(jnp.where(left, e_u * e_d, 0.0), axis=1, keepdims=True)
        z = jnp.exp(-jnp.abs(x))
        loss = jnp.maximum(-x, 0.0) + jnp.log1p(z)
        sig = jnp.where(x >= 0.0, z, 1.0) / (1.0 + z)
        coef = sig * (-1.0 / NT)
        out[rows, :] = jnp.where(left, coef * e_d, pltpu.roll(coef * e_u, D, 1))
        return tot + jnp.sum(loss, axis=0, keepdims=True)

    tot = lax.fori_loop(0, TB // 256, block, jnp.zeros((1, 1), F32))
    out[TB:TB + 8, :] = jnp.broadcast_to(tot, (8, 128))


def backward_kernel(a_hbm, g_in, ids, out_u, out_i, out_l,
                    a, ei, eu, pi, pu, rf, ro, rx, ry, ss, rs,
                    asem, g_all, gsem, gss, grs, wu, wi, acc_u, acc_i, su, si):
    lk = Links()
    loads = [pltpu.make_async_copy(a_hbm, a, asem)]
    gcopy = pltpu.make_async_copy(g_in, g_all.at[lk.slot], gsem)
    gcopy.start()
    loads[0].start()
    lk.barrier()
    pr = Prop(lk, a, ei, eu, pi, pu, rf, ro, rx, ry, ss, rs)
    gcopy.wait()
    ag = AllGather(lk, g_all, 0, TB // 2, TB // 2 + 8, gss, grs)
    ag.start()
    acc_u[...] = jnp.zeros_like(acc_u)
    acc_i[...] = jnp.zeros_like(acc_i)
    base_u = lk.slot * UB
    base_i = (lk.c * 4 + lk.r) * IB

    def scatter(b):
        def split(m, _):
            rows = pl.ds(_al(m * 256, 256), 256)
            left = lax.broadcasted_iota(jnp.int32, (256, 128), 1) < D
            g = g_all[b, rows, :]
            hi = g.astype(BF16).astype(F32)
            r1 = g - hi
            mid = r1.astype(BF16).astype(F32)
            lo = r1 - mid
            wu[rows, 0:128] = jnp.where(left, hi, pltpu.roll(mid, D, 1)).astype(BF16)
            wu[rows, 128:256] = lo.astype(BF16)
            wi[rows, 0:128] = jnp.where(left, pltpu.roll(hi, D, 1), mid).astype(BF16)
            wi[rows, 128:256] = pltpu.roll(lo, D, 1).astype(BF16)
            return 0

        lax.fori_loop(0, TB // 256, split, 0)
        cols = pl.ds(_al(b * TB, 128), TB)
        sub = lax.broadcasted_iota(jnp.int32, (256, TB), 0).astype(F32).astype(BF16)
        one, zero = jnp.array(1.0, BF16), jnp.array(0.0, BF16)

        def lanes(which, base):
            v = ids[which:which + 1, cols] - base
            v = jnp.where((v >= 0) & (v < 256), v, -1).astype(F32)
            return jnp.broadcast_to(v, (256, TB)).astype(BF16)

        def hot(which, base):
            return jnp.concatenate([jnp.where(lanes(which, base + m * 256) == sub, one, zero) for m in range(4)], axis=0)

        acc_u[...] = acc_u[...] + _dot(hot(0, base_u), wu[...])

        def items(m, _):
            rows = pl.ds(_al(m * 1024, 1024), 1024)
            acc_i[rows, :] = acc_i[rows, :] + _dot(hot(1, base_i + m * 1024) - hot(2, base_i + m * 1024), wi[...])
            return 0

        lax.fori_loop(0, IB // 1024, items, 0)

    scatter(lk.slot)
    for group, done in (((0,), 0), ((1, 2), 1), ((), 2), ((5,), 5), ((3, 4, 6), 6), ((), 4), ((7, 8), 8)):
        for i in group:
            ag.arrive(i)
        scatter(ag.slot(done))

    loss = g_all[0, TB:TB + 8, :]
    for b in range(1, 8):
        loss = loss + g_all[b, TB:TB + 8, :]
    out_l[...] = loss * (1.0 / NT)

    def seed(acc):
        s = (acc[:, 0:128] + pltpu.roll(acc[:, 0:128], D, 1)) + acc[:, 128:256]
        n = s.shape[0] // 2
        s = s * 0.25
        left = lax.broadcasted_iota(jnp.int32, (n, 128), 1) < D
        return jnp.where(left, s[:n], pltpu.roll(s[n:], D, 1)).T

    xu = seed(acc_u[...])
    for s in range(SY):
        v = xu[:D] if s == 0 else xu[D:]
        su[:, s * WY:(s + 1) * WY] = v
        pr.put_user(0, s, v.astype(BF16))
    xi = seed(acc_i[...])
    for s in range(SX):
        src = xi[:D] if s < SX // 2 else xi[D:]
        o = (s % (SX // 2)) * WX
        v = src[:, o:o + WX]
        si[:, s * WX:(s + 1) * WX] = v
        pr.put_item(0, s, v.astype(BF16))

    def user_final(k, s, v):
        v = su[:, s * WY:(s + 1) * WY] + v
        if k < STEPS - 1:
            pr.put_user(k + 1, s, v.astype(BF16))
        else:
            out_u[:, s * WY:(s + 1) * WY] = v

    def item_final(k, s, v):
        v = si[:, s * WX:(s + 1) * WX] + v
        if k < STEPS - 1:
            pr.put_item(k + 1, s, v.astype(BF16))
        else:
            out_i[:, s * WX:(s + 1) * WX] = v

    loads[0].wait()
    for k in range(STEPS):
        pr.step(k, user_final, item_final)
    pr.finish()
    ag.drain()


def finish_kernel(*refs):
    for src, dst in zip(refs[:4], refs[5:9]):
        dst[...] = src[...]
    refs[9][...] = refs[4][0:1, 0:1]


VM = pl.BlockSpec(memory_space=pltpu.VMEM)
SM = pl.BlockSpec(memory_space=pltpu.SMEM)
ANY = pl.BlockSpec(memory_space=pl.ANY)
DMA = pltpu.SemaphoreType.DMA


def _params(cid):
    return pltpu.CompilerParams(collective_id=cid, has_side_effects=True, vmem_limit_bytes=VMEM_LIMIT)


def solution(mesh):
    def local_fn(mask, e0u, e0i, triples):
        c, r, _, _ = _coords()
        slot = r * 2 + c
        out_u, out_i, table, a_hbm = pl.pallas_call(
            forward_kernel,
            name='forward',
            out_shape=(jax.ShapeDtypeStruct((D, UB), BF16), jax.ShapeDtypeStruct((D, IB), BF16),
                       jax.ShapeDtypeStruct((8, PR, 128), BF16), jax.ShapeDtypeStruct((RU, CI), BF16)),
            in_specs=[ANY, VM, VM],
            out_specs=(VM, VM, VM, ANY),
            scratch_shapes=PROP_SCRATCH + [
                pltpu.VMEM((NBUF, CH, CI), jnp.int32), DMA((NBUF,)),
                pltpu.VMEM((8, CI), F32), pltpu.VMEM((RU, 128), F32),
                pltpu.VMEM((4, 8, 1024), F32), pltpu.VMEM((2, 8, RU), F32), DMA((4,)), DMA((4,)),
                pltpu.VMEM((RU, 128), F32), pltpu.VMEM((1, CI), F32),
                pltpu.VMEM((D, UB), F32), pltpu.VMEM((D, IB), F32), DMA((AW,)),
                DMA((SX + 1, 9)), DMA((SX + 1, 9)),
            ],
            compiler_params=_params(0),
        )(mask, e0u.T, e0i.T)

        cols = triples.T
        mine = lax.dynamic_slice(cols, (0, slot * TB), (3, TB))
        per = UB + IB
        blk = mine // IB
        row_i = ((blk % 4) * 2 + blk // 4) * per + UB + mine % IB
        row_u = (mine // UB) * per + mine % UB
        ids = jnp.where(lax.broadcasted_iota(jnp.int32, (3, TB), 0) == 0, row_u, row_i)
        g = pl.pallas_call(
            lookup_kernel,
            name='lookup',
            out_shape=jax.ShapeDtypeStruct((TB + 8, 128), F32),
            in_specs=[ANY, SM],
            out_specs=VM,
            scratch_shapes=[pltpu.VMEM((8, PR, 128), BF16), DMA((8,)), pltpu.VMEM((8 * per, 128), F32)] + [pltpu.VMEM((TB, 128), F32)] * 3,
            compiler_params=pltpu.CompilerParams(vmem_limit_bytes=VMEM_LIMIT),
        )(table, ids.reshape(-1))

        d_u, d_i, loss = pl.pallas_call(
            backward_kernel,
            name='backward',
            out_shape=(jax.ShapeDtypeStruct((D, UB), F32), jax.ShapeDtypeStruct((D, IB), F32),
                       jax.ShapeDtypeStruct((8, 128), F32)),
            in_specs=[ANY, ANY, VM],
            out_specs=(VM, VM, VM),
            scratch_shapes=PROP_SCRATCH + [
                DMA, pltpu.VMEM((8, TB + 8, 128), F32), DMA, DMA((9,)), DMA((9,)),
                pltpu.VMEM((TB, 256), BF16), pltpu.VMEM((TB, 256), BF16),
                pltpu.VMEM((UB, 256), F32), pltpu.VMEM((IB, 256), F32),
                pltpu.VMEM((D, UB), F32), pltpu.VMEM((D, IB), F32),
            ],
            compiler_params=_params(1),
        )(a_hbm, g, cols)
        outs = (out_u, out_i, d_u, d_i)
        out_u, out_i, d_u, d_i, loss = pl.pallas_call(
            finish_kernel,
            name='finish',
            out_shape=tuple(jax.ShapeDtypeStruct(o.shape, o.dtype) for o in outs) + (jax.ShapeDtypeStruct((1, 1), F32),),
            in_specs=[VM] * 5,
            out_specs=(VM,) * 5,
        )(*outs, loss)
        return out_u.T, out_i.T, loss.reshape(()), d_u.T, d_i.T

    user_spec = P(('row', 'col'), None)
    item_spec = P(('col', 'row'), None)
    return jax.shard_map(local_fn, mesh=mesh, in_specs=(P('row', 'col'), user_spec, item_spec, P()),
                         out_specs=(user_spec, item_spec, P(), user_spec, item_spec), check_vma=False)
```
